8 devices in a mesh: dp: 1 (over z), cx: 2 (over y), cy: 2 (over x), cz: 2 (over core).
Axes of the slice: x: 2, y: 2, z: 1, core: 2. Of those that a mesh axis runs over, the one named last changes fastest.
Arguments:
- q: bfloat16 [2048, 64, 128], P(('dp', 'cx', 'cy', 'cz'))
- k: bfloat16 [2048, 8, 128], P(('dp', 'cx', 'cy', 'cz'))
- v: bfloat16 [2048, 8, 128], P(('dp', 'cx', 'cy', 'cz'))
Outputs:
- output: bfloat16 [2048, 64, 128], P(('dp', 'cx', 'cy', 'cz'))
All inputs are finite; a program needn't handle non-finite values.
Results may differ from the reference program's by a relative error of at most 0.00596145.
Values are sent between devices in bfloat16 or wider.
A program may use at most 1 GiB of HBM per device.

```python
import jax
import jax.numpy as jnp
from jax import lax

TOK = 256
DEV = 8
HQ = 64
HKV = 8
HEAD = 128


def setup_inputs(seed: int = 0, part: int = 0) -> dict:
    n = TOK * DEV
    key = jax.random.fold_in(jax.random.PRNGKey(seed), part)
    kq, kk, kv = jax.random.split(key, 3)
    q = jax.random.normal(kq, (n, HQ, HEAD), jnp.float32)
    k = jax.random.normal(kk, (n, HKV, HEAD), jnp.float32)
    v = jax.random.normal(kv, (n, HKV, HEAD), jnp.float32) * (0.5 * n ** 0.25)
    return {'q': q.astype(jnp.bfloat16), 'k': k.astype(jnp.bfloat16), 'v': v.astype(jnp.bfloat16)}


def reference(q, k, v):
    n = TOK * DEV
    g = HQ // HKV
    qb = min(n, 64)
    r = jnp.arange(n)
    pos = (r % TOK) * DEV + r // TOK
    kt = jnp.transpose(k, (1, 0, 2)).astype(jnp.float32)
    vt = jnp.transpose(v, (1, 0, 2)).astype(jnp.float32)
    qr = jnp.transpose(q.reshape(n // qb, qb, HKV, g, HEAD), (0, 2, 1, 3, 4))

    def head(qh, kh, vh, qp):
        s = jnp.einsum('qgd,kd->qgk', qh.astype(jnp.float32), kh) * HEAD ** -0.5
        s = jnp.where((pos[None, :] <= qp[:, None])[:, None, :], s, -jnp.inf)
        p = jnp.exp(s - jnp.max(s, axis=-1, keepdims=True))
        l = jnp.sum(p, axis=-1)
        o = jnp.einsum('qgk,kd->qgd', p.astype(jnp.bfloat16).astype(jnp.float32), vh)
        return o / l[..., None]

    def block(args):
        qblk, qp = args
        o = lax.map(lambda a: head(a[0], a[1], a[2], qp), (qblk, kt, vt))
        return jnp.transpose(o, (1, 0, 2, 3)).reshape(qb, HQ, HEAD)

    o = lax.map(block, (qr, pos.reshape(n // qb, qb)))
    return o.reshape(n, HQ, HEAD).astype(jnp.bfloat16)
```

```python
import functools
import jax
import jax.numpy as jnp
from jax import lax
from jax.experimental import pallas as pl
from jax.experimental.pallas import tpu as pltpu
from jax.sharding import PartitionSpec as P

T = 256
HQ = 64
HKV = 8
G = 8
D = 128
DEV = 8
NB = 8
SUB = T // NB
KB = DEV * SUB
C = (D ** -0.5) * 1.4426950408889634
NT = (((1,), (1,)), ((), ()))
AXES = ("cx", "cy", "cz")


def attn(q_ref, k_ref, v_ref, o_ref, bias, vt):
    me = (lax.axis_index("cx") * 2 + lax.axis_index("cy")) * 2 + lax.axis_index("cz")

    @pl.when(pl.program_id(0) == 0)
    def _():
        kk = lax.broadcasted_iota(jnp.int32, (KB, KB), 0)
        qq = lax.broadcasted_iota(jnp.int32, (KB, KB), 1)
        kpos = (kk % SUB) * DEV + kk // SUB
        qpos = (qq // G) * DEV + me
        bias[...] = jnp.where(kpos <= qpos, 0.0, -1e30)

    vt[...] = v_ref[0].T
    for j in range(NB):
        n = (j + 1) * KB
        q = q_ref[j * SUB:(j + 1) * SUB].reshape(KB, D)
        s = lax.dot_general(k_ref[0, :n], q, NT, preferred_element_type=jnp.float32)
        d = s[n - KB:] + bias[...]
        s = jnp.concatenate([s[:n - KB], d], axis=0) if j else d
        m = jnp.max(s, axis=0, keepdims=True)
        p = jnp.exp2((s - m) * C)
        l = jnp.sum(p, axis=0, keepdims=True)
        o = jnp.dot(vt[:, :n], p.astype(jnp.bfloat16), preferred_element_type=jnp.float32)
        o = (o * (1.0 / l)).T
        o_ref[j * SUB:(j + 1) * SUB] = o.astype(jnp.bfloat16).reshape(SUB, G, D)


def solution(mesh):
    spec = P(("dp", "cx", "cy", "cz"))

    def order(x):
        x = lax.all_gather(x, AXES, axis=0, tiled=True)
        x = x.reshape(DEV, NB, SUB, HKV, D)
        return jnp.transpose(x, (3, 1, 0, 2, 4)).reshape(HKV, DEV * T, D)

    def local(q, k, v):
        qo = pl.BlockSpec((T, G, D), lambda h: (0, h, 0))
        kv = pl.BlockSpec((1, DEV * T, D), lambda h: (h, 0, 0))
        return pl.pallas_call(
            attn,
            grid=(HKV,),
            out_shape=jax.ShapeDtypeStruct(q.shape, q.dtype),
            in_specs=[qo, kv, kv],
            out_specs=qo,
            scratch_shapes=[pltpu.VMEM((KB, KB), jnp.float32), pltpu.VMEM((D, DEV * T), jnp.bfloat16)],
            compiler_params=pltpu.CompilerParams(vmem_limit_bytes=60 << 20),
        )(q, order(k), order(v))

    return jax.shard_map(local, mesh=mesh, in_specs=(spec, spec, spec), out_specs=spec, check_vma=False)
```

```python
import jax
import jax.numpy as jnp
from jax import lax
from jax.experimental import pallas as pl
from jax.experimental.pallas import tpu as pltpu
from jax.sharding import PartitionSpec as P

T = 256
HKV = 8
G = 8
D = 128
NB = 8
SUB = T // NB
QB = SUB * G
S1 = 6
S2 = 2
C = (D ** -0.5) * 1.4426950408889634
NT = (((1,), (1,)), ((), ()))
ORDER = (0, 2, 4, 6, 7, 5, 3, 1)
BF = jnp.bfloat16
F32 = jnp.float32


def chunks(n):
    return [(r, min(r + 256, n)) for r in range(0, n, 256)]


def fold(f, x):
    return f(x.reshape(-1, 8, x.shape[-1]), axis=0)


def blocks(nslot, q_of, k_of, vt, bias, sref, begin, finish):
    rows = nslot * SUB
    st = {}

    def scores(j, c):
        r0, r1 = c
        parts = [k_of(*divmod(u, nslot)) for u in range(r0 // SUB, r1 // SUB)]
        s = lax.dot_general(jnp.concatenate(parts, axis=0), q_of(j), NT, preferred_element_type=F32)
        lo = max(r0, j * rows)
        if lo < r1:
            d = s[lo - r0:] + bias[lo - j * rows:r1 - j * rows]
            s = d if lo == r0 else jnp.concatenate([s[:lo - r0], d], axis=0)
        sref[ORDER.index(j) % 2, r0:r1] = s
        m = fold(jnp.max, s)
        st[j] = jnp.maximum(st[j], m) if j in st else m

    def values(j, c, m, acc):
        r0, r1 = c
        p = jnp.exp2((sref[ORDER.index(j) % 2, r0:r1] - m) * C)
        l = fold(jnp.sum, p)
        o = jnp.dot(vt[:, r0:r1], p.astype(BF), preferred_element_type=F32)
        return (acc[0] + l, acc[1] + o) if acc else (l, o)

    for c in chunks((ORDER[0] + 1) * rows):
        scores(ORDER[0], c)
    for i, j in enumerate(ORDER):
        m, a = begin(j, jnp.max(st[j], axis=0, keepdims=True))
        acc = None
        mine = chunks((j + 1) * rows)
        later = chunks((ORDER[i + 1] + 1) * rows) if i + 1 < NB else []
        done = 0
        for t, c in enumerate(mine):
            upto = len(later) * (t + 1) // len(mine)
            for u in range(done, upto):
                scores(ORDER[i + 1], later[u])
            done = upto
            acc = values(j, c, m, acc)
        finish(j, m, a, jnp.sum(acc[0], axis=0, keepdims=True), acc[1])


def kernel(q_hbm, k_hbm, v_hbm, o_hbm, qb, ob, raw, wide, kv1, kv2, vt, sref, bias1, bias2, oacc, ml,
           lsem, qsem, osem, ssem, rsem):
    cx, cy, cz = lax.axis_index("cx"), lax.axis_index("cy"), lax.axis_index("cz")
    me = (cx * 2 + cy) * 2 + cz
    nx = {"cy": 1 - cy}
    ny = {"cx": 1 - cx}
    sib = {"cz": 1 - cz}

    barrier = pltpu.get_barrier_semaphore()
    for dev in (nx, ny, sib):
        pl.semaphore_signal(barrier, inc=1, device_id=dev, device_id_type=pl.DeviceIdType.MESH)

    loads = [pltpu.make_async_copy(x, raw.at[i], lsem.at[i]) for i, x in enumerate((k_hbm, v_hbm))]
    for x in loads:
        x.start()

    def qload(h):
        return pltpu.make_async_copy(q_hbm.at[:, pl.ds(pl.multiple_of(h * G, G), G), :], qb.at[h], qsem.at[h])

    def ostore(h):
        return pltpu.make_async_copy(ob.at[h], o_hbm.at[:, pl.ds(pl.multiple_of(h * G, G), G), :], osem.at[h])

    @pl.loop(0, HKV)
    def _(h):
        qload(h).start()

    def rdma(kind, h):
        src, dst, dev = (
            (kv1.at[h, :, :, 0], kv1.at[h, :, :, 2], nx),
            (kv1.at[h, :, :, 0], kv1.at[h, :, :, 4], ny),
            (kv1.at[h, :, :, 0], kv1.at[h, :, :, 1], sib),
            (kv1.at[h, :, :, 2], kv1.at[h, :, :, 3], sib),
            (kv1.at[h, :, :, 4], kv1.at[h, :, :, 5], sib),
            (kv1.at[h, 0, :, 2], kv2.at[h, 0, :, 0], ny),
            (kv1.at[h, 1, :, 4], kv2.at[h, 1, :, 0], nx),
            (kv2.at[h, :, :, 0], kv2.at[h, :, :, 1], sib),
        )[kind]
        return pltpu.make_async_remote_copy(src, dst, ssem.at[kind, h], rsem.at[kind, h], dev,
                                            pl.DeviceIdType.MESH)

    def mask(nslot, base, ref):
        r = lax.broadcasted_iota(jnp.int32, (nslot * SUB, QB), 0)
        c = lax.broadcasted_iota(jnp.int32, (nslot * SUB, QB), 1)
        kpos = (r % SUB) * 8 + (me ^ (r // SUB + base))
        qpos = (c // G) * 8 + me
        ref[...] = jnp.where(kpos <= qpos, 0.0, -1e30)

    for i in range(2):
        loads[i].wait()
        wide[...] = raw[i].astype(F32).reshape(T * HKV, D)
        for h in range(HKV):
            kv1[h, i, :, 0] = wide[pl.ds(h, T, stride=HKV), :].astype(BF).reshape(NB, SUB, D)
    pl.semaphore_wait(barrier, 3)

    @pl.loop(0, HKV)
    def _(h):
        for kind in range(3):
            rdma(kind, h).start()

    mask(S1, 0, bias1)
    mask(S2, S1, bias2)

    def pass_on(h):
        rdma(0, h).wait_recv()
        rdma(1, h).wait_recv()
        for kind in (3, 4, 5, 6):
            rdma(kind, h).start()

    def pass_on2(h):
        rdma(5, h).wait_recv()
        rdma(6, h).wait_recv()
        rdma(7, h).start()

    pass_on(0)

    @pl.loop(0, HKV)
    def _(h):
        @pl.when(h < HKV - 1)
        def _():
            pass_on(h + 1)

        qload(h).wait()
        for kind in (2, 3, 4):
            rdma(kind, h).wait_recv()
        vt[...] = kv1[h, 1].reshape(S1 * T, D).T

        def finish(j, m, a, l, o):
            oacc[h, j] = o
            ml[h, j, 0:1] = m
            ml[h, j, 1:2] = l

        blocks(S1, lambda j: qb[h, j * SUB:(j + 1) * SUB].reshape(QB, D), lambda t, s: kv1[h, 0, t, s],
               vt, bias1, sref, lambda j, m: (m, None), finish)

    pass_on2(0)

    @pl.loop(0, HKV)
    def _(h):
        @pl.when(h < HKV - 1)
        def _():
            pass_on2(h + 1)

        rdma(7, h).wait_recv()
        vt[:, :S2 * T] = kv2[h, 1].reshape(S2 * T, D).T

        def begin(j, m):
            m1 = ml[h, j, 0:1]
            m = jnp.maximum(m, m1)
            return m, jnp.exp2((m1 - m) * C)

        def finish(j, m, a, l, o):
            l = ml[h, j, 1:2] * a + l
            r = 1.0 / l
            o = oacc[h, j] * (a * r) + o * r
            ob[h, j * SUB:(j + 1) * SUB] = o.T.astype(BF).reshape(SUB, G, D)

        blocks(S2, lambda j: qb[h, j * SUB:(j + 1) * SUB].reshape(QB, D), lambda t, s: kv2[h, 0, t, s],
               vt, bias2, sref, begin, finish)
        ostore(h).start()

    @pl.loop(0, HKV)
    def _(h):
        for kind in range(8):
            rdma(kind, h).wait_send()
        ostore(h).wait()


def solution(mesh):
    spec = P(("dp", "cx", "cy", "cz"))

    def local(q, k, v):
        hbm = pl.BlockSpec(memory_space=pl.ANY)
        return pl.pallas_call(
            kernel,
            out_shape=jax.ShapeDtypeStruct(q.shape, q.dtype),
            in_specs=[hbm] * 3,
            out_specs=hbm,
            scratch_shapes=[
                pltpu.VMEM((HKV, T, G, D), BF),
                pltpu.VMEM((HKV, T, G, D), BF),
                pltpu.VMEM((2, T, HKV, D), BF),
                pltpu.VMEM((T * HKV, D), F32),
                pltpu.VMEM((HKV, 2, NB, S1, SUB, D), BF),
                pltpu.VMEM((HKV, 2, NB, S2, SUB, D), BF),
                pltpu.VMEM((D, S1 * T), BF),
                pltpu.VMEM((2, S1 * T, QB), F32),
                pltpu.VMEM((S1 * SUB, QB), F32),
                pltpu.VMEM((S2 * SUB, QB), F32),
                pltpu.VMEM((HKV, NB, D, QB), F32),
                pltpu.VMEM((HKV, NB, 8, QB), F32),
                pltpu.SemaphoreType.DMA((2,)),
                pltpu.SemaphoreType.DMA((HKV,)),
                pltpu.SemaphoreType.DMA((HKV,)),
                pltpu.SemaphoreType.DMA((8, HKV)),
                pltpu.SemaphoreType.DMA((8, HKV)),
            ],
            compiler_params=pltpu.CompilerParams(
                vmem_limit_bytes=60 << 20, collective_id=0, has_side_effects=True),
        )(q, k, v)

    return jax.shard_map(local, mesh=mesh, in_specs=(spec, spec, spec), out_specs=spec, check_vma=False)
```

```python
import jax
import jax.numpy as jnp
from jax import lax
from jax.experimental import pallas as pl
from jax.experimental.pallas import tpu as pltpu
from jax.sharding import PartitionSpec as P

T = 256
HKV = 8
G = 8
D = 128
NB = 8
SUB = T // NB
QB = SUB * G
S1 = 6
S2 = 2
C = (D ** -0.5) * 1.4426950408889634
NT = (((1,), (1,)), ((), ()))
ORDER = (0, 2, 4, 6, 7, 5, 3, 1)
BF = jnp.bfloat16
F32 = jnp.float32


def chunks(n):
    return [(r, min(r + 256, n)) for r in range(0, n, 256)]


def by_tile(kv, h, nslot):
    return jnp.concatenate([kv[h, s, 1, t * SUB:(t + 1) * SUB] for t in range(NB) for s in range(nslot)], axis=0)


def fold(f, x):
    return f(x.reshape(-1, 8, x.shape[-1]), axis=0)


def blocks(nslot, q_of, k_of, vt, bias, sref, begin, finish):
    rows = nslot * SUB
    st = {}

    def scores(j, c):
        r0, r1 = c
        parts = [k_of(*divmod(u, nslot)) for u in range(r0 // SUB, r1 // SUB)]
        s = lax.dot_general(jnp.concatenate(parts, axis=0), q_of(j), NT, preferred_element_type=F32)
        lo = max(r0, j * rows)
        if lo < r1:
            d = s[lo - r0:] + bias[lo - j * rows:r1 - j * rows]
            s = d if lo == r0 else jnp.concatenate([s[:lo - r0], d], axis=0)
        sref[ORDER.index(j) % 2, r0:r1] = s
        m = fold(jnp.max, s)
        st[j] = jnp.maximum(st[j], m) if j in st else m

    def values(j, c, m, acc):
        r0, r1 = c
        p = jnp.exp2((sref[ORDER.index(j) % 2, r0:r1] - m) * C)
        l = fold(jnp.sum, p)
        o = jnp.dot(vt[:, r0:r1], p.astype(BF), preferred_element_type=F32)
        return (acc[0] + l, acc[1] + o) if acc else (l, o)

    for c in chunks((ORDER[0] + 1) * rows):
        scores(ORDER[0], c)
    for i, j in enumerate(ORDER):
        m, a = begin(j, jnp.max(st[j], axis=0, keepdims=True))
        acc = None
        mine = chunks((j + 1) * rows)
        later = chunks((ORDER[i + 1] + 1) * rows) if i + 1 < NB else []
        done = 0
        for t, c in enumerate(mine):
            upto = len(later) * (t + 1) // len(mine)
            for u in range(done, upto):
                scores(ORDER[i + 1], later[u])
            done = upto
            acc = values(j, c, m, acc)
        finish(j, m, a, jnp.sum(acc[0], axis=0, keepdims=True), acc[1])


def kernel(q_hbm, k_hbm, v_hbm, ob, qb, raw, wide, kv1, kv2, vt, sref, bias1, bias2, oacc, ml,
           lsem, qsem, ssem, rsem):
    cx, cy, cz = lax.axis_index("cx"), lax.axis_index("cy"), lax.axis_index("cz")
    me = (cx * 2 + cy) * 2 + cz
    nx = {"cy": 1 - cy}
    ny = {"cx": 1 - cx}
    sib = {"cz": 1 - cz}

    barrier = pltpu.get_barrier_semaphore()
    for dev in (nx, ny, sib):
        pl.semaphore_signal(barrier, inc=1, device_id=dev, device_id_type=pl.DeviceIdType.MESH)

    loads = [pltpu.make_async_copy(x, raw.at[i], lsem.at[i]) for i, x in enumerate((k_hbm, v_hbm))]
    for x in loads:
        x.start()

    def qload(h):
        return pltpu.make_async_copy(q_hbm.at[:, pl.ds(pl.multiple_of(h * G, G), G), :], qb.at[h], qsem.at[h])

    @pl.loop(0, HKV)
    def _(h):
        qload(h).start()

    def rdma(kind, h):
        src, dst, dev = (
            (kv1.at[h, 0], kv1.at[h, 2], nx),
            (kv1.at[h, 0], kv1.at[h, 4], ny),
            (kv1.at[h, 0], kv1.at[h, 1], sib),
            (kv1.at[h, 2], kv1.at[h, 3], sib),
            (kv1.at[h, 4], kv1.at[h, 5], sib),
            (kv1.at[h, 2, 0], kv2.at[h, 0, 0], ny),
            (kv1.at[h, 4, 1], kv2.at[h, 0, 1], nx),
            (kv2.at[h, 0], kv2.at[h, 1], sib),
        )[kind]
        return pltpu.make_async_remote_copy(src, dst, ssem.at[kind, h], rsem.at[kind, h], dev,
                                            pl.DeviceIdType.MESH)

    def mask(nslot, base, ref):
        r = lax.broadcasted_iota(jnp.int32, (nslot * SUB, QB), 0)
        c = lax.broadcasted_iota(jnp.int32, (nslot * SUB, QB), 1)
        kpos = (r % SUB) * 8 + (me ^ (r // SUB + base))
        qpos = (c // G) * 8 + me
        ref[...] = jnp.where(kpos <= qpos, 0.0, -1e30)

    for i in range(2):
        loads[i].wait()
        wide[...] = raw[i].astype(F32).reshape(T * HKV, D)
        for h in range(HKV):
            kv1[h, 0, i] = wide[pl.ds(h, T, stride=HKV), :].astype(BF)
    pl.semaphore_wait(barrier, 3)

    @pl.loop(0, HKV)
    def _(h):
        for kind in range(3):
            rdma(kind, h).start()

    mask(S1, 0, bias1)
    mask(S2, S1, bias2)

    def pass_on(h):
        rdma(0, h).wait_recv()
        rdma(1, h).wait_recv()
        for kind in (3, 4, 5, 6):
            rdma(kind, h).start()

    def pass_on2(h):
        rdma(5, h).wait_recv()
        rdma(6, h).wait_recv()
        rdma(7, h).start()

    pass_on(0)

    @pl.loop(0, HKV)
    def _(h):
        @pl.when(h < HKV - 1)
        def _():
            pass_on(h + 1)

        qload(h).wait()
        for kind in (2, 3, 4):
            rdma(kind, h).wait_recv()
        vt[...] = by_tile(kv1, h, S1).T

        def finish(j, m, a, l, o):
            oacc[h, j] = o
            ml[h, j, 0:1] = m
            ml[h, j, 1:2] = l

        blocks(S1, lambda j: qb[h, j * SUB:(j + 1) * SUB].reshape(QB, D), lambda t, s: kv1[h, s, 0, t * SUB:(t + 1) * SUB],
               vt, bias1, sref, lambda j, m: (m, None), finish)

    pass_on2(0)

    @pl.loop(0, HKV)
    def _(h):
        @pl.when(h < HKV - 1)
        def _():
            pass_on2(h + 1)

        rdma(7, h).wait_recv()
        vt[:, :S2 * T] = by_tile(kv2, h, S2).T

        def begin(j, m):
            m1 = ml[h, j, 0:1]
            m = jnp.maximum(m, m1)
            return m, jnp.exp2((m1 - m) * C)

        def finish(j, m, a, l, o):
            l = ml[h, j, 1:2] * a + l
            r = 1.0 / l
            o = oacc[h, j] * (a * r) + o * r
            ob[h, j * SUB:(j + 1) * SUB] = o.T.astype(BF).reshape(SUB, G, D)

        blocks(S2, lambda j: qb[h, j * SUB:(j + 1) * SUB].reshape(QB, D), lambda t, s: kv2[h, s, 0, t * SUB:(t + 1) * SUB],
               vt, bias2, sref, begin, finish)

    @pl.loop(0, HKV)
    def _(h):
        for kind in range(8):
            rdma(kind, h).wait_send()


def spread(ob, o_hbm, sem):
    copies = [pltpu.make_async_copy(ob.at[h], o_hbm.at[:, h * G:(h + 1) * G, :], sem.at[h]) for h in range(HKV)]
    for x in copies:
        x.start()
    for x in copies:
        x.wait()


def solution(mesh):
    spec = P(("dp", "cx", "cy", "cz"))

    def local(q, k, v):
        hbm = pl.BlockSpec(memory_space=pltpu.HBM)
        vmem = pl.BlockSpec(memory_space=pltpu.VMEM)
        heads = pl.pallas_call(
            kernel,
            out_shape=pltpu.VMEM((HKV, T, G, D), BF),
            in_specs=[hbm] * 3,
            out_specs=vmem,
            scratch_shapes=[
                pltpu.VMEM((HKV, T, G, D), BF),
                pltpu.VMEM((2, T, HKV, D), BF),
                pltpu.VMEM((T * HKV, D), F32),
                pltpu.VMEM((HKV, S1, 2, T, D), BF),
                pltpu.VMEM((HKV, S2, 2, T, D), BF),
                pltpu.VMEM((D, S1 * T), BF),
                pltpu.VMEM((2, S1 * T, QB), F32),
                pltpu.VMEM((S1 * SUB, QB), F32),
                pltpu.VMEM((S2 * SUB, QB), F32),
                pltpu.VMEM((HKV, NB, D, QB), F32),
                pltpu.VMEM((HKV, NB, 8, QB), F32),
                pltpu.SemaphoreType.DMA((2,)),
                pltpu.SemaphoreType.DMA((HKV,)),
                pltpu.SemaphoreType.DMA((8, HKV)),
                pltpu.SemaphoreType.DMA((8, HKV)),
            ],
            compiler_params=pltpu.CompilerParams(
                vmem_limit_bytes=48 << 20, collective_id=0, has_side_effects=True),
        )(q, k, v)
        return pl.pallas_call(
            spread,
            out_shape=jax.ShapeDtypeStruct(q.shape, q.dtype),
            in_specs=[vmem],
            out_specs=hbm,
            scratch_shapes=[pltpu.SemaphoreType.DMA((HKV,))],
            compiler_params=pltpu.CompilerParams(vmem_limit_bytes=1 << 20),
        )(heads)

    return jax.shard_map(local, mesh=mesh, in_specs=(spec, spec, spec), out_specs=spec, check_vma=False)
```

```python
import jax
import jax.numpy as jnp
from jax import lax
from jax.experimental import pallas as pl
from jax.experimental.pallas import tpu as pltpu
from jax.sharding import PartitionSpec as P

T = 256
HKV = 8
G = 8
D = 128
NB = 8
SUB = T // NB
QB = SUB * G
S1 = 6
S2 = 2
C = (D ** -0.5) * 1.4426950408889634
NT = (((1,), (1,)), ((), ()))
ORDER = (0, 2, 4, 6, 7, 5, 3, 1)
BF = jnp.bfloat16
F32 = jnp.float32


def chunks(n):
    return [(r, min(r + 256, n)) for r in range(0, n, 256)]


def by_tile(kv, h, nslot):
    return jnp.concatenate([kv[h, s, 1, t * SUB:(t + 1) * SUB] for t in range(NB) for s in range(nslot)], axis=0)


def fold(f, x):
    return f(x.reshape(-1, 8, x.shape[-1]), axis=0)


def blocks(nslot, q_of, k_of, vt, bias, sref, begin, finish):
    rows = nslot * SUB
    st = {}

    def scores(j, c):
        r0, r1 = c
        parts = [k_of(*divmod(u, nslot)) for u in range(r0 // SUB, r1 // SUB)]
        s = lax.dot_general(jnp.concatenate(parts, axis=0), q_of(j), NT, preferred_element_type=F32)
        lo = max(r0, j * rows)
        if lo < r1:
            d = s[lo - r0:] + bias[lo - j * rows:r1 - j * rows]
            s = d if lo == r0 else jnp.concatenate([s[:lo - r0], d], axis=0)
        sref[ORDER.index(j) % 2, r0:r1] = s
        m = fold(jnp.max, s)
        st[j] = jnp.maximum(st[j], m) if j in st else m

    def values(j, c, m, acc):
        r0, r1 = c
        p = jnp.exp2((sref[ORDER.index(j) % 2, r0:r1] - m) * C)
        l = fold(jnp.sum, p)
        o = jnp.dot(vt[:, r0:r1], p.astype(BF), preferred_element_type=F32)
        return (acc[0] + l, acc[1] + o) if acc else (l, o)

    for c in chunks((ORDER[0] + 1) * rows):
        scores(ORDER[0], c)
    for i, j in enumerate(ORDER):
        m, a = begin(j, jnp.max(st[j], axis=0, keepdims=True))
        acc = None
        mine = chunks((j + 1) * rows)
        later = chunks((ORDER[i + 1] + 1) * rows) if i + 1 < NB else []
        done = 0
        for t, c in enumerate(mine):
            upto = len(later) * (t + 1) // len(mine)
            for u in range(done, upto):
                scores(ORDER[i + 1], later[u])
            done = upto
            acc = values(j, c, m, acc)
        finish(j, m, a, jnp.sum(acc[0], axis=0, keepdims=True), acc[1])


def diagonal(h, out, qb, kv2, bias2, oacc, ml, vt, sref):
    vt[:, :S2 * T] = by_tile(kv2, h, S2).T

    def begin(j, m):
        m1 = ml[h, j, 0:1]
        m = jnp.maximum(m, m1)
        return m, jnp.exp2((m1 - m) * C)

    def finish(j, m, a, l, o):
        l = ml[h, j, 1:2] * a + l
        r = 1.0 / l
        o = oacc[h, j] * (a * r) + o * r
        out[j * SUB:(j + 1) * SUB] = o.T.astype(BF).reshape(SUB, G, D)

    blocks(S2, lambda j: qb[h, j * SUB:(j + 1) * SUB].reshape(QB, D),
           lambda t, s: kv2[h, s, 0, t * SUB:(t + 1) * SUB], vt, bias2, sref, begin, finish)


def kernel(q_hbm, k_hbm, v_hbm, ob, qb, kv2, bias2, oacc, ml, raw, wide, kv1, vt, sref, bias1,
           lsem, qsem, ssem, rsem):
    cx, cy, cz = lax.axis_index("cx"), lax.axis_index("cy"), lax.axis_index("cz")
    me = (cx * 2 + cy) * 2 + cz
    nx = {"cy": 1 - cy}
    ny = {"cx": 1 - cx}
    sib = {"cz": 1 - cz}

    barrier = pltpu.get_barrier_semaphore()
    for dev in (nx, ny, sib):
        pl.semaphore_signal(barrier, inc=1, device_id=dev, device_id_type=pl.DeviceIdType.MESH)

    loads = [pltpu.make_async_copy(x, raw.at[i], lsem.at[i]) for i, x in enumerate((k_hbm, v_hbm))]
    for x in loads:
        x.start()

    def qload(h):
        return pltpu.make_async_copy(q_hbm.at[:, pl.ds(pl.multiple_of(h * G, G), G), :], qb.at[h], qsem.at[h])

    @pl.loop(0, HKV)
    def _(h):
        qload(h).start()

    def rdma(kind, h):
        src, dst, dev = (
            (kv1.at[h, 0], kv1.at[h, 2], nx),
            (kv1.at[h, 0], kv1.at[h, 4], ny),
            (kv1.at[h, 0], kv1.at[h, 1], sib),
            (kv1.at[h, 2], kv1.at[h, 3], sib),
            (kv1.at[h, 4], kv1.at[h, 5], sib),
            (kv1.at[h, 2, 0], kv2.at[h, 0, 0], ny),
            (kv1.at[h, 4, 1], kv2.at[h, 0, 1], nx),
            (kv2.at[h, 0], kv2.at[h, 1], sib),
        )[kind]
        return pltpu.make_async_remote_copy(src, dst, ssem.at[kind, h], rsem.at[kind, h], dev,
                                            pl.DeviceIdType.MESH)

    def mask(nslot, base, ref):
        r = lax.broadcasted_iota(jnp.int32, (nslot * SUB, QB), 0)
        c = lax.broadcasted_iota(jnp.int32, (nslot * SUB, QB), 1)
        kpos = (r % SUB) * 8 + (me ^ (r // SUB + base))
        qpos = (c // G) * 8 + me
        ref[...] = jnp.where(kpos <= qpos, 0.0, -1e30)

    for i in range(2):
        loads[i].wait()
        wide[i] = raw[i].astype(F32).reshape(T * HKV, D)

    def send(h):
        for kind in range(3):
            rdma(kind, h).start()

    for h in range(HKV):
        for i in range(2):
            kv1[h, 0, i] = wide[i, pl.ds(h, T, stride=HKV), :].astype(BF)
        if h == 1:
            pl.semaphore_wait(barrier, 3)
        if h:
            send(h - 1)

    mask(S1, 0, bias1)
    mask(S2, S1, bias2)
    send(HKV - 1)

    def pass_on(h):
        rdma(0, h).wait_recv()
        rdma(1, h).wait_recv()
        for kind in (3, 4, 5, 6):
            rdma(kind, h).start()

    def pass_on2(h):
        rdma(5, h).wait_recv()
        rdma(6, h).wait_recv()
        rdma(7, h).start()

    pass_on(0)

    @pl.loop(0, HKV)
    def _(h):
        @pl.when(h < HKV - 1)
        def _():
            pass_on(h + 1)

        qload(h).wait()
        for kind in (2, 3, 4):
            rdma(kind, h).wait_recv()
        vt[...] = by_tile(kv1, h, S1).T

        def finish(j, m, a, l, o):
            oacc[h, j] = o
            ml[h, j, 0:1] = m
            ml[h, j, 1:2] = l

        blocks(S1, lambda j: qb[h, j * SUB:(j + 1) * SUB].reshape(QB, D), lambda t, s: kv1[h, s, 0, t * SUB:(t + 1) * SUB],
               vt, bias1, sref, lambda j, m: (m, None), finish)

    pass_on2(0)

    @pl.loop(0, HKV - 1)
    def _(h):
        pass_on2(h + 1)
        rdma(7, h).wait_recv()
        diagonal(h, ob.at[h], qb, kv2, bias2, oacc, ml, vt, sref)

    rdma(7, HKV - 1).wait_recv()

    @pl.loop(0, HKV)
    def _(h):
        for kind in range(8):
            rdma(kind, h).wait_send()


def spread(ob, qb, kv2, bias2, oacc, ml, o_hbm, last, vt, sref, sem):
    copies = [pltpu.make_async_copy(ob.at[h] if h < HKV - 1 else last, o_hbm.at[:, h * G:(h + 1) * G, :], sem.at[h])
              for h in range(HKV)]
    for x in copies[:-1]:
        x.start()
    diagonal(HKV - 1, last, qb, kv2, bias2, oacc, ml, vt, sref)
    copies[-1].start()
    for x in copies:
        x.wait()


def solution(mesh):
    spec = P(("dp", "cx", "cy", "cz"))

    def local(q, k, v):
        hbm = pl.BlockSpec(memory_space=pltpu.HBM)
        vmem = pl.BlockSpec(memory_space=pltpu.VMEM)
        parts = pl.pallas_call(
            kernel,
            out_shape=[
                pltpu.VMEM((HKV - 1, T, G, D), BF),
                pltpu.VMEM((HKV, T, G, D), BF),
                pltpu.VMEM((HKV, S2, 2, T, D), BF),
                pltpu.VMEM((S2 * SUB, QB), F32),
                pltpu.VMEM((HKV, NB, D, QB), F32),
                pltpu.VMEM((HKV, NB, 8, QB), F32),
            ],
            in_specs=[hbm] * 3,
            out_specs=[vmem] * 6,
            scratch_shapes=[
                pltpu.VMEM((2, T, HKV, D), BF),
                pltpu.VMEM((2, T * HKV, D), F32),
                pltpu.VMEM((HKV, S1, 2, T, D), BF),
                pltpu.VMEM((D, S1 * T), BF),
                pltpu.VMEM((2, S1 * T, QB), F32),
                pltpu.VMEM((S1 * SUB, QB), F32),
                pltpu.SemaphoreType.DMA((2,)),
                pltpu.SemaphoreType.DMA((HKV,)),
                pltpu.SemaphoreType.DMA((8, HKV)),
                pltpu.SemaphoreType.DMA((8, HKV)),
            ],
            compiler_params=pltpu.CompilerParams(
                vmem_limit_bytes=36 << 20, collective_id=0, has_side_effects=True),
        )(*(pltpu.with_memory_space_constraint(x, pltpu.HBM) for x in (q, k, v)))
        return pl.pallas_call(
            spread,
            out_shape=jax.ShapeDtypeStruct(q.shape, q.dtype),
            in_specs=[vmem] * 6,
            out_specs=hbm,
            scratch_shapes=[
                pltpu.VMEM((T, G, D), BF),
                pltpu.VMEM((D, S2 * T), BF),
                pltpu.VMEM((2, S2 * T, QB), F32),
                pltpu.SemaphoreType.DMA((HKV,)),
            ],
            compiler_params=pltpu.CompilerParams(vmem_limit_bytes=8 << 20),
        )(*parts)

    return jax.shard_map(local, mesh=mesh, in_specs=(spec, spec, spec), out_specs=spec, check_vma=False)
```

```python
import jax
import jax.numpy as jnp
from jax import lax
from jax.experimental import pallas as pl
from jax.experimental.pallas import tpu as pltpu
from jax.sharding import PartitionSpec as P

T = 256
HKV = 8
G = 8
D = 128
NB = 8
SUB = T // NB
QB = SUB * G
S1 = 6
S2 = 2
C = (D ** -0.5) * 1.4426950408889634
NT = (((1,), (1,)), ((), ()))
ORDER = (0, 2, 4, 6, 7, 5, 3, 1)
BF = jnp.bfloat16
F32 = jnp.float32


def chunks(n):
    return [(r, min(r + 256, n)) for r in range(0, n, 256)]


def by_tile(kv, h, nslot):
    return jnp.concatenate([kv[h, s, 1, t * SUB:(t + 1) * SUB] for t in range(NB) for s in range(nslot)], axis=0)


def fold(f, x):
    return f(x.reshape(-1, 8, x.shape[-1]), axis=0)


def blocks(nslot, q_of, k_of, vt, bias, sref, begin, finish):
    rows = nslot * SUB
    st = {}

    def scores(j, c):
        r0, r1 = c
        parts = [k_of(*divmod(u, nslot)) for u in range(r0 // SUB, r1 // SUB)]
        s = lax.dot_general(jnp.concatenate(parts, axis=0), q_of(j), NT, preferred_element_type=F32)
        lo = max(r0, j * rows)
        if lo < r1:
            d = s[lo - r0:] + bias[lo - j * rows:r1 - j * rows]
            s = d if lo == r0 else jnp.concatenate([s[:lo - r0], d], axis=0)
        sref[ORDER.index(j) % 2, r0:r1] = s
        m = fold(jnp.max, s)
        st[j] = jnp.maximum(st[j], m) if j in st else m

    def values(j, c, m, acc):
        r0, r1 = c
        p = jnp.exp2((sref[ORDER.index(j) % 2, r0:r1] - m) * C)
        l = fold(jnp.sum, p)
        o = jnp.dot(vt[:, r0:r1], p.astype(BF), preferred_element_type=F32)
        return (acc[0] + l, acc[1] + o) if acc else (l, o)

    for c in chunks((ORDER[0] + 1) * rows):
        scores(ORDER[0], c)
    for i, j in enumerate(ORDER):
        m, a = begin(j, jnp.max(st[j], axis=0, keepdims=True))
        acc = None
        mine = chunks((j + 1) * rows)
        later = chunks((ORDER[i + 1] + 1) * rows) if i + 1 < NB else []
        done = 0
        for t, c in enumerate(mine):
            upto = len(later) * (t + 1) // len(mine)
            for u in range(done, upto):
                scores(ORDER[i + 1], later[u])
            done = upto
            acc = values(j, c, m, acc)
        finish(j, m, a, jnp.sum(acc[0], axis=0, keepdims=True), acc[1])


def diagonal(h, out, qb, kv2, bias2, oacc, ml, vt, sref, done=None):
    vt[:, :S2 * T] = by_tile(kv2, h, S2).T

    def begin(j, m):
        m1 = ml[h, j, 0:1]
        m = jnp.maximum(m, m1)
        return m, jnp.exp2((m1 - m) * C)

    def finish(j, m, a, l, o):
        if done:
            done(j)
        l = ml[h, j, 1:2] * a + l
        r = 1.0 / l
        o = oacc[h, j] * (a * r) + o * r
        out[j * SUB:(j + 1) * SUB] = o.T.astype(BF).reshape(SUB, G, D)

    blocks(S2, lambda j: qb[h, j * SUB:(j + 1) * SUB].reshape(QB, D),
           lambda t, s: kv2[h, s, 0, t * SUB:(t + 1) * SUB], vt, bias2, sref, begin, finish)


def kernel(q_hbm, k_hbm, v_hbm, ob, qb, kv2, bias2, oacc, ml, raw, wide, kv1, vt, sref, bias1,
           lsem, qsem, ssem, rsem):
    cx, cy, cz = lax.axis_index("cx"), lax.axis_index("cy"), lax.axis_index("cz")
    me = (cx * 2 + cy) * 2 + cz
    nx = {"cy": 1 - cy}
    ny = {"cx": 1 - cx}
    sib = {"cz": 1 - cz}

    barrier = pltpu.get_barrier_semaphore()
    for dev in (nx, ny, sib):
        pl.semaphore_signal(barrier, inc=1, device_id=dev, device_id_type=pl.DeviceIdType.MESH)

    loads = [pltpu.make_async_copy(x, raw.at[i], lsem.at[i]) for i, x in enumerate((k_hbm, v_hbm))]
    for x in loads:
        x.start()

    def qload(h):
        return pltpu.make_async_copy(q_hbm.at[:, pl.ds(pl.multiple_of(h * G, G), G), :], qb.at[h], qsem.at[h])

    def rdma(kind, h):
        src, dst, dev = (
            (kv1.at[h, 0], kv1.at[h, 2], nx),
            (kv1.at[h, 0], kv1.at[h, 4], ny),
            (kv1.at[h, 0], kv1.at[h, 1], sib),
            (kv1.at[h, 2], kv1.at[h, 3], sib),
            (kv1.at[h, 4], kv1.at[h, 5], sib),
            (kv1.at[h, 2, 0], kv2.at[h, 0, 0], ny),
            (kv1.at[h, 4, 1], kv2.at[h, 0, 1], nx),
            (kv2.at[h, 0], kv2.at[h, 1], sib),
        )[kind]
        return pltpu.make_async_remote_copy(src, dst, ssem.at[kind, h], rsem.at[kind, h], dev,
                                            pl.DeviceIdType.MESH)

    def mask(nslot, base, ref):
        r = lax.broadcasted_iota(jnp.int32, (nslot * SUB, QB), 0)
        c = lax.broadcasted_iota(jnp.int32, (nslot * SUB, QB), 1)
        kpos = (r % SUB) * 8 + (me ^ (r // SUB + base))
        qpos = (c // G) * 8 + me
        ref[...] = jnp.where(kpos <= qpos, 0.0, -1e30)

    for i in range(2):
        loads[i].wait()
        wide[i] = raw[i].astype(F32).reshape(T * HKV, D)

    def send(h):
        for kind in range(3):
            rdma(kind, h).start()

    for h in range(HKV):
        for i in range(2):
            kv1[h, 0, i] = wide[i, pl.ds(h, T, stride=HKV), :].astype(BF)
        if h == 1:
            pl.semaphore_wait(barrier, 3)
        if h:
            send(h - 1)

    mask(S2, S1, bias2)
    send(HKV - 1)

    @pl.loop(0, HKV)
    def _(h):
        qload(h).start()

    mask(S1, 0, bias1)

    def pass_on(h):
        rdma(0, h).wait_recv()
        rdma(1, h).wait_recv()
        for kind in (3, 4, 5, 6):
            rdma(kind, h).start()

    def pass_on2(h):
        rdma(5, h).wait_recv()
        rdma(6, h).wait_recv()
        rdma(7, h).start()

    pass_on(0)

    @pl.loop(0, HKV)
    def _(h):
        @pl.when(h < HKV - 1)
        def _():
            pass_on(h + 1)

        qload(h).wait()
        for kind in (2, 3, 4):
            rdma(kind, h).wait_recv()
        vt[...] = by_tile(kv1, h, S1).T

        def finish(j, m, a, l, o):
            oacc[h, j] = o
            ml[h, j, 0:1] = m
            ml[h, j, 1:2] = l

        blocks(S1, lambda j: qb[h, j * SUB:(j + 1) * SUB].reshape(QB, D), lambda t, s: kv1[h, s, 0, t * SUB:(t + 1) * SUB],
               vt, bias1, sref, lambda j, m: (m, None), finish)

    pass_on2(0)

    @pl.loop(0, HKV - 1)
    def _(h):
        pass_on2(h + 1)
        rdma(7, h).wait_recv()
        diagonal(h, ob.at[h], qb, kv2, bias2, oacc, ml, vt, sref)

    rdma(7, HKV - 1).wait_recv()

    @pl.loop(0, HKV)
    def _(h):
        for kind in range(8):
            rdma(kind, h).wait_send()


def spread(ob, qb, kv2, bias2, oacc, ml, o_hbm, last, vt, sref, sem):
    copies = [pltpu.make_async_copy(ob.at[h], o_hbm.at[:, h * G:(h + 1) * G, :], sem.at[h]) for h in range(HKV - 1)]
    copies += [pltpu.make_async_copy(last.at[j * SUB:(j + 1) * SUB],
                                     o_hbm.at[j * SUB:(j + 1) * SUB, (HKV - 1) * G:, :], sem.at[HKV - 1 + j])
               for j in range(NB)]
    for x in copies[:HKV - 1]:
        x.start()

    def done(j):
        i = ORDER.index(j)
        if i:
            copies[HKV - 1 + ORDER[i - 1]].start()

    diagonal(HKV - 1, last, qb, kv2, bias2, oacc, ml, vt, sref, done)
    copies[HKV - 1 + ORDER[-1]].start()
    for x in copies:
        x.wait()


def solution(mesh):
    spec = P(("dp", "cx", "cy", "cz"))

    def local(q, k, v):
        hbm = pl.BlockSpec(memory_space=pltpu.HBM)
        vmem = pl.BlockSpec(memory_space=pltpu.VMEM)
        parts = pl.pallas_call(
            kernel,
            out_shape=[
                pltpu.VMEM((HKV - 1, T, G, D), BF),
                pltpu.VMEM((HKV, T, G, D), BF),
                pltpu.VMEM((HKV, S2, 2, T, D), BF),
                pltpu.VMEM((S2 * SUB, QB), F32),
                pltpu.VMEM((HKV, NB, D, QB), F32),
                pltpu.VMEM((HKV, NB, 8, QB), F32),
            ],
            in_specs=[hbm] * 3,
            out_specs=[vmem] * 6,
            scratch_shapes=[
                pltpu.VMEM((2, T, HKV, D), BF),
                pltpu.VMEM((2, T * HKV, D), F32),
                pltpu.VMEM((HKV, S1, 2, T, D), BF),
                pltpu.VMEM((D, S1 * T), BF),
                pltpu.VMEM((2, S1 * T, QB), F32),
                pltpu.VMEM((S1 * SUB, QB), F32),
                pltpu.SemaphoreType.DMA((2,)),
                pltpu.SemaphoreType.DMA((HKV,)),
                pltpu.SemaphoreType.DMA((8, HKV)),
                pltpu.SemaphoreType.DMA((8, HKV)),
            ],
            compiler_params=pltpu.CompilerParams(
                vmem_limit_bytes=36 << 20, collective_id=0, has_side_effects=True),
        )(*(pltpu.with_memory_space_constraint(x, pltpu.HBM) for x in (q, k, v)))
        return pl.pallas_call(
            spread,
            out_shape=jax.ShapeDtypeStruct(q.shape, q.dtype),
            in_specs=[vmem] * 6,
            out_specs=hbm,
            scratch_shapes=[
                pltpu.VMEM((T, G, D), BF),
                pltpu.VMEM((D, S2 * T), BF),
                pltpu.VMEM((2, S2 * T, QB), F32),
                pltpu.SemaphoreType.DMA((HKV - 1 + NB,)),
            ],
            compiler_params=pltpu.CompilerParams(vmem_limit_bytes=8 << 20),
        )(*parts)

    return jax.shard_map(local, mesh=mesh, in_specs=(spec, spec, spec), out_specs=spec, check_vma=False)
```

```python
import jax
import jax.numpy as jnp
from jax import lax
from jax.experimental import pallas as pl
from jax.experimental.pallas import tpu as pltpu
from jax.sharding import PartitionSpec as P

T = 256
HKV = 8
G = 8
D = 128
NB = 8
SUB = T // NB
QB = SUB * G
S1 = 6
S2 = 2
C = (D ** -0.5) * 1.4426950408889634
NT = (((1,), (1,)), ((), ()))
ORDER = (0, 2, 4, 6, 7, 5, 3, 1)
BF = jnp.bfloat16
F32 = jnp.float32


def chunks(n):
    return [(r, min(r + 256, n)) for r in range(0, n, 256)]


def by_tile(kv, h, s0, ns):
    return jnp.concatenate([kv[h, s, 1, t * SUB:(t + 1) * SUB] for t in range(NB) for s in range(s0, s0 + ns)], axis=0)


def fold(f, x):
    return f(x.reshape(-1, 8, x.shape[-1]), axis=0)


def blocks(nslot, q_of, k_of, vt, bias, sref, begin, finish):
    rows = nslot * SUB
    st = {}

    def scores(j, c):
        r0, r1 = c
        parts = [k_of(*divmod(u, nslot)) for u in range(r0 // SUB, r1 // SUB)]
        s = lax.dot_general(jnp.concatenate(parts, axis=0), q_of(j), NT, preferred_element_type=F32)
        lo = max(r0, j * rows)
        if lo < r1:
            d = s[lo - r0:] + bias[lo - j * rows:r1 - j * rows]
            s = d if lo == r0 else jnp.concatenate([s[:lo - r0], d], axis=0)
        sref[ORDER.index(j) % 2, r0:r1] = s
        m = fold(jnp.max, s)
        st[j] = jnp.maximum(st[j], m) if j in st else m

    def values(j, c, m, acc):
        r0, r1 = c
        p = jnp.exp2((sref[ORDER.index(j) % 2, r0:r1] - m) * C)
        l = fold(jnp.sum, p)
        o = jnp.dot(vt[:, r0:r1], p.astype(BF), preferred_element_type=F32)
        return (acc[0] + l, acc[1] + o) if acc else (l, o)

    for c in chunks((ORDER[0] + 1) * rows):
        scores(ORDER[0], c)
    for i, j in enumerate(ORDER):
        m, a = begin(j, jnp.max(st[j], axis=0, keepdims=True))
        acc = None
        mine = chunks((j + 1) * rows)
        later = chunks((ORDER[i + 1] + 1) * rows) if i + 1 < NB else []
        done = 0
        for t, c in enumerate(mine):
            upto = len(later) * (t + 1) // len(mine)
            for u in range(done, upto):
                scores(ORDER[i + 1], later[u])
            done = upto
            acc = values(j, c, m, acc)
        finish(j, m, a, jnp.sum(acc[0], axis=0, keepdims=True), acc[1])


def attend(h, kv, s0, ns, bias, qb, oacc, ml, vt, sref, first=False, out=None):
    vt[:, :ns * T] = by_tile(kv, h, s0, ns).T

    def begin(j, m):
        if first:
            return m, None
        m1 = ml[h, j, 0:1]
        m = jnp.maximum(m, m1)
        return m, jnp.exp2((m1 - m) * C)

    def finish(j, m, a, l, o):
        if not first:
            l = ml[h, j, 1:2] * a + l
        if out is None:
            oacc[h, j] = o if first else oacc[h, j] * a + o
            ml[h, j, 0:1] = m
            ml[h, j, 1:2] = l
            return
        r = 1.0 / l
        o = oacc[h, j] * (a * r) + o * r
        out[j * SUB:(j + 1) * SUB] = o.T.astype(BF).reshape(SUB, G, D)

    blocks(ns, lambda j: qb[h, j * SUB:(j + 1) * SUB].reshape(QB, D),
           lambda t, s: kv[h, s0 + s, 0, t * SUB:(t + 1) * SUB], vt, bias, sref, begin, finish)


def kernel(q_hbm, k_hbm, v_hbm, ob, qb, kv2, bias2, oacc, ml, raw, wide, kv1, vt, sref, bias0, bias1,
           lsem, qsem, ssem, rsem):
    cx, cy, cz = lax.axis_index("cx"), lax.axis_index("cy"), lax.axis_index("cz")
    me = (cx * 2 + cy) * 2 + cz
    nx = {"cy": 1 - cy}
    ny = {"cx": 1 - cx}
    sib = {"cz": 1 - cz}

    barrier = pltpu.get_barrier_semaphore()
    for dev in (nx, ny, sib):
        pl.semaphore_signal(barrier, inc=1, device_id=dev, device_id_type=pl.DeviceIdType.MESH)

    loads = [pltpu.make_async_copy(x, raw.at[i], lsem.at[i]) for i, x in enumerate((k_hbm, v_hbm))]
    for x in loads:
        x.start()

    def qload(h):
        return pltpu.make_async_copy(q_hbm.at[:, pl.ds(pl.multiple_of(h * G, G), G), :], qb.at[h], qsem.at[h])

    def rdma(kind, h):
        src, dst, dev = (
            (kv1.at[h, 0], kv1.at[h, 2], nx),
            (kv1.at[h, 0], kv1.at[h, 4], ny),
            (kv1.at[h, 0], kv1.at[h, 1], sib),
            (kv1.at[h, 2], kv1.at[h, 3], sib),
            (kv1.at[h, 4], kv1.at[h, 5], sib),
            (kv1.at[h, 2, 0], kv2.at[h, 0, 0], ny),
            (kv1.at[h, 4, 1], kv2.at[h, 0, 1], nx),
            (kv2.at[h, 0], kv2.at[h, 1], sib),
        )[kind]
        return pltpu.make_async_remote_copy(src, dst, ssem.at[kind, h], rsem.at[kind, h], dev,
                                            pl.DeviceIdType.MESH)

    def mask(nslot, base, ref):
        r = lax.broadcasted_iota(jnp.int32, (nslot * SUB, QB), 0)
        c = lax.broadcasted_iota(jnp.int32, (nslot * SUB, QB), 1)
        kpos = (r % SUB) * 8 + (me ^ (r // SUB + base))
        qpos = (c // G) * 8 + me
        ref[...] = jnp.where(kpos <= qpos, 0.0, -1e30)

    for i in range(2):
        loads[i].wait()
        wide[i] = raw[i].astype(F32).reshape(T * HKV, D)

    def send(h):
        for kind in range(3):
            rdma(kind, h).start()

    for h in range(HKV):
        for i in range(2):
            kv1[h, 0, i] = wide[i, pl.ds(h, T, stride=HKV), :].astype(BF)
        if h == 1:
            pl.semaphore_wait(barrier, 3)
        if h:
            send(h - 1)

    mask(2, 0, bias0)
    send(HKV - 1)

    @pl.loop(0, HKV)
    def _(h):
        qload(h).start()

    mask(4, 2, bias1)
    mask(2, 6, bias2)

    def pass_on(h):
        rdma(0, h).wait_recv()
        rdma(1, h).wait_recv()
        for kind in (3, 4, 5, 6):
            rdma(kind, h).start()

    def pass_on2(h):
        rdma(5, h).wait_recv()
        rdma(6, h).wait_recv()
        rdma(7, h).start()

    @pl.loop(0, HKV)
    def _(h):
        qload(h).wait()
        rdma(2, h).wait_recv()
        attend(h, kv1, 0, 2, bias0, qb, oacc, ml, vt, sref, first=True)

    pass_on(0)

    @pl.loop(0, HKV)
    def _(h):
        @pl.when(h < HKV - 1)
        def _():
            pass_on(h + 1)

        for kind in (3, 4):
            rdma(kind, h).wait_recv()
        attend(h, kv1, 2, 4, bias1, qb, oacc, ml, vt, sref)

    pass_on2(0)

    @pl.loop(0, HKV - 1)
    def _(h):
        pass_on2(h + 1)
        rdma(7, h).wait_recv()
        attend(h, kv2, 0, 2, bias2, qb, oacc, ml, vt, sref, out=ob.at[h])

    rdma(7, HKV - 1).wait_recv()

    @pl.loop(0, HKV)
    def _(h):
        for kind in range(8):
            rdma(kind, h).wait_send()


def spread(ob, qb, kv2, bias2, oacc, ml, o_hbm, last, vt, sref, sem):
    copies = [pltpu.make_async_copy(ob.at[h] if h < HKV - 1 else last, o_hbm.at[:, h * G:(h + 1) * G, :], sem.at[h])
              for h in range(HKV)]
    for x in copies[:-1]:
        x.start()
    attend(HKV - 1, kv2, 0, 2, bias2, qb, oacc, ml, vt, sref, out=last)
    copies[-1].start()
    for x in copies:
        x.wait()


def solution(mesh):
    spec = P(("dp", "cx", "cy", "cz"))

    def local(q, k, v):
        hbm = pl.BlockSpec(memory_space=pltpu.HBM)
        vmem = pl.BlockSpec(memory_space=pltpu.VMEM)
        parts = pl.pallas_call(
            kernel,
            out_shape=[
                pltpu.VMEM((HKV - 1, T, G, D), BF),
                pltpu.VMEM((HKV, T, G, D), BF),
                pltpu.VMEM((HKV, S2, 2, T, D), BF),
                pltpu.VMEM((S2 * SUB, QB), F32),
                pltpu.VMEM((HKV, NB, D, QB), F32),
                pltpu.VMEM((HKV, NB, 8, QB), F32),
            ],
            in_specs=[hbm] * 3,
            out_specs=[vmem] * 6,
            scratch_shapes=[
                pltpu.VMEM((2, T, HKV, D), BF),
                pltpu.VMEM((2, T * HKV, D), F32),
                pltpu.VMEM((HKV, S1, 2, T, D), BF),
                pltpu.VMEM((D, 4 * T), BF),
                pltpu.VMEM((2, 4 * T, QB), F32),
                pltpu.VMEM((2 * SUB, QB), F32),
                pltpu.VMEM((4 * SUB, QB), F32),
                pltpu.SemaphoreType.DMA((2,)),
                pltpu.SemaphoreType.DMA((HKV,)),
                pltpu.SemaphoreType.DMA((8, HKV)),
                pltpu.SemaphoreType.DMA((8, HKV)),
            ],
            compiler_params=pltpu.CompilerParams(
                vmem_limit_bytes=36 << 20, collective_id=0, has_side_effects=True),
        )(*(pltpu.with_memory_space_constraint(x, pltpu.HBM) for x in (q, k, v)))
        return pl.pallas_call(
            spread,
            out_shape=jax.ShapeDtypeStruct(q.shape, q.dtype),
            in_specs=[vmem] * 6,
            out_specs=hbm,
            scratch_shapes=[
                pltpu.VMEM((T, G, D), BF),
                pltpu.VMEM((D, S2 * T), BF),
                pltpu.VMEM((2, S2 * T, QB), F32),
                pltpu.SemaphoreType.DMA((HKV,)),
            ],
            compiler_params=pltpu.CompilerParams(vmem_limit_bytes=8 << 20),
        )(*parts)

    return jax.shard_map(local, mesh=mesh, in_specs=(spec, spec, spec), out_specs=spec, check_vma=False)
```

```python
import jax
import jax.numpy as jnp
from jax import lax
from jax.experimental import pallas as pl
from jax.experimental.pallas import tpu as pltpu
from jax.sharding import PartitionSpec as P

T = 256
HKV = 8
G = 8
D = 128
NB = 8
SUB = T // NB
QB = SUB * G
S1 = 6
S2 = 2
C = (D ** -0.5) * 1.4426950408889634
ORDER = (0, 2, 4, 6, 7, 5, 3, 1)
AHEAD = 3
U0, U1, U2 = 2,2,1
BF = jnp.bfloat16
F32 = jnp.float32
NT = (((1,), (1,)), ((), ()))


def chunks(n):
    return [(r, min(r + 256, n)) for r in range(0, n, 256)]


def by_tile(kv, h, s0, ns):
    return jnp.concatenate([kv[h, s, 1, t * SUB:(t + 1) * SUB] for t in range(NB) for s in range(s0, s0 + ns)], axis=0)


def fold(f, x):
    return f(x.reshape(-1, 8, x.shape[-1]), axis=0)


def attend(heads, kv, s0, ns, bias, qt, oacc, ml, vt, sref, arrive=None, first=False, out=None):
    rows = ns * SUB
    items = [(u, j) for u in range(len(heads)) for j in ORDER]
    tops = {}

    def scores(i, c):
        u, j = items[i]
        h = heads[u]
        r0, r1 = c
        if j == ORDER[0] and r0 == 0:
            if arrive:
                arrive(u)
            vt[u, :, :ns * T] = by_tile(kv, h, s0, ns).T
        parts = [kv[h, s0 + x % ns, 0, x // ns * SUB:(x // ns + 1) * SUB] for x in range(r0 // SUB, r1 // SUB)]
        s = lax.dot_general(jnp.concatenate(parts, axis=0), qt[h, j * SUB:(j + 1) * SUB].reshape(QB, D), NT,
                            preferred_element_type=F32)
        lo = max(r0, j * rows)
        if lo < r1:
            d = s[lo - r0:] + bias[lo - j * rows:r1 - j * rows]
            s = d if lo == r0 else jnp.concatenate([s[:lo - r0], d], axis=0)
        sref[i % (AHEAD + 1), r0:r1] = s
        m = fold(jnp.max, s)
        tops[i] = jnp.maximum(tops[i], m) if i in tops else m

    def values(i, c, m, acc):
        u, j = items[i]
        r0, r1 = c
        p = jnp.exp2((sref[i % (AHEAD + 1), r0:r1] - m) * C)
        l = fold(jnp.sum, p)
        o = jnp.dot(vt[u, :, r0:r1], p.astype(BF), preferred_element_type=F32)
        return (acc[0] + l, acc[1] + o) if acc else (l, o)

    def finish(i, m, a, l, o):
        u, j = items[i]
        h = heads[u]
        if not first:
            l = ml[h, j, 1:2] * a + l
        if out is None:
            oacc[h, j] = o if first else oacc[h, j] * a + o
            ml[h, j, 0:1] = m
            ml[h, j, 1:2] = l
            return
        r = 1.0 / l
        o = oacc[h, j] * (a * r) + o * r
        out(u)[j * SUB:(j + 1) * SUB] = o.T.astype(BF).reshape(SUB, G, D)

    todo = [(i, c) for i, (u, j) in enumerate(items) for c in chunks((j + 1) * rows)]
    total = len(todo)
    sizes = [len(chunks((j + 1) * rows)) for u, j in items]
    at = 0
    while at < total and todo[at][0] < AHEAD:
        scores(*todo[at])
        at += 1
    for i, (u, j) in enumerate(items):
        top = jnp.max(tops[i], axis=0, keepdims=True)
        m, a = top, None
        if not first:
            m1 = ml[heads[u], j, 0:1]
            m = jnp.maximum(top, m1)
            a = jnp.exp2((m1 - m) * C)
        acc = None
        goal = sum(sizes[:i + AHEAD + 1])
        start = at
        mine = chunks((j + 1) * rows)
        for t, c in enumerate(mine):
            upto = start + (goal - start) * (t + 1) // len(mine)
            while at < upto:
                scores(*todo[at])
                at += 1
            acc = values(i, c, m, acc)
        finish(i, m, a, jnp.sum(acc[0], axis=0, keepdims=True), acc[1])


def kernel(q_hbm, k_hbm, v_hbm, ob, qt, kv2, bias2, oacc, ml, raw, wide, kv1, vt, sref, bias0, bias1,
           lsem, qsem, ssem, rsem):
    cx, cy, cz = lax.axis_index("cx"), lax.axis_index("cy"), lax.axis_index("cz")
    me = (cx * 2 + cy) * 2 + cz
    nx = {"cy": 1 - cy}
    ny = {"cx": 1 - cx}
    sib = {"cz": 1 - cz}

    barrier = pltpu.get_barrier_semaphore()
    for dev in (nx, ny, sib):
        pl.semaphore_signal(barrier, inc=1, device_id=dev, device_id_type=pl.DeviceIdType.MESH)

    loads = [pltpu.make_async_copy(x, raw.at[i], lsem.at[i]) for i, x in enumerate((k_hbm, v_hbm))]
    for x in loads:
        x.start()

    def qload(h):
        return pltpu.make_async_copy(q_hbm.at[:, pl.ds(pl.multiple_of(h * G, G), G), :], qt.at[h], qsem.at[h])

    def rdma(kind, h):
        src, dst, dev = (
            (kv1.at[h, 0], kv1.at[h, 2], nx),
            (kv1.at[h, 0], kv1.at[h, 4], ny),
            (kv1.at[h, 0], kv1.at[h, 1], sib),
            (kv1.at[h, 2], kv1.at[h, 3], sib),
            (kv1.at[h, 4], kv1.at[h, 5], sib),
            (kv1.at[h, 2, 0], kv2.at[h, 0, 0], ny),
            (kv1.at[h, 4, 1], kv2.at[h, 0, 1], nx),
            (kv2.at[h, 0], kv2.at[h, 1], sib),
        )[kind]
        return pltpu.make_async_remote_copy(src, dst, ssem.at[kind, h], rsem.at[kind, h], dev,
                                            pl.DeviceIdType.MESH)

    def mask(nslot, base, ref):
        r = lax.broadcasted_iota(jnp.int32, (nslot * SUB, QB), 0)
        c = lax.broadcasted_iota(jnp.int32, (nslot * SUB, QB), 1)
        kpos = (r % SUB) * 8 + (me ^ (r // SUB + base))
        qpos = (c // G) * 8 + me
        ref[...] = jnp.where(kpos <= qpos, 0.0, -1e30)

    for i in range(2):
        loads[i].wait()
        wide[i] = raw[i].astype(F32).reshape(T * HKV, D)

    def send(h):
        for kind in range(3):
            rdma(kind, h).start()

    for h in range(HKV):
        for i in range(2):
            kv1[h, 0, i] = wide[i, pl.ds(h, T, stride=HKV), :].astype(BF)
        if h == 1:
            pl.semaphore_wait(barrier, 3)
        if h:
            send(h - 1)

    mask(2, 0, bias0)
    send(HKV - 1)

    @pl.loop(0, HKV)
    def _(h):
        qload(h).start()

    mask(4, 2, bias1)
    mask(2, 6, bias2)

    def pass_on(h):
        rdma(0, h).wait_recv()
        rdma(1, h).wait_recv()
        for kind in (3, 4, 5, 6):
            rdma(kind, h).start()

    def pass_on2(h):
        rdma(5, h).wait_recv()
        rdma(6, h).wait_recv()
        rdma(7, h).start()

    @pl.loop(0, HKV // U0)
    def _(g):
        heads = [g * U0 + u for u in range(U0)]

        def arrive(u):
            h = heads[u]
            qload(h).wait()
            rdma(2, h).wait_recv()

        attend(heads, kv1, 0, 2, bias0, qt, oacc, ml, vt, sref, arrive, first=True)

    pass_on(0)

    @pl.loop(0, HKV // U1)
    def _(g):
        heads = [g * U1 + u for u in range(U1)]

        def arrive(u):
            h = heads[u]
            if u < U1 - 1:
                pass_on(h + 1)
            else:
                @pl.when(h < HKV - 1)
                def _():
                    pass_on(h + 1)

            rdma(3, h).wait_recv()
            rdma(4, h).wait_recv()

        attend(heads, kv1, 2, 4, bias1, qt, oacc, ml, vt, sref, arrive)

    pass_on2(0)

    @pl.loop(0, (HKV - 1) // U2)
    def _(g):
        heads = [g * U2 + u for u in range(U2)]

        def arrive(u):
            pass_on2(heads[u] + 1)
            rdma(7, heads[u]).wait_recv()

        attend(heads, kv2, 0, 2, bias2, qt, oacc, ml, vt, sref, arrive, out=lambda u: ob.at[heads[u]])

    rdma(7, HKV - 1).wait_recv()

    @pl.loop(0, HKV)
    def _(h):
        for kind in range(8):
            rdma(kind, h).wait_send()


def spread(ob, qt, kv2, bias2, oacc, ml, o_hbm, last, vt, sref, sem):
    copies = [pltpu.make_async_copy(ob.at[h] if h < HKV - 1 else last, o_hbm.at[:, h * G:(h + 1) * G, :], sem.at[h])
              for h in range(HKV)]
    for x in copies[:-1]:
        x.start()
    attend([HKV - 1], kv2, 0, 2, bias2, qt, oacc, ml, vt, sref, out=lambda u: last)
    copies[-1].start()
    for x in copies:
        x.wait()


def solution(mesh):
    spec = P(("dp", "cx", "cy", "cz"))

    def local(q, k, v):
        hbm = pl.BlockSpec(memory_space=pltpu.HBM)
        vmem = pl.BlockSpec(memory_space=pltpu.VMEM)
        parts = pl.pallas_call(
            kernel,
            out_shape=[
                pltpu.VMEM((HKV - 1, T, G, D), BF),
                pltpu.VMEM((HKV, T, G, D), BF),
                pltpu.VMEM((HKV, S2, 2, T, D), BF),
                pltpu.VMEM((S2 * SUB, QB), F32),
                pltpu.VMEM((HKV, NB, D, QB), F32),
                pltpu.VMEM((HKV, NB, 8, QB), F32),
            ],
            in_specs=[hbm] * 3,
            out_specs=[vmem] * 6,
            scratch_shapes=[
                pltpu.VMEM((2, T, HKV, D), BF),
                pltpu.VMEM((2, T * HKV, D), F32),
                pltpu.VMEM((HKV, S1, 2, T, D), BF),
                pltpu.VMEM((max(U0, U1, U2), D, 4 * T), BF),
                pltpu.VMEM((AHEAD + 1, 4 * T, QB), F32),
                pltpu.VMEM((2 * SUB, QB), F32),
                pltpu.VMEM((4 * SUB, QB), F32),
                pltpu.SemaphoreType.DMA((2,)),
                pltpu.SemaphoreType.DMA((HKV,)),
                pltpu.SemaphoreType.DMA((8, HKV)),
                pltpu.SemaphoreType.DMA((8, HKV)),
            ],
            compiler_params=pltpu.CompilerParams(
                vmem_limit_bytes=36 << 20, collective_id=0, has_side_effects=True),
        )(*(pltpu.with_memory_space_constraint(x, pltpu.HBM) for x in (q, k, v)))
        return pl.pallas_call(
            spread,
            out_shape=jax.ShapeDtypeStruct(q.shape, q.dtype),
            in_specs=[vmem] * 6,
            out_specs=hbm,
            scratch_shapes=[
                pltpu.VMEM((T, G, D), BF),
                pltpu.VMEM((1, D, S2 * T), BF),
                pltpu.VMEM((AHEAD + 1, S2 * T, QB), F32),
                pltpu.SemaphoreType.DMA((HKV,)),
            ],
            compiler_params=pltpu.CompilerParams(vmem_limit_bytes=8 << 20),
        )(*parts)

    return jax.shard_map(local, mesh=mesh, in_specs=(spec, spec, spec), out_specs=spec, check_vma=False)
```

```python
import jax
import jax.numpy as jnp
from jax import lax
from jax.experimental import pallas as pl
from jax.experimental.pallas import tpu as pltpu
from jax.sharding import PartitionSpec as P

T = 256
HKV = 8
G = 8
D = 128
NB = 8
SUB = T // NB
QB = SUB * G
S1 = 6
S2 = 2
C = (D ** -0.5) * 1.4426950408889634
ORDER = (0, 2, 4, 6, 7, 5, 3, 1)
AHEAD = 4
U0, U1, U2 = 1, 1, 1
BF = jnp.bfloat16
F32 = jnp.float32
NT = (((1,), (1,)), ((), ()))


def chunks(n):
    return [(r, min(r + 256, n)) for r in range(0, n, 256)]


def by_tile(kv, h, s0, ns):
    return jnp.concatenate([kv[h, s, 1, t * SUB:(t + 1) * SUB] for t in range(NB) for s in range(s0, s0 + ns)], axis=0)


def fold(f, x):
    return f(x.reshape(-1, 8, x.shape[-1]), axis=0)


def attend(heads, kv, s0, ns, bias, qt, oacc, ml, vt, sref, arrive=None, first=False, out=None):
    rows = ns * SUB
    items = [(u, j) for u in range(len(heads)) for j in ORDER]
    tops = {}

    def scores(i, c):
        u, j = items[i]
        h = heads[u]
        r0, r1 = c
        if j == ORDER[0] and r0 == 0:
            if arrive:
                arrive(u)
            vt[u, :, :ns * T] = by_tile(kv, h, s0, ns).T
        parts = [kv[h, s0 + x % ns, 0, x // ns * SUB:(x // ns + 1) * SUB] for x in range(r0 // SUB, r1 // SUB)]
        s = lax.dot_general(jnp.concatenate(parts, axis=0), qt[h, j * SUB:(j + 1) * SUB].reshape(QB, D), NT,
                            preferred_element_type=F32)
        lo = max(r0, j * rows)
        if lo < r1:
            d = s[lo - r0:] + bias[lo - j * rows:r1 - j * rows]
            s = d if lo == r0 else jnp.concatenate([s[:lo - r0], d], axis=0)
        sref[i % (AHEAD + 1), r0:r1] = s
        m = fold(jnp.max, s)
        tops[i] = jnp.maximum(tops[i], m) if i in tops else m

    def values(i, c, m, acc):
        u, j = items[i]
        r0, r1 = c
        p = jnp.exp2((sref[i % (AHEAD + 1), r0:r1] - m) * C)
        l = fold(jnp.sum, p)
        o = jnp.dot(vt[u, :, r0:r1], p.astype(BF), preferred_element_type=F32)
        return (acc[0] + l, acc[1] + o) if acc else (l, o)

    def finish(i, m, a, l, o):
        u, j = items[i]
        h = heads[u]
        if not first:
            l = ml[h, j, 1:2] * a + l
        if out is None:
            oacc[h, j] = o if first else oacc[h, j] * a + o
            ml[h, j, 0:1] = m
            ml[h, j, 1:2] = l
            return
        r = 1.0 / l
        o = oacc[h, j] * (a * r) + o * r
        out(u)[j * SUB:(j + 1) * SUB] = o.T.astype(BF).reshape(SUB, G, D)

    todo = [(i, c) for i, (u, j) in enumerate(items) for c in chunks((j + 1) * rows)]
    total = len(todo)
    sizes = [len(chunks((j + 1) * rows)) for u, j in items]
    at = 0
    while at < total and todo[at][0] < AHEAD:
        scores(*todo[at])
        at += 1
    for i, (u, j) in enumerate(items):
        top = jnp.max(tops[i], axis=0, keepdims=True)
        m, a = top, None
        if not first:
            m1 = ml[heads[u], j, 0:1]
            m = jnp.maximum(top, m1)
            a = jnp.exp2((m1 - m) * C)
        acc = None
        goal = sum(sizes[:i + AHEAD + 1])
        start = at
        mine = chunks((j + 1) * rows)
        for t, c in enumerate(mine):
            upto = start + (goal - start) * (t + 1) // len(mine)
            while at < upto:
                scores(*todo[at])
                at += 1
            acc = values(i, c, m, acc)
        finish(i, m, a, jnp.sum(acc[0], axis=0, keepdims=True), acc[1])


def kernel(q_hbm, k_hbm, v_hbm, ob, qt, kv2, bias2, oacc, ml, raw, wide, kv1, vt, sref, bias0, bias1,
           lsem, qsem, ssem, rsem):
    cx, cy, cz = lax.axis_index("cx"), lax.axis_index("cy"), lax.axis_index("cz")
    me = (cx * 2 + cy) * 2 + cz
    nx = {"cy": 1 - cy}
    ny = {"cx": 1 - cx}
    sib = {"cz": 1 - cz}

    barrier = pltpu.get_barrier_semaphore()
    for dev in (nx, ny, sib):
        pl.semaphore_signal(barrier, inc=1, device_id=dev, device_id_type=pl.DeviceIdType.MESH)

    loads = [pltpu.make_async_copy(x, raw.at[i], lsem.at[i]) for i, x in enumerate((k_hbm, v_hbm))]
    for x in loads:
        x.start()

    def qload(h):
        return pltpu.make_async_copy(q_hbm.at[:, pl.ds(pl.multiple_of(h * G, G), G), :], qt.at[h], qsem.at[h])

    def rdma(kind, h):
        src, dst, dev = (
            (kv1.at[h, 0], kv1.at[h, 2], nx),
            (kv1.at[h, 0], kv1.at[h, 4], ny),
            (kv1.at[h, 0], kv1.at[h, 1], sib),
            (kv1.at[h, 2], kv1.at[h, 3], sib),
            (kv1.at[h, 4], kv1.at[h, 5], sib),
            (kv1.at[h, 2, 0], kv2.at[h, 0, 0], ny),
            (kv1.at[h, 4, 1], kv2.at[h, 0, 1], nx),
            (kv2.at[h, 0], kv2.at[h, 1], sib),
        )[kind]
        return pltpu.make_async_remote_copy(src, dst, ssem.at[kind, h], rsem.at[kind, h], dev,
                                            pl.DeviceIdType.MESH)

    def mask(nslot, base, ref):
        r = lax.broadcasted_iota(jnp.int32, (nslot * SUB, QB), 0)
        c = lax.broadcasted_iota(jnp.int32, (nslot * SUB, QB), 1)
        kpos = (r % SUB) * 8 + (me ^ (r // SUB + base))
        qpos = (c // G) * 8 + me
        ref[...] = jnp.where(kpos <= qpos, 0.0, -1e30)

    for i in range(2):
        loads[i].wait()
        wide[i] = raw[i].astype(F32).reshape(T * HKV, D)

    def send(h):
        for kind in range(3):
            rdma(kind, h).start()

    for h in range(HKV):
        for i in range(2):
            kv1[h, 0, i] = wide[i, pl.ds(h, T, stride=HKV), :].astype(BF)
        if h == 1:
            pl.semaphore_wait(barrier, 3)
        if h:
            send(h - 1)

    mask(2, 0, bias0)
    send(HKV - 1)

    @pl.loop(0, HKV)
    def _(h):
        qload(h).start()

    mask(4, 2, bias1)
    mask(2, 6, bias2)

    def pass_on(h):
        rdma(0, h).wait_recv()
        rdma(1, h).wait_recv()
        for kind in (3, 4, 5, 6):
            rdma(kind, h).start()

    def pass_on2(h):
        rdma(5, h).wait_recv()
        rdma(6, h).wait_recv()
        rdma(7, h).start()

    @pl.loop(0, HKV // U0)
    def _(g):
        heads = [g * U0 + u for u in range(U0)]

        def arrive(u):
            h = heads[u]
            qload(h).wait()
            rdma(2, h).wait_recv()

        attend(heads, kv1, 0, 2, bias0, qt, oacc, ml, vt, sref, arrive, first=True)

    pass_on(0)

    @pl.loop(0, HKV // U1)
    def _(g):
        heads = [g * U1 + u for u in range(U1)]

        def arrive(u):
            h = heads[u]
            if u < U1 - 1:
                pass_on(h + 1)
            else:
                @pl.when(h < HKV - 1)
                def _():
                    pass_on(h + 1)

            rdma(3, h).wait_recv()
            rdma(4, h).wait_recv()

        attend(heads, kv1, 2, 4, bias1, qt, oacc, ml, vt, sref, arrive)

    pass_on2(0)

    @pl.loop(0, (HKV - 1) // U2)
    def _(g):
        heads = [g * U2 + u for u in range(U2)]

        def arrive(u):
            pass_on2(heads[u] + 1)
            rdma(7, heads[u]).wait_recv()

        attend(heads, kv2, 0, 2, bias2, qt, oacc, ml, vt, sref, arrive, out=lambda u: ob.at[heads[u]])

    rdma(7, HKV - 1).wait_recv()

    @pl.loop(0, HKV)
    def _(h):
        for kind in range(8):
            rdma(kind, h).wait_send()


def spread(ob, qt, kv2, bias2, oacc, ml, o_hbm, last, vt, sref, sem):
    def put(src, h):
        return pltpu.make_async_copy(src, o_hbm.at[:, pl.ds(pl.multiple_of(h * G, G), G), :], sem.at[h])

    @pl.loop(0, HKV - 1)
    def _(h):
        put(ob.at[h], h).start()

    attend([HKV - 1], kv2, 0, 2, bias2, qt, oacc, ml, vt, sref, out=lambda u: last)
    put(last, HKV - 1).start()

    @pl.loop(0, HKV - 1)
    def _(h):
        put(ob.at[h], h).wait()

    put(last, HKV - 1).wait()


def solution(mesh):
    spec = P(("dp", "cx", "cy", "cz"))

    def local(q, k, v):
        hbm = pl.BlockSpec(memory_space=pltpu.HBM)
        vmem = pl.BlockSpec(memory_space=pltpu.VMEM)
        parts = pl.pallas_call(
            kernel,
            out_shape=[
                pltpu.VMEM((HKV - 1, T, G, D), BF),
                pltpu.VMEM((HKV, T, G, D), BF),
                pltpu.VMEM((HKV, S2, 2, T, D), BF),
                pltpu.VMEM((S2 * SUB, QB), F32),
                pltpu.VMEM((HKV, NB, D, QB), F32),
                pltpu.VMEM((HKV, NB, 8, QB), F32),
            ],
            in_specs=[hbm] * 3,
            out_specs=[vmem] * 6,
            scratch_shapes=[
                pltpu.VMEM((2, T, HKV, D), BF),
                pltpu.VMEM((2, T * HKV, D), F32),
                pltpu.VMEM((HKV, S1, 2, T, D), BF),
                pltpu.VMEM((max(U0, U1, U2), D, 4 * T), BF),
                pltpu.VMEM((AHEAD + 1, 4 * T, QB), F32),
                pltpu.VMEM((2 * SUB, QB), F32),
                pltpu.VMEM((4 * SUB, QB), F32),
                pltpu.SemaphoreType.DMA((2,)),
                pltpu.SemaphoreType.DMA((HKV,)),
                pltpu.SemaphoreType.DMA((8, HKV)),
                pltpu.SemaphoreType.DMA((8, HKV)),
            ],
            compiler_params=pltpu.CompilerParams(
                vmem_limit_bytes=36 << 20, collective_id=0, has_side_effects=True),
        )(*(pltpu.with_memory_space_constraint(x, pltpu.HBM) for x in (q, k, v)))
        return pl.pallas_call(
            spread,
            out_shape=jax.ShapeDtypeStruct(q.shape, q.dtype),
            in_specs=[vmem] * 6,
            out_specs=hbm,
            scratch_shapes=[
                pltpu.VMEM((T, G, D), BF),
                pltpu.VMEM((1, D, S2 * T), BF),
                pltpu.VMEM((AHEAD + 1, S2 * T, QB), F32),
                pltpu.SemaphoreType.DMA((HKV,)),
            ],
            compiler_params=pltpu.CompilerParams(vmem_limit_bytes=8 << 20),
        )(*parts)

    return jax.shard_map(local, mesh=mesh, in_specs=(spec, spec, spec), out_specs=spec, check_vma=False)
```

```python
import jax
import jax.numpy as jnp
from jax import lax
from jax.experimental import pallas as pl
from jax.experimental.pallas import tpu as pltpu
from jax.sharding import PartitionSpec as P

T = 256
HKV = 8
G = 8
D = 128
NB = 8
SUB = T // NB
QB = SUB * G
S1 = 6
S2 = 2
C = (D ** -0.5) * 1.4426950408889634
ORDER = (0, 2, 4, 6, 7, 5, 3, 1)
AHEAD = 4
U0, U1, U2 = 1, 1, 1
BF = jnp.bfloat16
F32 = jnp.float32
NT = (((1,), (1,)), ((), ()))


def chunks(n):
    return [(r, min(r + 256, n)) for r in range(0, n, 256)]


def by_tile(piece, kind, ns):
    return jnp.concatenate([piece(kind, x, t) for t in range(NB) for x in range(ns)], axis=0)


def fold(f, x):
    return f(x.reshape(-1, 8, x.shape[-1]), axis=0)


def attend(heads, piece_of, ns, bias, qt, oacc, ml, vt, sref, arrive=None, first=False, out=None):
    rows = ns * SUB
    items = [(u, j) for u in range(len(heads)) for j in ORDER]
    tops = {}

    def scores(i, c):
        u, j = items[i]
        h = heads[u]
        r0, r1 = c
        if j == ORDER[0] and r0 == 0:
            if arrive:
                arrive(u)
            vt[u, :, :ns * T] = by_tile(piece_of(h), 1, ns).T
        parts = [piece_of(h)(0, x % ns, x // ns) for x in range(r0 // SUB, r1 // SUB)]
        s = lax.dot_general(jnp.concatenate(parts, axis=0), qt[h, j * SUB:(j + 1) * SUB].reshape(QB, D), NT,
                            preferred_element_type=F32)
        lo = max(r0, j * rows)
        if lo < r1:
            d = s[lo - r0:] + bias[lo - j * rows:r1 - j * rows]
            s = d if lo == r0 else jnp.concatenate([s[:lo - r0], d], axis=0)
        sref[i % (AHEAD + 1), r0:r1] = s
        m = fold(jnp.max, s)
        tops[i] = jnp.maximum(tops[i], m) if i in tops else m

    def values(i, c, m, acc):
        u, j = items[i]
        r0, r1 = c
        p = jnp.exp2((sref[i % (AHEAD + 1), r0:r1] - m) * C)
        l = fold(jnp.sum, p)
        o = jnp.dot(vt[u, :, r0:r1], p.astype(BF), preferred_element_type=F32)
        return (acc[0] + l, acc[1] + o) if acc else (l, o)

    def finish(i, m, a, l, o):
        u, j = items[i]
        h = heads[u]
        if not first:
            l = ml[h, j, 1:2] * a + l
        if out is None:
            oacc[h, j] = o if first else oacc[h, j] * a + o
            ml[h, j, 0:1] = m
            ml[h, j, 1:2] = l
            return
        r = 1.0 / l
        o = oacc[h, j] * (a * r) + o * r
        out(u)[j * SUB:(j + 1) * SUB] = o.T.astype(BF).reshape(SUB, G, D)

    todo = [(i, c) for i, (u, j) in enumerate(items) for c in chunks((j + 1) * rows)]
    total = len(todo)
    sizes = [len(chunks((j + 1) * rows)) for u, j in items]
    at = 0
    while at < total and todo[at][0] < AHEAD:
        scores(*todo[at])
        at += 1
    for i, (u, j) in enumerate(items):
        top = jnp.max(tops[i], axis=0, keepdims=True)
        m, a = top, None
        if not first:
            m1 = ml[heads[u], j, 0:1]
            m = jnp.maximum(top, m1)
            a = jnp.exp2((m1 - m) * C)
        acc = None
        goal = sum(sizes[:i + AHEAD + 1])
        start = at
        mine = chunks((j + 1) * rows)
        for t, c in enumerate(mine):
            upto = start + (goal - start) * (t + 1) // len(mine)
            while at < upto:
                scores(*todo[at])
                at += 1
            acc = values(i, c, m, acc)
        finish(i, m, a, jnp.sum(acc[0], axis=0, keepdims=True), acc[1])


def near(kv1, chip):
    def of(h):
        return lambda kind, x, t: kv1[h, kind, chip + x // 2, x % 2, t * SUB:(t + 1) * SUB]
    return of


def far(kv2):
    def of(h):
        return lambda kind, x, t: kv2[h, kind, x, t * SUB:(t + 1) * SUB]
    return of


def kernel(q_hbm, k_hbm, v_hbm, ob, qt, kv2, bias2, oacc, ml, raw, wide, kv1, vt, sref, bias0, bias1,
           lsem, qsem, ssem, rsem):
    cx, cy, cz = lax.axis_index("cx"), lax.axis_index("cy"), lax.axis_index("cz")
    me = (cx * 2 + cy) * 2 + cz
    chip = cx * 2 + cy
    mine = 1 - cz

    def over(core):
        return {"cx": cx + cz - 2 * cx * cz, "cy": cy + mine - 2 * cy * mine, "cz": core}

    sib = {"cz": 1 - cz}

    barrier = pltpu.get_barrier_semaphore()
    for dev in ({"cx": cx, "cy": 1 - cy, "cz": 0}, {"cx": 1 - cx, "cy": cy, "cz": 1}, sib):
        pl.semaphore_signal(barrier, inc=1, device_id=dev, device_id_type=pl.DeviceIdType.MESH)

    loads = [pltpu.make_async_copy(x, raw.at[i], lsem.at[i]) for i, x in enumerate((k_hbm, v_hbm))]
    for x in loads:
        x.start()

    def qload(h):
        return pltpu.make_async_copy(q_hbm.at[:, pl.ds(pl.multiple_of(h * G, G), G), :], qt.at[h], qsem.at[h])

    def rdma(src, dst, send, recv, h, dev):
        return pltpu.make_async_remote_copy(src, dst, ssem.at[send, h], rsem.at[recv, h], dev,
                                            pl.DeviceIdType.MESH)

    def swap(h):
        return rdma(kv1.at[h, :, 0, cz], kv1.at[h, :, 0, cz], 0, 5, h, sib)

    def out_k(h):
        return rdma(kv1.at[h, 0, 0], kv1.at[h, 0, 1 + cz], 1, cz, h, over(1))

    def out_v(h):
        return rdma(kv1.at[h, 1, 0], kv1.at[h, 1, 1 + cz], 2, cz, h, over(0))

    def half_k(z):
        return rdma(kv1.at[0, 0, 0, z], kv1.at[0, 0, 1 + cz, z], 1, cz, 0, over(1))

    def half_v(z):
        return rdma(kv1.at[0, 1, 0, z], kv1.at[0, 1, 1 + cz, z], 2, cz, 0, over(0))

    def relay(h):
        return rdma(kv1.at[h, mine, 1:3], kv1.at[h, mine, 1:3], 3, 2, h, sib)

    def forward(h):
        return rdma(kv1.at[h, mine, 2 - cz], kv2.at[h, mine], 4, 3, h, over(cz))

    def relay2(h):
        return rdma(kv2.at[h, mine], kv2.at[h, mine], 5, 4, h, sib)

    def arrived(dst, recv, h):
        rdma(dst, dst, 0, recv, h, sib).wait_recv()

    def mask(nslot, far_chip, ref):
        r = lax.broadcasted_iota(jnp.int32, (nslot * SUB, QB), 0)
        c = lax.broadcasted_iota(jnp.int32, (nslot * SUB, QB), 1)
        x = r // SUB
        kpos = (r % SUB) * 8 + (chip ^ (x // 2 + far_chip)) * 2 + x % 2
        qpos = (c // G) * 8 + me
        ref[...] = jnp.where(kpos <= qpos, 0.0, -1e30)

    for i in range(2):
        loads[i].wait()
        wide[i] = raw[i].astype(F32).reshape(T * HKV, D)

    for h in range(HKV):
        for i in range(2):
            kv1[h, i, 0, cz] = wide[i, pl.ds(h, T, stride=HKV), :].astype(BF)
        if h == 1:
            pl.semaphore_wait(barrier, 3)
            half_k(cz).start()
            half_v(cz).start()
        if h:
            swap(h - 1).start()

    mask(2, 0, bias0)
    swap(HKV - 1).start()

    arrived(kv1.at[0, :, 0, cz], 5, 0)
    half_k(1 - cz).start()
    half_v(1 - cz).start()

    @pl.loop(1, HKV)
    def _(h):
        arrived(kv1.at[h, :, 0, cz], 5, h)
        out_k(h).start()
        out_v(h).start()

    @pl.loop(0, HKV)
    def _(h):
        qload(h).start()

    mask(4, 1, bias1)
    mask(2, 3, bias2)

    def pass_on(h):
        arrived(kv1.at[h, mine, 1], 0, h)
        arrived(kv1.at[h, mine, 2], 1, h)
        relay(h).start()
        forward(h).start()

    def pass_on2(h):
        arrived(kv2.at[h, mine], 3, h)
        relay2(h).start()

    @pl.loop(0, HKV // U0)
    def _(g):
        heads = [g * U0 + u for u in range(U0)]

        def arrive(u):
            h = heads[u]
            qload(h).wait()

        attend(heads, near(kv1, 0), 2, bias0, qt, oacc, ml, vt, sref, arrive, first=True)

    pass_on(0)

    @pl.loop(0, HKV // U1)
    def _(g):
        heads = [g * U1 + u for u in range(U1)]

        def arrive(u):
            h = heads[u]
            if u < U1 - 1:
                pass_on(h + 1)
            else:
                @pl.when(h < HKV - 1)
                def _():
                    pass_on(h + 1)

            arrived(kv1.at[h, cz, 1:3], 2, h)

        attend(heads, near(kv1, 1), 4, bias1, qt, oacc, ml, vt, sref, arrive)

    pass_on2(0)

    @pl.loop(0, (HKV - 1) // U2)
    def _(g):
        heads = [g * U2 + u for u in range(U2)]

        def arrive(u):
            pass_on2(heads[u] + 1)
            arrived(kv2.at[heads[u], cz], 4, heads[u])

        attend(heads, far(kv2), 2, bias2, qt, oacc, ml, vt, sref, arrive, out=lambda u: ob.at[heads[u]])

    arrived(kv2.at[HKV - 1, cz], 4, HKV - 1)

    @pl.loop(0, HKV)
    def _(h):
        for sent in (swap, out_k, out_v, relay, forward, relay2):
            sent(h).wait_send()


def spread(ob, qt, kv2, bias2, oacc, ml, o_hbm, last, vt, sref, sem):
    def put(src, h):
        return pltpu.make_async_copy(src, o_hbm.at[:, pl.ds(pl.multiple_of(h * G, G), G), :], sem.at[h])

    @pl.loop(0, HKV - 1)
    def _(h):
        put(ob.at[h], h).start()

    attend([HKV - 1], far(kv2), 2, bias2, qt, oacc, ml, vt, sref, out=lambda u: last)
    put(last, HKV - 1).start()

    @pl.loop(0, HKV - 1)
    def _(h):
        put(ob.at[h], h).wait()

    put(last, HKV - 1).wait()


def solution(mesh):
    spec = P(("dp", "cx", "cy", "cz"))

    def local(q, k, v):
        hbm = pl.BlockSpec(memory_space=pltpu.HBM)
        vmem = pl.BlockSpec(memory_space=pltpu.VMEM)
        parts = pl.pallas_call(
            kernel,
            out_shape=[
                pltpu.VMEM((HKV - 1, T, G, D), BF),
                pltpu.VMEM((HKV, T, G, D), BF),
                pltpu.VMEM((HKV, 2, 2, T, D), BF),
                pltpu.VMEM((S2 * SUB, QB), F32),
                pltpu.VMEM((HKV, NB, D, QB), F32),
                pltpu.VMEM((HKV, NB, 8, QB), F32),
            ],
            in_specs=[hbm] * 3,
            out_specs=[vmem] * 6,
            scratch_shapes=[
                pltpu.VMEM((2, T, HKV, D), BF),
                pltpu.VMEM((2, T * HKV, D), F32),
                pltpu.VMEM((HKV, 2, 3, 2, T, D), BF),
                pltpu.VMEM((max(U0, U1, U2), D, 4 * T), BF),
                pltpu.VMEM((AHEAD + 1, 4 * T, QB), F32),
                pltpu.VMEM((2 * SUB, QB), F32),
                pltpu.VMEM((4 * SUB, QB), F32),
                pltpu.SemaphoreType.DMA((2,)),
                pltpu.SemaphoreType.DMA((HKV,)),
                pltpu.SemaphoreType.DMA((6, HKV)),
                pltpu.SemaphoreType.DMA((6, HKV)),
            ],
            compiler_params=pltpu.CompilerParams(
                vmem_limit_bytes=36 << 20, collective_id=0, has_side_effects=True),
        )(*(pltpu.with_memory_space_constraint(x, pltpu.HBM) for x in (q, k, v)))
        return pl.pallas_call(
            spread,
            out_shape=jax.ShapeDtypeStruct(q.shape, q.dtype),
            in_specs=[vmem] * 6,
            out_specs=hbm,
            scratch_shapes=[
                pltpu.VMEM((T, G, D), BF),
                pltpu.VMEM((1, D, S2 * T), BF),
                pltpu.VMEM((AHEAD + 1, S2 * T, QB), F32),
                pltpu.SemaphoreType.DMA((HKV,)),
            ],
            compiler_params=pltpu.CompilerParams(vmem_limit_bytes=8 << 20),
        )(*parts)

    return jax.shard_map(local, mesh=mesh, in_specs=(spec, spec, spec), out_specs=spec, check_vma=False)
```

```python
import jax
import jax.numpy as jnp
from jax import lax
from jax.experimental import pallas as pl
from jax.experimental.pallas import tpu as pltpu
from jax.sharding import PartitionSpec as P

T = 256
CUT = 160
HKV = 8
G = 8
D = 128
NB = 8
SUB = T // NB
QB = SUB * G
S1 = 6
S2 = 2
C = (D ** -0.5) * 1.4426950408889634
ORDER = (0, 2, 4, 6, 7, 5, 3, 1)
AHEAD = 4
U0, U1, U2 = 1, 1, 1
BF = jnp.bfloat16
F32 = jnp.float32
NT = (((1,), (1,)), ((), ()))


def chunks(n):
    return [(r, min(r + 256, n)) for r in range(0, n, 256)]


def by_tile(kv, h, s0, ns):
    return jnp.concatenate([kv[h, s, 1, t * SUB:(t + 1) * SUB] for t in range(NB) for s in range(s0, s0 + ns)], axis=0)


def fold(f, x):
    return f(x.reshape(-1, 8, x.shape[-1]), axis=0)


def attend(heads, kv, s0, ns, bias, qt, oacc, ml, vt, sref, arrive=None, first=False, out=None):
    rows = ns * SUB
    items = [(u, j) for u in range(len(heads)) for j in ORDER]
    tops = {}

    def scores(i, c):
        u, j = items[i]
        h = heads[u]
        r0, r1 = c
        if j == ORDER[0] and r0 == 0:
            if arrive:
                arrive(u)
            vt[u, :, :ns * T] = by_tile(kv, h, s0, ns).T
        parts = [kv[h, s0 + x % ns, 0, x // ns * SUB:(x // ns + 1) * SUB] for x in range(r0 // SUB, r1 // SUB)]
        s = lax.dot_general(jnp.concatenate(parts, axis=0), qt[h, j * SUB:(j + 1) * SUB].reshape(QB, D), NT,
                            preferred_element_type=F32)
        lo = max(r0, j * rows)
        if lo < r1:
            d = s[lo - r0:] + bias[lo - j * rows:r1 - j * rows]
            s = d if lo == r0 else jnp.concatenate([s[:lo - r0], d], axis=0)
        sref[i % (AHEAD + 1), r0:r1] = s
        m = fold(jnp.max, s)
        tops[i] = jnp.maximum(tops[i], m) if i in tops else m

    def values(i, c, m, acc):
        u, j = items[i]
        r0, r1 = c
        p = jnp.exp2((sref[i % (AHEAD + 1), r0:r1] - m) * C)
        l = fold(jnp.sum, p)
        o = jnp.dot(vt[u, :, r0:r1], p.astype(BF), preferred_element_type=F32)
        return (acc[0] + l, acc[1] + o) if acc else (l, o)

    def finish(i, m, a, l, o):
        u, j = items[i]
        h = heads[u]
        if not first:
            l = ml[h, j, 1:2] * a + l
        if out is None:
            oacc[h, j] = o if first else oacc[h, j] * a + o
            ml[h, j, 0:1] = m
            ml[h, j, 1:2] = l
            return
        r = 1.0 / l
        o = oacc[h, j] * (a * r) + o * r
        out(u)[j * SUB:(j + 1) * SUB] = o.T.astype(BF).reshape(SUB, G, D)

    todo = [(i, c) for i, (u, j) in enumerate(items) for c in chunks((j + 1) * rows)]
    total = len(todo)
    sizes = [len(chunks((j + 1) * rows)) for u, j in items]
    at = 0
    while at < total and todo[at][0] < AHEAD:
        scores(*todo[at])
        at += 1
    for i, (u, j) in enumerate(items):
        top = jnp.max(tops[i], axis=0, keepdims=True)
        m, a = top, None
        if not first:
            m1 = ml[heads[u], j, 0:1]
            m = jnp.maximum(top, m1)
            a = jnp.exp2((m1 - m) * C)
        acc = None
        goal = sum(sizes[:i + AHEAD + 1])
        start = at
        mine = chunks((j + 1) * rows)
        for t, c in enumerate(mine):
            upto = start + (goal - start) * (t + 1) // len(mine)
            while at < upto:
                scores(*todo[at])
                at += 1
            acc = values(i, c, m, acc)
        finish(i, m, a, jnp.sum(acc[0], axis=0, keepdims=True), acc[1])


def kernel(q_hbm, k_hbm, v_hbm, ob, qt, kv2, bias2, oacc, ml, raw, wide, kv1, vt, sref, bias0, bias1,
           lsem, qsem, ssem, rsem, lssem, lrsem):
    cx, cy, cz = lax.axis_index("cx"), lax.axis_index("cy"), lax.axis_index("cz")
    me = (cx * 2 + cy) * 2 + cz
    nx = {"cy": 1 - cy}
    ny = {"cx": 1 - cx}
    sib = {"cz": 1 - cz}

    barrier = pltpu.get_barrier_semaphore()
    for dev in (nx, ny, sib):
        pl.semaphore_signal(barrier, inc=1, device_id=dev, device_id_type=pl.DeviceIdType.MESH)

    loads = [pltpu.make_async_copy(x, raw.at[i], lsem.at[i]) for i, x in enumerate((k_hbm, v_hbm))]
    for x in loads:
        x.start()

    def qload(h):
        return pltpu.make_async_copy(q_hbm.at[:, pl.ds(pl.multiple_of(h * G, G), G), :], qt.at[h], qsem.at[h])

    def rdma(kind, h, i=None):
        src, dst, dev = (
            (kv1.at[h, 0], kv1.at[h, 2], nx),
            (kv1.at[h, 0], kv1.at[h, 4], ny),
            (kv1.at[h, 0], kv1.at[h, 1], sib),
            (kv1.at[h, 2], kv1.at[h, 3], sib),
            (kv1.at[h, 4], kv1.at[h, 5], sib),
            (kv1.at[h, 2, 0], kv2.at[h, 0, 0], ny),
            (kv1.at[h, 4, 1], kv2.at[h, 0, 1], nx),
            (kv2.at[h, 0], kv2.at[h, 1], sib),
        )[kind]
        if i is not None:
            src, dst = src.at[i], dst.at[i]
        return pltpu.make_async_remote_copy(src, dst, ssem.at[kind, h], rsem.at[kind, h], dev,
                                            pl.DeviceIdType.MESH)

    def last(i, part):
        rows = pl.ds(0, CUT) if part == 0 else pl.ds(CUT, T - CUT)
        src = kv1.at[HKV - 1, (2, 4)[i], i, rows]
        dst = kv2.at[HKV - 1, 1 if part == 2 else 0, i, rows]
        dev = (ny, nx)[i] if part < 2 else ((ny, nx)[i] | sib)
        return pltpu.make_async_remote_copy(src, dst, lssem.at[i, part], lrsem.at[i, part], dev,
                                            pl.DeviceIdType.MESH)

    def last_relay():
        rows = pl.ds(0, CUT)
        return pltpu.make_async_remote_copy(kv2.at[HKV - 1, 0, :, rows], kv2.at[HKV - 1, 1, :, rows],
                                            ssem.at[7, HKV - 1], rsem.at[7, HKV - 1], sib, pl.DeviceIdType.MESH)

    def mask(nslot, base, ref):
        r = lax.broadcasted_iota(jnp.int32, (nslot * SUB, QB), 0)
        c = lax.broadcasted_iota(jnp.int32, (nslot * SUB, QB), 1)
        kpos = (r % SUB) * 8 + (me ^ (r // SUB + base))
        qpos = (c // G) * 8 + me
        ref[...] = jnp.where(kpos <= qpos, 0.0, -1e30)

    def relaid(h, i):
        kv1[h, 0, i] = wide[i, pl.ds(h, T, stride=HKV), :].astype(BF)

    def send(h):
        for kind in range(3):
            rdma(kind, h).start()

    for i in range(2):
        loads[i].wait()
        wide[i] = raw[i].astype(F32).reshape(T * HKV, D)
        relaid(0, i)
        relaid(1, i)
        if i == 0:
            pl.semaphore_wait(barrier, 3)
        for kind in range(3):
            rdma(kind, 0, i).start()

    for h in range(2, HKV):
        for i in range(2):
            relaid(h, i)
        send(h - 1)

    mask(2, 0, bias0)
    send(HKV - 1)

    @pl.loop(0, HKV)
    def _(h):
        qload(h).start()

    mask(4, 2, bias1)
    mask(2, 6, bias2)

    def pass_on(h):
        rdma(0, h).wait_recv()
        rdma(1, h).wait_recv()
        for kind in (3, 4):
            rdma(kind, h).start()

        @pl.when(h < HKV - 1)
        def _():
            for kind in (5, 6):
                rdma(kind, h).start()

        @pl.when(h == HKV - 1)
        def _():
            for part in range(3):
                for i in range(2):
                    last(i, part).start()

    def pass_on2(h):
        @pl.when(h < HKV - 1)
        def _():
            rdma(5, h).wait_recv()
            rdma(6, h).wait_recv()
            rdma(7, h).start()

        @pl.when(h == HKV - 1)
        def _():
            for i in range(2):
                last(i, 0).wait_recv()
            last_relay().start()

    @pl.loop(0, HKV // U0)
    def _(g):
        heads = [g * U0 + u for u in range(U0)]

        def arrive(u):
            h = heads[u]
            qload(h).wait()
            rdma(2, h).wait_recv()

        attend(heads, kv1, 0, 2, bias0, qt, oacc, ml, vt, sref, arrive, first=True)

    pass_on(jnp.int32(0))

    @pl.loop(0, HKV // U1)
    def _(g):
        heads = [g * U1 + u for u in range(U1)]

        def arrive(u):
            h = heads[u]
            if u < U1 - 1:
                pass_on(h + 1)
            else:
                @pl.when(h < HKV - 1)
                def _():
                    pass_on(h + 1)

            rdma(3, h).wait_recv()
            rdma(4, h).wait_recv()

        attend(heads, kv1, 2, 4, bias1, qt, oacc, ml, vt, sref, arrive)

    pass_on2(jnp.int32(0))

    @pl.loop(0, (HKV - 1) // U2)
    def _(g):
        heads = [g * U2 + u for u in range(U2)]

        def arrive(u):
            pass_on2(heads[u] + 1)
            rdma(7, heads[u]).wait_recv()

        attend(heads, kv2, 0, 2, bias2, qt, oacc, ml, vt, sref, arrive, out=lambda u: ob.at[heads[u]])

    for part in (1, 2):
        for i in range(2):
            last(i, part).wait_recv()
    last_relay().wait_recv()

    @pl.loop(0, HKV)
    def _(h):
        for kind in range(5):
            rdma(kind, h).wait_send()

    @pl.loop(0, HKV - 1)
    def _(h):
        for kind in range(5, 8):
            rdma(kind, h).wait_send()

    for part in range(3):
        for i in range(2):
            last(i, part).wait_send()
    last_relay().wait_send()


def spread(ob, qt, kv2, bias2, oacc, ml, o_hbm, last, vt, sref, sem):
    def put(src, h):
        return pltpu.make_async_copy(src, o_hbm.at[:, pl.ds(pl.multiple_of(h * G, G), G), :], sem.at[h])

    @pl.loop(0, HKV - 1)
    def _(h):
        put(ob.at[h], h).start()

    attend([HKV - 1], kv2, 0, 2, bias2, qt, oacc, ml, vt, sref, out=lambda u: last)
    put(last, HKV - 1).start()

    @pl.loop(0, HKV - 1)
    def _(h):
        put(ob.at[h], h).wait()

    put(last, HKV - 1).wait()


def solution(mesh):
    spec = P(("dp", "cx", "cy", "cz"))

    def local(q, k, v):
        hbm = pl.BlockSpec(memory_space=pltpu.HBM)
        vmem = pl.BlockSpec(memory_space=pltpu.VMEM)
        parts = pl.pallas_call(
            kernel,
            out_shape=[
                pltpu.VMEM((HKV - 1, T, G, D), BF),
                pltpu.VMEM((HKV, T, G, D), BF),
                pltpu.VMEM((HKV, S2, 2, T, D), BF),
                pltpu.VMEM((S2 * SUB, QB), F32),
                pltpu.VMEM((HKV, NB, D, QB), F32),
                pltpu.VMEM((HKV, NB, 8, QB), F32),
            ],
            in_specs=[hbm] * 3,
            out_specs=[vmem] * 6,
            scratch_shapes=[
                pltpu.VMEM((2, T, HKV, D), BF),
                pltpu.VMEM((2, T * HKV, D), F32),
                pltpu.VMEM((HKV, S1, 2, T, D), BF),
                pltpu.VMEM((max(U0, U1, U2), D, 4 * T), BF),
                pltpu.VMEM((AHEAD + 1, 4 * T, QB), F32),
                pltpu.VMEM((2 * SUB, QB), F32),
                pltpu.VMEM((4 * SUB, QB), F32),
                pltpu.SemaphoreType.DMA((2,)),
                pltpu.SemaphoreType.DMA((HKV,)),
                pltpu.SemaphoreType.DMA((8, HKV)),
                pltpu.SemaphoreType.DMA((8, HKV)),
                pltpu.SemaphoreType.DMA((2, 3)),
                pltpu.SemaphoreType.DMA((2, 3)),
            ],
            compiler_params=pltpu.CompilerParams(
                vmem_limit_bytes=36 << 20, collective_id=0, has_side_effects=True),
        )(*(pltpu.with_memory_space_constraint(x, pltpu.HBM) for x in (q, k, v)))
        return pl.pallas_call(
            spread,
            out_shape=jax.ShapeDtypeStruct(q.shape, q.dtype),
            in_specs=[vmem] * 6,
            out_specs=hbm,
            scratch_shapes=[
                pltpu.VMEM((T, G, D), BF),
                pltpu.VMEM((1, D, S2 * T), BF),
                pltpu.VMEM((AHEAD + 1, S2 * T, QB), F32),
                pltpu.SemaphoreType.DMA((HKV,)),
            ],
            compiler_params=pltpu.CompilerParams(vmem_limit_bytes=8 << 20),
        )(*parts)

    return jax.shard_map(local, mesh=mesh, in_specs=(spec, spec, spec), out_specs=spec, check_vma=False)
```

```python
import jax
import jax.numpy as jnp
from jax import lax
from jax.experimental import pallas as pl
from jax.experimental.pallas import tpu as pltpu
from jax.sharding import PartitionSpec as P

T = 256
HKV = 8
G = 8
D = 128
NB = 8
SUB = T // NB
QB = SUB * G
S1 = 6
S2 = 2
C = (D ** -0.5) * 1.4426950408889634
ORDER = (0, 2, 4, 6, 7, 5, 3, 1)
AHEAD = 4
U0, U1, U2 = 2, 2, 1
BF = jnp.bfloat16
F32 = jnp.float32
NT = (((1,), (1,)), ((), ()))


def chunks(n):
    return [(r, min(r + 256, n)) for r in range(0, n, 256)]


def by_tile(kv, h, s0, ns):
    return jnp.concatenate([kv[h, s, 1, t * SUB:(t + 1) * SUB] for t in range(NB) for s in range(s0, s0 + ns)], axis=0)


def fold(f, x):
    return f(x.reshape(-1, 8, x.shape[-1]), axis=0)


def attend(heads, kv, s0, ns, bias, qt, oacc, ml, vt, sref, arrive=None, first=False, out=None):
    rows = ns * SUB
    items = [(u, j) for u in range(len(heads)) for j in ORDER]
    tops = {}

    def scores(i, c):
        u, j = items[i]
        h = heads[u]
        r0, r1 = c
        if j == ORDER[0] and r0 == 0:
            if arrive:
                arrive(u)
            vt[u, :, :ns * T] = by_tile(kv, h, s0, ns).T
        parts = [kv[h, s0 + x % ns, 0, x // ns * SUB:(x // ns + 1) * SUB] for x in range(r0 // SUB, r1 // SUB)]
        s = lax.dot_general(jnp.concatenate(parts, axis=0), qt[h, j * SUB:(j + 1) * SUB].reshape(QB, D), NT,
                            preferred_element_type=F32)
        lo = max(r0, j * rows)
        if lo < r1:
            d = s[lo - r0:] + bias[lo - j * rows:r1 - j * rows]
            s = d if lo == r0 else jnp.concatenate([s[:lo - r0], d], axis=0)
        sref[i % (AHEAD + 1), r0:r1] = s
        m = fold(jnp.max, s)
        tops[i] = jnp.maximum(tops[i], m) if i in tops else m

    def values(i, c, m, acc):
        u, j = items[i]
        r0, r1 = c
        p = jnp.exp2((sref[i % (AHEAD + 1), r0:r1] - m) * C)
        l = fold(jnp.sum, p)
        o = jnp.dot(vt[u, :, r0:r1], p.astype(BF), preferred_element_type=F32)
        return (acc[0] + l, acc[1] + o) if acc else (l, o)

    def finish(i, m, a, l, o):
        u, j = items[i]
        h = heads[u]
        if not first:
            l = ml[h, j, 1:2] * a + l
        if out is None:
            oacc[h, j] = o if first else oacc[h, j] * a + o
            ml[h, j, 0:1] = m
            ml[h, j, 1:2] = l
            return
        r = 1.0 / l
        o = oacc[h, j] * (a * r) + o * r
        out(u)[j * SUB:(j + 1) * SUB] = o.T.astype(BF).reshape(SUB, G, D)

    todo = [(i, c) for i, (u, j) in enumerate(items) for c in chunks((j + 1) * rows)]
    total = len(todo)
    sizes = [len(chunks((j + 1) * rows)) for u, j in items]
    at = 0
    while at < total and todo[at][0] < AHEAD:
        scores(*todo[at])
        at += 1
    for i, (u, j) in enumerate(items):
        top = jnp.max(tops[i], axis=0, keepdims=True)
        m, a = top, None
        if not first:
            m1 = ml[heads[u], j, 0:1]
            m = jnp.maximum(top, m1)
            a = jnp.exp2((m1 - m) * C)
        acc = None
        goal = sum(sizes[:i + AHEAD + 1])
        start = at
        mine = chunks((j + 1) * rows)
        for t, c in enumerate(mine):
            upto = start + (goal - start) * (t + 1) // len(mine)
            while at < upto:
                scores(*todo[at])
                at += 1
            acc = values(i, c, m, acc)
        finish(i, m, a, jnp.sum(acc[0], axis=0, keepdims=True), acc[1])


def kernel(q_hbm, k_hbm, v_hbm, ob, qt, kv2, bias2, oacc, ml, raw, wide, kv1, vt, sref, bias0, bias1,
           lsem, qsem, ssem, rsem):
    cx, cy, cz = lax.axis_index("cx"), lax.axis_index("cy"), lax.axis_index("cz")
    me = (cx * 2 + cy) * 2 + cz
    nx = {"cy": 1 - cy}
    ny = {"cx": 1 - cx}
    sib = {"cz": 1 - cz}

    barrier = pltpu.get_barrier_semaphore()
    for dev in (nx, ny, sib):
        pl.semaphore_signal(barrier, inc=1, device_id=dev, device_id_type=pl.DeviceIdType.MESH)

    loads = [pltpu.make_async_copy(x, raw.at[i], lsem.at[i]) for i, x in enumerate((k_hbm, v_hbm))]
    for x in loads:
        x.start()

    def qload(h):
        return pltpu.make_async_copy(q_hbm.at[:, pl.ds(pl.multiple_of(h * G, G), G), :], qt.at[h], qsem.at[h])

    def rdma(kind, h):
        two = pl.ds(h if kind < 3 else 0, 2)
        src, dst, dev = (
            (kv1.at[two, 0], kv1.at[two, 2], nx),
            (kv1.at[two, 0], kv1.at[two, 4], ny),
            (kv1.at[two, 0], kv1.at[two, 1], sib),
            (kv1.at[h, 2], kv1.at[h, 3], sib),
            (kv1.at[h, 4], kv1.at[h, 5], sib),
            (kv1.at[h, 2, 0], kv2.at[h, 0, 0], ny),
            (kv1.at[h, 4, 1], kv2.at[h, 0, 1], nx),
            (kv2.at[h, 0], kv2.at[h, 1], sib),
        )[kind]
        return pltpu.make_async_remote_copy(src, dst, ssem.at[kind, h], rsem.at[kind, h], dev,
                                            pl.DeviceIdType.MESH)

    def mask(nslot, base, ref):
        r = lax.broadcasted_iota(jnp.int32, (nslot * SUB, QB), 0)
        c = lax.broadcasted_iota(jnp.int32, (nslot * SUB, QB), 1)
        kpos = (r % SUB) * 8 + (me ^ (r // SUB + base))
        qpos = (c // G) * 8 + me
        ref[...] = jnp.where(kpos <= qpos, 0.0, -1e30)

    for i in range(2):
        loads[i].wait()
        wide[i] = raw[i].astype(F32).reshape(T * HKV, D)

    def send(h):
        for kind in range(3):
            rdma(kind, h).start()

    for h in range(HKV):
        for i in range(2):
            kv1[h, 0, i] = wide[i, pl.ds(h, T, stride=HKV), :].astype(BF)
        if h == 2:
            pl.semaphore_wait(barrier, 3)
        if h and h % 2 == 0:
            send(h - 2)

    mask(2, 0, bias0)
    send(HKV - 2)

    @pl.loop(0, HKV)
    def _(h):
        qload(h).start()

    mask(4, 2, bias1)
    mask(2, 6, bias2)

    def pass_on(h):
        rdma(0, h).wait_recv()
        rdma(1, h).wait_recv()
        for u in range(2):
            for kind in (3, 4, 5, 6):
                rdma(kind, h + u).start()

    def pass_on2(h):
        rdma(5, h).wait_recv()
        rdma(6, h).wait_recv()
        rdma(7, h).start()

    @pl.loop(0, HKV // U0)
    def _(g):
        heads = [g * U0 + u for u in range(U0)]

        def arrive(u):
            h = heads[u]
            qload(h).wait()
            if u == 0:
                rdma(2, h).wait_recv()

        attend(heads, kv1, 0, 2, bias0, qt, oacc, ml, vt, sref, arrive, first=True)

    pass_on(0)

    @pl.loop(0, HKV // U1)
    def _(g):
        heads = [g * U1 + u for u in range(U1)]

        def arrive(u):
            h = heads[u]
            if u == 1:
                @pl.when(h < HKV - 1)
                def _():
                    pass_on(h + 1)

            rdma(3, h).wait_recv()
            rdma(4, h).wait_recv()

        attend(heads, kv1, 2, 4, bias1, qt, oacc, ml, vt, sref, arrive)

    pass_on2(0)

    @pl.loop(0, (HKV - 1) // U2)
    def _(g):
        heads = [g * U2 + u for u in range(U2)]

        def arrive(u):
            pass_on2(heads[u] + 1)
            rdma(7, heads[u]).wait_recv()

        attend(heads, kv2, 0, 2, bias2, qt, oacc, ml, vt, sref, arrive, out=lambda u: ob.at[heads[u]])

    rdma(7, HKV - 1).wait_recv()

    @pl.loop(0, HKV // 2)
    def _(g):
        for kind in range(3):
            rdma(kind, 2 * g).wait_send()

    @pl.loop(0, HKV)
    def _(h):
        for kind in range(3, 8):
            rdma(kind, h).wait_send()


def spread(ob, qt, kv2, bias2, oacc, ml, o_hbm, last, vt, sref, sem):
    def put(src, h):
        return pltpu.make_async_copy(src, o_hbm.at[:, pl.ds(pl.multiple_of(h * G, G), G), :], sem.at[h])

    @pl.loop(0, HKV - 1)
    def _(h):
        put(ob.at[h], h).start()

    attend([HKV - 1], kv2, 0, 2, bias2, qt, oacc, ml, vt, sref, out=lambda u: last)
    put(last, HKV - 1).start()

    @pl.loop(0, HKV - 1)
    def _(h):
        put(ob.at[h], h).wait()

    put(last, HKV - 1).wait()


def solution(mesh):
    spec = P(("dp", "cx", "cy", "cz"))

    def local(q, k, v):
        hbm = pl.BlockSpec(memory_space=pltpu.HBM)
        vmem = pl.BlockSpec(memory_space=pltpu.VMEM)
        parts = pl.pallas_call(
            kernel,
            out_shape=[
                pltpu.VMEM((HKV - 1, T, G, D), BF),
                pltpu.VMEM((HKV, T, G, D), BF),
                pltpu.VMEM((HKV, S2, 2, T, D), BF),
                pltpu.VMEM((S2 * SUB, QB), F32),
                pltpu.VMEM((HKV, NB, D, QB), F32),
                pltpu.VMEM((HKV, NB, 8, QB), F32),
            ],
            in_specs=[hbm] * 3,
            out_specs=[vmem] * 6,
            scratch_shapes=[
                pltpu.VMEM((2, T, HKV, D), BF),
                pltpu.VMEM((2, T * HKV, D), F32),
                pltpu.VMEM((HKV, S1, 2, T, D), BF),
                pltpu.VMEM((max(U0, U1, U2), D, 4 * T), BF),
                pltpu.VMEM((AHEAD + 1, 4 * T, QB), F32),
                pltpu.VMEM((2 * SUB, QB), F32),
                pltpu.VMEM((4 * SUB, QB), F32),
                pltpu.SemaphoreType.DMA((2,)),
                pltpu.SemaphoreType.DMA((HKV,)),
                pltpu.SemaphoreType.DMA((8, HKV)),
                pltpu.SemaphoreType.DMA((8, HKV)),
            ],
            compiler_params=pltpu.CompilerParams(
                vmem_limit_bytes=36 << 20, collective_id=0, has_side_effects=True),
        )(*(pltpu.with_memory_space_constraint(x, pltpu.HBM) for x in (q, k, v)))
        return pl.pallas_call(
            spread,
            out_shape=jax.ShapeDtypeStruct(q.shape, q.dtype),
            in_specs=[vmem] * 6,
            out_specs=hbm,
            scratch_shapes=[
                pltpu.VMEM((T, G, D), BF),
                pltpu.VMEM((1, D, S2 * T), BF),
                pltpu.VMEM((AHEAD + 1, S2 * T, QB), F32),
                pltpu.SemaphoreType.DMA((HKV,)),
            ],
            compiler_params=pltpu.CompilerParams(vmem_limit_bytes=8 << 20),
        )(*parts)

    return jax.shard_map(local, mesh=mesh, in_specs=(spec, spec, spec), out_specs=spec, check_vma=False)
```

```python
import jax
import jax.numpy as jnp
from jax import lax
from jax.experimental import pallas as pl
from jax.experimental.pallas import tpu as pltpu
from jax.sharding import PartitionSpec as P

T = 256
CUT = 160
HKV = 8
G = 8
D = 128
NB = 8
SUB = T // NB
QB = SUB * G
S1 = 6
S2 = 2
C = (D ** -0.5) * 1.4426950408889634
ORDER = (0, 2, 4, 6, 7, 5, 3, 1)
AHEAD = 4
HOOK = 4
U0, U1, U2 = 1, 1, 1
BF = jnp.bfloat16
F32 = jnp.float32
NT = (((1,), (1,)), ((), ()))


def chunks(n):
    return [(r, min(r + 256, n)) for r in range(0, n, 256)]


def by_tile(kv, h, s0, ns):
    return jnp.concatenate([kv[h, s, 1, t * SUB:(t + 1) * SUB] for t in range(NB) for s in range(s0, s0 + ns)], axis=0)


def fold(f, x):
    return f(x.reshape(-1, 8, x.shape[-1]), axis=0)


def attend(heads, kv, s0, ns, bias, qt, oacc, ml, vt, sref, arrive=None, first=False, out=None, hook=None):
    rows = ns * SUB
    items = [(u, j) for u in range(len(heads)) for j in ORDER]
    tops = {}

    def scores(i, c):
        u, j = items[i]
        h = heads[u]
        r0, r1 = c
        if j == ORDER[0] and r0 == 0:
            if arrive:
                arrive(u)
            vt[u, :, :ns * T] = by_tile(kv, h, s0, ns).T
        parts = [kv[h, s0 + x % ns, 0, x // ns * SUB:(x // ns + 1) * SUB] for x in range(r0 // SUB, r1 // SUB)]
        s = lax.dot_general(jnp.concatenate(parts, axis=0), qt[h, j * SUB:(j + 1) * SUB].reshape(QB, D), NT,
                            preferred_element_type=F32)
        lo = max(r0, j * rows)
        if lo < r1:
            d = s[lo - r0:] + bias[lo - j * rows:r1 - j * rows]
            s = d if lo == r0 else jnp.concatenate([s[:lo - r0], d], axis=0)
        sref[i % (AHEAD + 1), r0:r1] = s
        m = fold(jnp.max, s)
        tops[i] = jnp.maximum(tops[i], m) if i in tops else m

    def values(i, c, m, acc):
        u, j = items[i]
        r0, r1 = c
        p = jnp.exp2((sref[i % (AHEAD + 1), r0:r1] - m) * C)
        l = fold(jnp.sum, p)
        o = jnp.dot(vt[u, :, r0:r1], p.astype(BF), preferred_element_type=F32)
        return (acc[0] + l, acc[1] + o) if acc else (l, o)

    def finish(i, m, a, l, o):
        u, j = items[i]
        h = heads[u]
        if not first:
            l = ml[h, j, 1:2] * a + l
        if out is None:
            oacc[h, j] = o if first else oacc[h, j] * a + o
            ml[h, j, 0:1] = m
            ml[h, j, 1:2] = l
            return
        r = 1.0 / l
        o = oacc[h, j] * (a * r) + o * r
        out(u)[j * SUB:(j + 1) * SUB] = o.T.astype(BF).reshape(SUB, G, D)

    todo = [(i, c) for i, (u, j) in enumerate(items) for c in chunks((j + 1) * rows)]
    total = len(todo)
    sizes = [len(chunks((j + 1) * rows)) for u, j in items]
    at = 0
    while at < total and todo[at][0] < AHEAD:
        scores(*todo[at])
        at += 1
    for i, (u, j) in enumerate(items):
        if hook and i == HOOK:
            hook()
        top = jnp.max(tops[i], axis=0, keepdims=True)
        m, a = top, None
        if not first:
            m1 = ml[heads[u], j, 0:1]
            m = jnp.maximum(top, m1)
            a = jnp.exp2((m1 - m) * C)
        acc = None
        goal = sum(sizes[:i + AHEAD + 1])
        start = at
        mine = chunks((j + 1) * rows)
        for t, c in enumerate(mine):
            upto = start + (goal - start) * (t + 1) // len(mine)
            while at < upto:
                scores(*todo[at])
                at += 1
            acc = values(i, c, m, acc)
        finish(i, m, a, jnp.sum(acc[0], axis=0, keepdims=True), acc[1])


def kernel(q_hbm, k_hbm, v_hbm, ob, qt, kv2, bias2, oacc, ml, raw, wide, kv1, vt, sref, bias0, bias1,
           lsem, qsem, ssem, rsem, lssem, lrsem):
    cx, cy, cz = lax.axis_index("cx"), lax.axis_index("cy"), lax.axis_index("cz")
    me = (cx * 2 + cy) * 2 + cz
    nx = {"cy": 1 - cy}
    ny = {"cx": 1 - cx}
    sib = {"cz": 1 - cz}

    barrier = pltpu.get_barrier_semaphore()
    for dev in (nx, ny, sib):
        pl.semaphore_signal(barrier, inc=1, device_id=dev, device_id_type=pl.DeviceIdType.MESH)

    loads = [pltpu.make_async_copy(x, raw.at[i], lsem.at[i]) for i, x in enumerate((k_hbm, v_hbm))]
    for x in loads:
        x.start()

    def qload(h):
        return pltpu.make_async_copy(q_hbm.at[:, pl.ds(pl.multiple_of(h * G, G), G), :], qt.at[h], qsem.at[h])

    def rdma(kind, h, i=None):
        src, dst, dev = (
            (kv1.at[h, 0], kv1.at[h, 2], nx),
            (kv1.at[h, 0], kv1.at[h, 4], ny),
            (kv1.at[h, 0], kv1.at[h, 1], sib),
            (kv1.at[h, 2], kv1.at[h, 3], sib),
            (kv1.at[h, 4], kv1.at[h, 5], sib),
            (kv1.at[h, 2, 0], kv2.at[h, 0, 0], ny),
            (kv1.at[h, 4, 1], kv2.at[h, 0, 1], nx),
            (kv2.at[h, 0], kv2.at[h, 1], sib),
        )[kind]
        if i is not None:
            src, dst = src.at[i], dst.at[i]
        return pltpu.make_async_remote_copy(src, dst, ssem.at[kind, h], rsem.at[kind, h], dev,
                                            pl.DeviceIdType.MESH)

    def last(i, part):
        rows = pl.ds(0, CUT) if part == 0 else pl.ds(CUT, T - CUT)
        src = kv1.at[HKV - 1, (2, 4)[i], i, rows]
        dst = kv2.at[HKV - 1, 1 if part == 2 else 0, i, rows]
        dev = (ny, nx)[i] if part < 2 else ((ny, nx)[i] | sib)
        return pltpu.make_async_remote_copy(src, dst, lssem.at[i, part], lrsem.at[i, part], dev,
                                            pl.DeviceIdType.MESH)

    def last_relay():
        rows = pl.ds(0, CUT)
        return pltpu.make_async_remote_copy(kv2.at[HKV - 1, 0, :, rows], kv2.at[HKV - 1, 1, :, rows],
                                            ssem.at[7, HKV - 1], rsem.at[7, HKV - 1], sib, pl.DeviceIdType.MESH)

    def mask(nslot, base, ref):
        r = lax.broadcasted_iota(jnp.int32, (nslot * SUB, QB), 0)
        c = lax.broadcasted_iota(jnp.int32, (nslot * SUB, QB), 1)
        kpos = (r % SUB) * 8 + (me ^ (r // SUB + base))
        qpos = (c // G) * 8 + me
        ref[...] = jnp.where(kpos <= qpos, 0.0, -1e30)

    def relaid(h, i):
        kv1[h, 0, i] = wide[i, pl.ds(h, T, stride=HKV), :].astype(BF)

    def send(h):
        for kind in range(3):
            rdma(kind, h).start()

    for i in range(2):
        loads[i].wait()
        wide[i] = raw[i].astype(F32).reshape(T * HKV, D)
        relaid(0, i)
        relaid(1, i)
        if i == 0:
            pl.semaphore_wait(barrier, 3)
        for kind in range(3):
            rdma(kind, 0, i).start()

    for h in range(2, HKV):
        for i in range(2):
            relaid(h, i)
        send(h - 1)

    mask(2, 0, bias0)
    send(HKV - 1)

    @pl.loop(0, HKV)
    def _(h):
        qload(h).start()

    mask(4, 2, bias1)
    mask(2, 6, bias2)

    def pass_on(h):
        rdma(0, h).wait_recv()
        rdma(1, h).wait_recv()
        for kind in (3, 4):
            rdma(kind, h).start()

        @pl.when(h < HKV - 1)
        def _():
            for kind in (5, 6):
                rdma(kind, h).start()

        @pl.when(h == HKV - 1)
        def _():
            for part in range(3):
                for i in range(2):
                    last(i, part).start()

    def pass_on2(h):
        @pl.when(h < HKV - 1)
        def _():
            rdma(5, h).wait_recv()
            rdma(6, h).wait_recv()
            rdma(7, h).start()

        @pl.when(h == HKV - 1)
        def _():
            for i in range(2):
                last(i, 0).wait_recv()
            last_relay().start()

    @pl.loop(0, HKV // U0)
    def _(g):
        heads = [g * U0 + u for u in range(U0)]

        def arrive(u):
            h = heads[u]
            qload(h).wait()
            rdma(2, h).wait_recv()

        attend(heads, kv1, 0, 2, bias0, qt, oacc, ml, vt, sref, arrive, first=True)

    pass_on(jnp.int32(0))

    @pl.loop(0, HKV - 1)
    def _(h):
        pass_on(h + 1)
        rdma(3, h).wait_recv()
        rdma(4, h).wait_recv()
        attend([h], kv1, 2, 4, bias1, qt, oacc, ml, vt, sref)

    rdma(3, HKV - 1).wait_recv()
    rdma(4, HKV - 1).wait_recv()
    attend([HKV - 1], kv1, 2, 4, bias1, qt, oacc, ml, vt, sref, hook=lambda: pass_on2(jnp.int32(0)))

    @pl.loop(0, (HKV - 1) // U2)
    def _(g):
        heads = [g * U2 + u for u in range(U2)]

        def arrive(u):
            pass_on2(heads[u] + 1)
            rdma(7, heads[u]).wait_recv()

        attend(heads, kv2, 0, 2, bias2, qt, oacc, ml, vt, sref, arrive, out=lambda u: ob.at[heads[u]])

    for part in (1, 2):
        for i in range(2):
            last(i, part).wait_recv()
    last_relay().wait_recv()

    @pl.loop(0, HKV)
    def _(h):
        for kind in range(5):
            rdma(kind, h).wait_send()

    @pl.loop(0, HKV - 1)
    def _(h):
        for kind in range(5, 8):
            rdma(kind, h).wait_send()

    for part in range(3):
        for i in range(2):
            last(i, part).wait_send()
    last_relay().wait_send()


def spread(ob, qt, kv2, bias2, oacc, ml, o_hbm, last, vt, sref, sem):
    def put(src, h):
        return pltpu.make_async_copy(src, o_hbm.at[:, pl.ds(pl.multiple_of(h * G, G), G), :], sem.at[h])

    @pl.loop(0, HKV - 1)
    def _(h):
        put(ob.at[h], h).start()

    attend([HKV - 1], kv2, 0, 2, bias2, qt, oacc, ml, vt, sref, out=lambda u: last)
    put(last, HKV - 1).start()

    @pl.loop(0, HKV - 1)
    def _(h):
        put(ob.at[h], h).wait()

    put(last, HKV - 1).wait()


def solution(mesh):
    spec = P(("dp", "cx", "cy", "cz"))

    def local(q, k, v):
        hbm = pl.BlockSpec(memory_space=pltpu.HBM)
        vmem = pl.BlockSpec(memory_space=pltpu.VMEM)
        parts = pl.pallas_call(
            kernel,
            out_shape=[
                pltpu.VMEM((HKV - 1, T, G, D), BF),
                pltpu.VMEM((HKV, T, G, D), BF),
                pltpu.VMEM((HKV, S2, 2, T, D), BF),
                pltpu.VMEM((S2 * SUB, QB), F32),
                pltpu.VMEM((HKV, NB, D, QB), F32),
                pltpu.VMEM((HKV, NB, 8, QB), F32),
            ],
            in_specs=[hbm] * 3,
            out_specs=[vmem] * 6,
            scratch_shapes=[
                pltpu.VMEM((2, T, HKV, D), BF),
                pltpu.VMEM((2, T * HKV, D), F32),
                pltpu.VMEM((HKV, S1, 2, T, D), BF),
                pltpu.VMEM((max(U0, U1, U2), D, 4 * T), BF),
                pltpu.VMEM((AHEAD + 1, 4 * T, QB), F32),
                pltpu.VMEM((2 * SUB, QB), F32),
                pltpu.VMEM((4 * SUB, QB), F32),
                pltpu.SemaphoreType.DMA((2,)),
                pltpu.SemaphoreType.DMA((HKV,)),
                pltpu.SemaphoreType.DMA((8, HKV)),
                pltpu.SemaphoreType.DMA((8, HKV)),
                pltpu.SemaphoreType.DMA((2, 3)),
                pltpu.SemaphoreType.DMA((2, 3)),
            ],
            compiler_params=pltpu.CompilerParams(
                vmem_limit_bytes=36 << 20, collective_id=0, has_side_effects=True),
        )(*(pltpu.with_memory_space_constraint(x, pltpu.HBM) for x in (q, k, v)))
        return pl.pallas_call(
            spread,
            out_shape=jax.ShapeDtypeStruct(q.shape, q.dtype),
            in_specs=[vmem] * 6,
            out_specs=hbm,
            scratch_shapes=[
                pltpu.VMEM((T, G, D), BF),
                pltpu.VMEM((1, D, S2 * T), BF),
                pltpu.VMEM((AHEAD + 1, S2 * T, QB), F32),
                pltpu.SemaphoreType.DMA((HKV,)),
            ],
            compiler_params=pltpu.CompilerParams(vmem_limit_bytes=8 << 20),
        )(*parts)

    return jax.shard_map(local, mesh=mesh, in_specs=(spec, spec, spec), out_specs=spec, check_vma=False)
```

```python
import jax
import jax.numpy as jnp
from jax import lax
from jax.experimental import pallas as pl
from jax.experimental.pallas import tpu as pltpu
from jax.sharding import PartitionSpec as P

T = 256
HKV = 8
G = 8
D = 128
NB = 8
SUB = T // NB
QB = SUB * G
S1 = 6
S2 = 2
C = (D ** -0.5) * 1.4426950408889634
ORDER = (0, 2, 4, 6, 7, 5, 3, 1)
AHEAD = 4
HOOK = 4
U0, U1, U2 = 1, 1, 1
BF = jnp.bfloat16
F32 = jnp.float32
NT = (((1,), (1,)), ((), ()))


def chunks(n):
    return [(r, min(r + 256, n)) for r in range(0, n, 256)]


def by_tile(piece, kind, ns):
    return jnp.concatenate([piece(kind, x, t) for t in range(NB) for x in range(ns)], axis=0)


def fold(f, x):
    return f(x.reshape(-1, 8, x.shape[-1]), axis=0)


def attend(heads, piece_of, ns, bias, qt, oacc, ml, vt, sref, arrive=None, first=False, out=None, hook=None):
    rows = ns * SUB
    items = [(u, j) for u in range(len(heads)) for j in ORDER]
    tops = {}

    def scores(i, c):
        u, j = items[i]
        h = heads[u]
        r0, r1 = c
        if j == ORDER[0] and r0 == 0:
            if arrive:
                arrive(u)
            vt[u, :, :ns * T] = by_tile(piece_of(h), 1, ns).T
        parts = [piece_of(h)(0, x % ns, x // ns) for x in range(r0 // SUB, r1 // SUB)]
        s = lax.dot_general(jnp.concatenate(parts, axis=0), qt[h, j * SUB:(j + 1) * SUB].reshape(QB, D), NT,
                            preferred_element_type=F32)
        lo = max(r0, j * rows)
        if lo < r1:
            d = s[lo - r0:] + bias[lo - j * rows:r1 - j * rows]
            s = d if lo == r0 else jnp.concatenate([s[:lo - r0], d], axis=0)
        sref[i % (AHEAD + 1), r0:r1] = s
        m = fold(jnp.max, s)
        tops[i] = jnp.maximum(tops[i], m) if i in tops else m

    def values(i, c, m, acc):
        u, j = items[i]
        r0, r1 = c
        p = jnp.exp2((sref[i % (AHEAD + 1), r0:r1] - m) * C)
        l = fold(jnp.sum, p)
        o = jnp.dot(vt[u, :, r0:r1], p.astype(BF), preferred_element_type=F32)
        return (acc[0] + l, acc[1] + o) if acc else (l, o)

    def finish(i, m, a, l, o):
        u, j = items[i]
        h = heads[u]
        if not first:
            l = ml[h, j, 1:2] * a + l
        if out is None:
            oacc[h, j] = o if first else oacc[h, j] * a + o
            ml[h, j, 0:1] = m
            ml[h, j, 1:2] = l
            return
        r = 1.0 / l
        o = oacc[h, j] * (a * r) + o * r
        out(u)[j * SUB:(j + 1) * SUB] = o.T.astype(BF).reshape(SUB, G, D)

    todo = [(i, c) for i, (u, j) in enumerate(items) for c in chunks((j + 1) * rows)]
    total = len(todo)
    sizes = [len(chunks((j + 1) * rows)) for u, j in items]
    at = 0
    while at < total and todo[at][0] < AHEAD:
        scores(*todo[at])
        at += 1
    for i, (u, j) in enumerate(items):
        if hook and i == HOOK:
            hook()
        top = jnp.max(tops[i], axis=0, keepdims=True)
        m, a = top, None
        if not first:
            m1 = ml[heads[u], j, 0:1]
            m = jnp.maximum(top, m1)
            a = jnp.exp2((m1 - m) * C)
        acc = None
        goal = sum(sizes[:i + AHEAD + 1])
        start = at
        mine = chunks((j + 1) * rows)
        for t, c in enumerate(mine):
            upto = start + (goal - start) * (t + 1) // len(mine)
            while at < upto:
                scores(*todo[at])
                at += 1
            acc = values(i, c, m, acc)
        finish(i, m, a, jnp.sum(acc[0], axis=0, keepdims=True), acc[1])


def near(kv1, chip):
    def of(h):
        return lambda kind, x, t: kv1[h, kind, chip + x // 2, x % 2, t * SUB:(t + 1) * SUB]
    return of


def far(kv2):
    def of(h):
        return lambda kind, x, t: kv2[h, kind, x, t * SUB:(t + 1) * SUB]
    return of


def kernel(q_hbm, k_hbm, v_hbm, ob, qt, kv2, bias2, oacc, ml, raw, wide, kv1, vt, sref, bias0, bias1,
           lsem, qsem, ssem, rsem, lssem, lrsem):
    cx, cy, cz = lax.axis_index("cx"), lax.axis_index("cy"), lax.axis_index("cz")
    me = (cx * 2 + cy) * 2 + cz
    chip = cx * 2 + cy
    mine = 1 - cz

    def over(core):
        return {"cx": cx + cz - 2 * cx * cz, "cy": cy + mine - 2 * cy * mine, "cz": core}

    sib = {"cz": 1 - cz}

    barrier = pltpu.get_barrier_semaphore()
    for dev in ({"cx": cx, "cy": 1 - cy, "cz": 0}, {"cx": 1 - cx, "cy": cy, "cz": 1}, sib):
        pl.semaphore_signal(barrier, inc=1, device_id=dev, device_id_type=pl.DeviceIdType.MESH)

    loads = [pltpu.make_async_copy(x, raw.at[i], lsem.at[i]) for i, x in enumerate((k_hbm, v_hbm))]
    for x in loads:
        x.start()

    def qload(h):
        return pltpu.make_async_copy(q_hbm.at[:, pl.ds(pl.multiple_of(h * G, G), G), :], qt.at[h], qsem.at[h])

    def rdma(src, dst, send, recv, h, dev):
        return pltpu.make_async_remote_copy(src, dst, ssem.at[send, h], rsem.at[recv, h], dev,
                                            pl.DeviceIdType.MESH)

    def swap(h):
        return rdma(kv1.at[h, :, 0, cz], kv1.at[h, :, 0, cz], 0, 5, h, sib)

    def out_k(h):
        return rdma(kv1.at[h, 0, 0], kv1.at[h, 0, 1 + cz], 1, cz, h, over(1))

    def out_v(h):
        return rdma(kv1.at[h, 1, 0], kv1.at[h, 1, 1 + cz], 2, cz, h, over(0))

    def half(h, i, z):
        return rdma(kv1.at[h, i, 0, z], kv1.at[h, i, 1 + cz, z], 1 + i, cz, h, over(1 - i))

    def relay(h):
        return rdma(kv1.at[h, mine, 1:3], kv1.at[h, mine, 1:3], 3, 2, h, sib)

    def forward(h):
        return rdma(kv1.at[h, mine, 2 - cz], kv2.at[h, mine], 4, 3, h, over(cz))

    def last(part):
        z = 0 if part == 0 else 1
        return pltpu.make_async_remote_copy(kv1.at[HKV - 1, mine, 2 - cz, z], kv2.at[HKV - 1, mine, z],
                                            lssem.at[part], lrsem.at[part], over(1 - cz if part == 2 else cz),
                                            pl.DeviceIdType.MESH)

    def last_relay():
        return rdma(kv2.at[HKV - 1, mine, 0], kv2.at[HKV - 1, mine, 0], 5, 4, HKV - 1, sib)

    def relay2(h):
        return rdma(kv2.at[h, mine], kv2.at[h, mine], 5, 4, h, sib)

    def arrived(dst, recv, h):
        rdma(dst, dst, 0, recv, h, sib).wait_recv()

    def mask(nslot, far_chip, ref):
        r = lax.broadcasted_iota(jnp.int32, (nslot * SUB, QB), 0)
        c = lax.broadcasted_iota(jnp.int32, (nslot * SUB, QB), 1)
        x = r // SUB
        kpos = (r % SUB) * 8 + (chip ^ (x // 2 + far_chip)) * 2 + x % 2
        qpos = (c // G) * 8 + me
        ref[...] = jnp.where(kpos <= qpos, 0.0, -1e30)

    def relaid(h, i):
        kv1[h, i, 0, cz] = wide[i, pl.ds(h, T, stride=HKV), :].astype(BF)

    for i in range(2):
        loads[i].wait()
        wide[i] = raw[i].astype(F32).reshape(T * HKV, D)
        relaid(0, i)
        relaid(1, i)
        if i == 0:
            pl.semaphore_wait(barrier, 3)
        half(0, i, cz).start()
    swap(0).start()

    for h in range(2, HKV):
        for i in range(2):
            relaid(h, i)
        if h == 2:
            for i in range(2):
                half(1, i, cz).start()
        swap(h - 1).start()

    mask(2, 0, bias0)
    swap(HKV - 1).start()

    for h in range(2):
        arrived(kv1.at[h, :, 0, cz], 5, h)
        for i in range(2):
            half(h, i, 1 - cz).start()

    @pl.loop(2, HKV)
    def _(h):
        arrived(kv1.at[h, :, 0, cz], 5, h)
        out_k(h).start()
        out_v(h).start()

    @pl.loop(0, HKV)
    def _(h):
        qload(h).start()

    mask(4, 1, bias1)
    mask(2, 3, bias2)

    def pass_on(h):
        arrived(kv1.at[h, mine, 1], 0, h)
        arrived(kv1.at[h, mine, 2], 1, h)
        relay(h).start()

        @pl.when(h < HKV - 1)
        def _():
            forward(h).start()

        @pl.when(h == HKV - 1)
        def _():
            for part in range(3):
                last(part).start()

    def pass_on2(h):
        @pl.when(h < HKV - 1)
        def _():
            arrived(kv2.at[h, mine], 3, h)
            relay2(h).start()

        @pl.when(h == HKV - 1)
        def _():
            last(0).wait_recv()
            last_relay().start()

    @pl.loop(0, HKV // U0)
    def _(g):
        heads = [g * U0 + u for u in range(U0)]

        def arrive(u):
            h = heads[u]
            qload(h).wait()

        attend(heads, near(kv1, 0), 2, bias0, qt, oacc, ml, vt, sref, arrive, first=True)

    pass_on(jnp.int32(0))

    @pl.loop(0, HKV - 1)
    def _(h):
        pass_on(h + 1)
        arrived(kv1.at[h, cz, 1:3], 2, h)
        attend([h], near(kv1, 1), 4, bias1, qt, oacc, ml, vt, sref)

    arrived(kv1.at[HKV - 1, cz, 1:3], 2, HKV - 1)
    attend([HKV - 1], near(kv1, 1), 4, bias1, qt, oacc, ml, vt, sref, hook=lambda: pass_on2(jnp.int32(0)))

    @pl.loop(0, (HKV - 1) // U2)
    def _(g):
        heads = [g * U2 + u for u in range(U2)]

        def arrive(u):
            pass_on2(heads[u] + 1)
            arrived(kv2.at[heads[u], cz], 4, heads[u])

        attend(heads, far(kv2), 2, bias2, qt, oacc, ml, vt, sref, arrive, out=lambda u: ob.at[heads[u]])

    for part in (1, 2):
        last(part).wait_recv()
    last_relay().wait_recv()

    @pl.loop(0, HKV)
    def _(h):
        for sent in (swap, out_k, out_v, relay):
            sent(h).wait_send()

    @pl.loop(0, HKV - 1)
    def _(h):
        forward(h).wait_send()
        relay2(h).wait_send()

    for part in range(3):
        last(part).wait_send()
    last_relay().wait_send()


def spread(ob, qt, kv2, bias2, oacc, ml, o_hbm, last, vt, sref, sem):
    def put(src, h):
        return pltpu.make_async_copy(src, o_hbm.at[:, pl.ds(pl.multiple_of(h * G, G), G), :], sem.at[h])

    @pl.loop(0, HKV - 1)
    def _(h):
        put(ob.at[h], h).start()

    attend([HKV - 1], far(kv2), 2, bias2, qt, oacc, ml, vt, sref, out=lambda u: last)
    put(last, HKV - 1).start()

    @pl.loop(0, HKV - 1)
    def _(h):
        put(ob.at[h], h).wait()

    put(last, HKV - 1).wait()


def solution(mesh):
    spec = P(("dp", "cx", "cy", "cz"))

    def local(q, k, v):
        hbm = pl.BlockSpec(memory_space=pltpu.HBM)
        vmem = pl.BlockSpec(memory_space=pltpu.VMEM)
        parts = pl.pallas_call(
            kernel,
            out_shape=[
                pltpu.VMEM((HKV - 1, T, G, D), BF),
                pltpu.VMEM((HKV, T, G, D), BF),
                pltpu.VMEM((HKV, 2, 2, T, D), BF),
                pltpu.VMEM((S2 * SUB, QB), F32),
                pltpu.VMEM((HKV, NB, D, QB), F32),
                pltpu.VMEM((HKV, NB, 8, QB), F32),
            ],
            in_specs=[hbm] * 3,
            out_specs=[vmem] * 6,
            scratch_shapes=[
                pltpu.VMEM((2, T, HKV, D), BF),
                pltpu.VMEM((2, T * HKV, D), F32),
                pltpu.VMEM((HKV, 2, 3, 2, T, D), BF),
                pltpu.VMEM((max(U0, U1, U2), D, 4 * T), BF),
                pltpu.VMEM((AHEAD + 1, 4 * T, QB), F32),
                pltpu.VMEM((2 * SUB, QB), F32),
                pltpu.VMEM((4 * SUB, QB), F32),
                pltpu.SemaphoreType.DMA((2,)),
                pltpu.SemaphoreType.DMA((HKV,)),
                pltpu.SemaphoreType.DMA((6, HKV)),
                pltpu.SemaphoreType.DMA((6, HKV)),
                pltpu.SemaphoreType.DMA((3,)),
                pltpu.SemaphoreType.DMA((3,)),
            ],
            compiler_params=pltpu.CompilerParams(
                vmem_limit_bytes=36 << 20, collective_id=0, has_side_effects=True),
        )(*(pltpu.with_memory_space_constraint(x, pltpu.HBM) for x in (q, k, v)))
        return pl.pallas_call(
            spread,
            out_shape=jax.ShapeDtypeStruct(q.shape, q.dtype),
            in_specs=[vmem] * 6,
            out_specs=hbm,
            scratch_shapes=[
                pltpu.VMEM((T, G, D), BF),
                pltpu.VMEM((1, D, S2 * T), BF),
                pltpu.VMEM((AHEAD + 1, S2 * T, QB), F32),
                pltpu.SemaphoreType.DMA((HKV,)),
            ],
            compiler_params=pltpu.CompilerParams(vmem_limit_bytes=8 << 20),
        )(*parts)

    return jax.shard_map(local, mesh=mesh, in_specs=(spec, spec, spec), out_specs=spec, check_vma=False)
```

```python
import jax
import jax.numpy as jnp
from jax import lax
from jax.experimental import pallas as pl
from jax.experimental.pallas import tpu as pltpu
from jax.sharding import PartitionSpec as P

T = 256
HKV = 8
G = 8
D = 128
NB = 8
SUB = T // NB
QB = SUB * G
S1 = 6
S2 = 2
C = (D ** -0.5) * 1.4426950408889634
ORDER = (0, 2, 4, 6, 7, 5, 3, 1)
AHEAD = 4
HOOK = 4
U0, U1, U2 = 1, 1, 1
BF = jnp.bfloat16
F32 = jnp.float32
NT = (((1,), (1,)), ((), ()))


def chunks(n):
    return [(r, min(r + 256, n)) for r in range(0, n, 256)]


def by_tile(piece, kind, ns):
    return jnp.concatenate([piece(kind, x, t) for t in range(NB) for x in range(ns)], axis=0)


def fold(f, x):
    return f(x.reshape(-1, 8, x.shape[-1]), axis=0)


def attend(heads, piece_of, ns, bias, qt, oacc, ml, vt, sref, arrive=None, first=False, out=None, hook=None):
    rows = ns * SUB
    items = [(u, j) for u in range(len(heads)) for j in ORDER]
    tops = {}

    def scores(i, c):
        u, j = items[i]
        h = heads[u]
        r0, r1 = c
        if j == ORDER[0] and r0 == 0:
            if arrive:
                arrive(u)
            vt[u, :, :ns * T] = by_tile(piece_of(h), 1, ns).T
        parts = [piece_of(h)(0, x % ns, x // ns) for x in range(r0 // SUB, r1 // SUB)]
        s = lax.dot_general(jnp.concatenate(parts, axis=0), qt[h, j * SUB:(j + 1) * SUB].reshape(QB, D), NT,
                            preferred_element_type=F32)
        lo = max(r0, j * rows)
        if lo < r1:
            d = s[lo - r0:] + bias[lo - j * rows:r1 - j * rows]
            s = d if lo == r0 else jnp.concatenate([s[:lo - r0], d], axis=0)
        sref[i % (AHEAD + 1), r0:r1] = s
        m = fold(jnp.max, s)
        tops[i] = jnp.maximum(tops[i], m) if i in tops else m

    def values(i, c, m, acc):
        u, j = items[i]
        r0, r1 = c
        p = jnp.exp2((sref[i % (AHEAD + 1), r0:r1] - m) * C)
        l = fold(jnp.sum, p)
        o = jnp.dot(vt[u, :, r0:r1], p.astype(BF), preferred_element_type=F32)
        return (acc[0] + l, acc[1] + o) if acc else (l, o)

    def finish(i, m, a, l, o):
        u, j = items[i]
        h = heads[u]
        if not first:
            l = ml[h, j, 1:2] * a + l
        if out is None:
            oacc[h, j] = o if first else oacc[h, j] * a + o
            ml[h, j, 0:1] = m
            ml[h, j, 1:2] = l
            return
        r = 1.0 / l
        o = oacc[h, j] * (a * r) + o * r
        out(u)[j * SUB:(j + 1) * SUB] = o.T.astype(BF).reshape(SUB, G, D)

    todo = [(i, c) for i, (u, j) in enumerate(items) for c in chunks((j + 1) * rows)]
    total = len(todo)
    sizes = [len(chunks((j + 1) * rows)) for u, j in items]
    at = 0
    while at < total and todo[at][0] < AHEAD:
        scores(*todo[at])
        at += 1
    for i, (u, j) in enumerate(items):
        if hook and i == HOOK:
            hook()
        top = jnp.max(tops[i], axis=0, keepdims=True)
        m, a = top, None
        if not first:
            m1 = ml[heads[u], j, 0:1]
            m = jnp.maximum(top, m1)
            a = jnp.exp2((m1 - m) * C)
        acc = None
        goal = sum(sizes[:i + AHEAD + 1])
        start = at
        mine = chunks((j + 1) * rows)
        for t, c in enumerate(mine):
            upto = start + (goal - start) * (t + 1) // len(mine)
            while at < upto:
                scores(*todo[at])
                at += 1
            acc = values(i, c, m, acc)
        finish(i, m, a, jnp.sum(acc[0], axis=0, keepdims=True), acc[1])


def near(kv1, chip):
    def of(h):
        return lambda kind, x, t: kv1[h, kind, chip + x // 2, x % 2, t * SUB:(t + 1) * SUB]
    return of


def far(kv2):
    def of(h):
        return lambda kind, x, t: kv2[h, kind, x, t * SUB:(t + 1) * SUB]
    return of


def kernel(q_hbm, k_hbm, v_hbm, ob, qt, kv2, bias2, oacc, ml, raw, wide, kv1, vt, sref, bias0, bias1,
           lsem, qsem, ssem, rsem, lssem, lrsem):
    cx, cy, cz = lax.axis_index("cx"), lax.axis_index("cy"), lax.axis_index("cz")
    me = (cx * 2 + cy) * 2 + cz
    chip = cx * 2 + cy
    link = 1 - (cx + cz - 2 * cx * cz)
    mine = 1 - link

    def over(role):
        x = cx + link - 2 * cx * link
        y = cy + mine - 2 * cy * mine
        return {"cx": x, "cy": y, "cz": x + (1 - role) - 2 * x * (1 - role)}

    sib = {"cz": 1 - cz}

    barrier = pltpu.get_barrier_semaphore()
    for dev in ({"cy": 1 - cy, "cz": 1 - cx}, {"cx": 1 - cx, "cz": 1 - cx}, sib):
        pl.semaphore_signal(barrier, inc=1, device_id=dev, device_id_type=pl.DeviceIdType.MESH)

    loads = [pltpu.make_async_copy(x, raw.at[i], lsem.at[i]) for i, x in enumerate((k_hbm, v_hbm))]
    for x in loads:
        x.start()

    def qload(h):
        return pltpu.make_async_copy(q_hbm.at[:, pl.ds(pl.multiple_of(h * G, G), G), :], qt.at[h], qsem.at[h])

    def rdma(src, dst, send, recv, h, dev):
        return pltpu.make_async_remote_copy(src, dst, ssem.at[send, h], rsem.at[recv, h], dev,
                                            pl.DeviceIdType.MESH)

    def swap(h):
        return rdma(kv1.at[h, :, 0, cz], kv1.at[h, :, 0, cz], 0, 5, h, sib)

    def out_k(h):
        return rdma(kv1.at[h, 0, 0], kv1.at[h, 0, 1 + link], 1, link, h, over(1))

    def out_v(h):
        return rdma(kv1.at[h, 1, 0], kv1.at[h, 1, 1 + link], 2, link, h, over(0))

    def half(h, i, z):
        return rdma(kv1.at[h, i, 0, z], kv1.at[h, i, 1 + link, z], 1 + i, link, h, over(1 - i))

    def relay(h):
        return rdma(kv1.at[h, mine, 1:3], kv1.at[h, mine, 1:3], 3, 2, h, sib)

    def forward(h):
        return rdma(kv1.at[h, mine, 2 - link], kv2.at[h, mine], 4, 3, h, over(link))

    def last(part):
        z = 0 if part == 0 else 1
        return pltpu.make_async_remote_copy(kv1.at[HKV - 1, mine, 2 - link, z], kv2.at[HKV - 1, mine, z],
                                            lssem.at[part], lrsem.at[part], over(mine if part == 2 else link),
                                            pl.DeviceIdType.MESH)

    def last_relay():
        return rdma(kv2.at[HKV - 1, mine, 0], kv2.at[HKV - 1, mine, 0], 5, 4, HKV - 1, sib)

    def relay2(h):
        return rdma(kv2.at[h, mine], kv2.at[h, mine], 5, 4, h, sib)

    def arrived(dst, recv, h):
        rdma(dst, dst, 0, recv, h, sib).wait_recv()

    def mask(nslot, far_chip, ref):
        r = lax.broadcasted_iota(jnp.int32, (nslot * SUB, QB), 0)
        c = lax.broadcasted_iota(jnp.int32, (nslot * SUB, QB), 1)
        x = r // SUB
        kpos = (r % SUB) * 8 + (chip ^ (x // 2 + far_chip)) * 2 + x % 2
        qpos = (c // G) * 8 + me
        ref[...] = jnp.where(kpos <= qpos, 0.0, -1e30)

    def relaid(h, i):
        kv1[h, i, 0, cz] = wide[i, pl.ds(h, T, stride=HKV), :].astype(BF)

    for i in range(2):
        loads[i].wait()
        wide[i] = raw[i].astype(F32).reshape(T * HKV, D)
        relaid(0, i)
        relaid(1, i)
        if i == 0:
            pl.semaphore_wait(barrier, 3)
        half(0, i, cz).start()
    swap(0).start()

    for h in range(2, HKV):
        for i in range(2):
            relaid(h, i)
        if h == 2:
            for i in range(2):
                half(1, i, cz).start()
        swap(h - 1).start()

    mask(2, 0, bias0)
    swap(HKV - 1).start()

    for h in range(2):
        arrived(kv1.at[h, :, 0, cz], 5, h)
        for i in range(2):
            half(h, i, 1 - cz).start()

    @pl.loop(2, HKV)
    def _(h):
        arrived(kv1.at[h, :, 0, cz], 5, h)
        out_k(h).start()
        out_v(h).start()

    @pl.loop(0, HKV)
    def _(h):
        qload(h).start()

    mask(4, 1, bias1)
    mask(2, 3, bias2)

    def pass_on(h):
        arrived(kv1.at[h, mine, 1], 0, h)
        arrived(kv1.at[h, mine, 2], 1, h)
        relay(h).start()

        @pl.when(h < HKV - 1)
        def _():
            forward(h).start()

        @pl.when(h == HKV - 1)
        def _():
            for part in range(3):
                last(part).start()

    def pass_on2(h):
        @pl.when(h < HKV - 1)
        def _():
            arrived(kv2.at[h, mine], 3, h)
            relay2(h).start()

        @pl.when(h == HKV - 1)
        def _():
            last(0).wait_recv()
            last_relay().start()

    @pl.loop(0, HKV // U0)
    def _(g):
        heads = [g * U0 + u for u in range(U0)]

        def arrive(u):
            h = heads[u]
            qload(h).wait()

        attend(heads, near(kv1, 0), 2, bias0, qt, oacc, ml, vt, sref, arrive, first=True)

    pass_on(jnp.int32(0))

    @pl.loop(0, HKV - 1)
    def _(h):
        pass_on(h + 1)
        arrived(kv1.at[h, link, 1:3], 2, h)
        attend([h], near(kv1, 1), 4, bias1, qt, oacc, ml, vt, sref)

    arrived(kv1.at[HKV - 1, link, 1:3], 2, HKV - 1)
    attend([HKV - 1], near(kv1, 1), 4, bias1, qt, oacc, ml, vt, sref, hook=lambda: pass_on2(jnp.int32(0)))

    @pl.loop(0, (HKV - 1) // U2)
    def _(g):
        heads = [g * U2 + u for u in range(U2)]

        def arrive(u):
            pass_on2(heads[u] + 1)
            arrived(kv2.at[heads[u], link], 4, heads[u])

        attend(heads, far(kv2), 2, bias2, qt, oacc, ml, vt, sref, arrive, out=lambda u: ob.at[heads[u]])

    for part in (1, 2):
        last(part).wait_recv()
    last_relay().wait_recv()

    @pl.loop(0, HKV)
    def _(h):
        for sent in (swap, out_k, out_v, relay):
            sent(h).wait_send()

    @pl.loop(0, HKV - 1)
    def _(h):
        forward(h).wait_send()
        relay2(h).wait_send()

    for part in range(3):
        last(part).wait_send()
    last_relay().wait_send()


def spread(ob, qt, kv2, bias2, oacc, ml, o_hbm, last, vt, sref, sem):
    def put(src, h):
        return pltpu.make_async_copy(src, o_hbm.at[:, pl.ds(pl.multiple_of(h * G, G), G), :], sem.at[h])

    @pl.loop(0, HKV - 1)
    def _(h):
        put(ob.at[h], h).start()

    attend([HKV - 1], far(kv2), 2, bias2, qt, oacc, ml, vt, sref, out=lambda u: last)
    put(last, HKV - 1).start()

    @pl.loop(0, HKV - 1)
    def _(h):
        put(ob.at[h], h).wait()

    put(last, HKV - 1).wait()


def solution(mesh):
    spec = P(("dp", "cx", "cy", "cz"))

    def local(q, k, v):
        hbm = pl.BlockSpec(memory_space=pltpu.HBM)
        vmem = pl.BlockSpec(memory_space=pltpu.VMEM)
        parts = pl.pallas_call(
            kernel,
            out_shape=[
                pltpu.VMEM((HKV - 1, T, G, D), BF),
                pltpu.VMEM((HKV, T, G, D), BF),
                pltpu.VMEM((HKV, 2, 2, T, D), BF),
                pltpu.VMEM((S2 * SUB, QB), F32),
                pltpu.VMEM((HKV, NB, D, QB), F32),
                pltpu.VMEM((HKV, NB, 8, QB), F32),
            ],
            in_specs=[hbm] * 3,
            out_specs=[vmem] * 6,
            scratch_shapes=[
                pltpu.VMEM((2, T, HKV, D), BF),
                pltpu.VMEM((2, T * HKV, D), F32),
                pltpu.VMEM((HKV, 2, 3, 2, T, D), BF),
                pltpu.VMEM((max(U0, U1, U2), D, 4 * T), BF),
                pltpu.VMEM((AHEAD + 1, 4 * T, QB), F32),
                pltpu.VMEM((2 * SUB, QB), F32),
                pltpu.VMEM((4 * SUB, QB), F32),
                pltpu.SemaphoreType.DMA((2,)),
                pltpu.SemaphoreType.DMA((HKV,)),
                pltpu.SemaphoreType.DMA((6, HKV)),
                pltpu.SemaphoreType.DMA((6, HKV)),
                pltpu.SemaphoreType.DMA((3,)),
                pltpu.SemaphoreType.DMA((3,)),
            ],
            compiler_params=pltpu.CompilerParams(
                vmem_limit_bytes=36 << 20, collective_id=0, has_side_effects=True),
        )(*(pltpu.with_memory_space_constraint(x, pltpu.HBM) for x in (q, k, v)))
        return pl.pallas_call(
            spread,
            out_shape=jax.ShapeDtypeStruct(q.shape, q.dtype),
            in_specs=[vmem] * 6,
            out_specs=hbm,
            scratch_shapes=[
                pltpu.VMEM((T, G, D), BF),
                pltpu.VMEM((1, D, S2 * T), BF),
                pltpu.VMEM((AHEAD + 1, S2 * T, QB), F32),
                pltpu.SemaphoreType.DMA((HKV,)),
            ],
            compiler_params=pltpu.CompilerParams(vmem_limit_bytes=8 << 20),
        )(*parts)

    return jax.shard_map(local, mesh=mesh, in_specs=(spec, spec, spec), out_specs=spec, check_vma=False)
```

```python
import jax
import jax.numpy as jnp
from jax import lax
from jax.experimental import pallas as pl
from jax.experimental.pallas import tpu as pltpu
from jax.sharding import PartitionSpec as P

T = 256
HKV = 8
G = 8
D = 128
NB = 8
SUB = T // NB
QB = SUB * G
S1 = 6
S2 = 2
C = (D ** -0.5) * 1.4426950408889634
ORDER = (0, 2, 4, 6, 7, 5, 3, 1)
AHEAD = 4
HOOK = 4
U0, U1, U2 = 1, 1, 1
BF = jnp.bfloat16
F32 = jnp.float32
NT = (((1,), (1,)), ((), ()))


def chunks(n):
    return [(r, min(r + 256, n)) for r in range(0, n, 256)]


def by_tile(piece, kind, ns):
    return jnp.concatenate([piece(kind, x, t) for t in range(NB) for x in range(ns)], axis=0)


def fold(f, x):
    return f(x.reshape(-1, 8, x.shape[-1]), axis=0)


def attend(heads, piece_of, ns, bias, qt, oacc, ml, vt, sref, arrive=None, first=False, out=None, hook=None):
    rows = ns * SUB
    items = [(u, j) for u in range(len(heads)) for j in ORDER]
    tops = {}

    def scores(i, c):
        u, j = items[i]
        h = heads[u]
        r0, r1 = c
        if j == ORDER[0] and r0 == 0:
            if arrive:
                arrive(u)
            vt[u, :, :ns * T] = by_tile(piece_of(h), 1, ns).T
        parts = [piece_of(h)(0, x % ns, x // ns) for x in range(r0 // SUB, r1 // SUB)]
        s = lax.dot_general(jnp.concatenate(parts, axis=0), qt[h, j * SUB:(j + 1) * SUB].reshape(QB, D), NT,
                            preferred_element_type=F32)
        lo = max(r0, j * rows)
        if lo < r1:
            d = s[lo - r0:] + bias[lo - j * rows:r1 - j * rows]
            s = d if lo == r0 else jnp.concatenate([s[:lo - r0], d], axis=0)
        sref[i % (AHEAD + 1), r0:r1] = s
        m = fold(jnp.max, s)
        tops[i] = jnp.maximum(tops[i], m) if i in tops else m

    def values(i, c, m, acc):
        u, j = items[i]
        r0, r1 = c
        p = jnp.exp2((sref[i % (AHEAD + 1), r0:r1] - m) * C)
        l = fold(jnp.sum, p)
        o = jnp.dot(vt[u, :, r0:r1], p.astype(BF), preferred_element_type=F32)
        return (acc[0] + l, acc[1] + o) if acc else (l, o)

    def finish(i, m, a, l, o):
        u, j = items[i]
        h = heads[u]
        if not first:
            l = ml[h, j, 1:2] * a + l
        if out is None:
            oacc[h, j] = o if first else oacc[h, j] * a + o
            ml[h, j, 0:1] = m
            ml[h, j, 1:2] = l
            return
        r = 1.0 / l
        o = oacc[h, j] * (a * r) + o * r
        out(u)[j * SUB:(j + 1) * SUB] = o.T.astype(BF).reshape(SUB, G, D)

    todo = [(i, c) for i, (u, j) in enumerate(items) for c in chunks((j + 1) * rows)]
    total = len(todo)
    sizes = [len(chunks((j + 1) * rows)) for u, j in items]
    at = 0
    while at < total and todo[at][0] < AHEAD:
        scores(*todo[at])
        at += 1
    for i, (u, j) in enumerate(items):
        if hook and i == HOOK:
            hook()
        top = jnp.max(tops[i], axis=0, keepdims=True)
        m, a = top, None
        if not first:
            m1 = ml[heads[u], j, 0:1]
            m = jnp.maximum(top, m1)
            a = jnp.exp2((m1 - m) * C)
        acc = None
        goal = sum(sizes[:i + AHEAD + 1])
        start = at
        mine = chunks((j + 1) * rows)
        for t, c in enumerate(mine):
            upto = start + (goal - start) * (t + 1) // len(mine)
            while at < upto:
                scores(*todo[at])
                at += 1
            acc = values(i, c, m, acc)
        finish(i, m, a, jnp.sum(acc[0], axis=0, keepdims=True), acc[1])


def near(kv1, chip):
    def of(h):
        return lambda kind, x, t: kv1[h, kind, chip + x // 2, x % 2, t * SUB:(t + 1) * SUB]
    return of


def far(kv2):
    def of(h):
        return lambda kind, x, t: kv2[h, kind, x, t * SUB:(t + 1) * SUB]
    return of


def kernel(q_hbm, k_hbm, v_hbm, ob, qt, kv2, bias2, oacc, ml, raw, wide, kv1, vt, sref, bias0, bias1,
           lsem, qsem, ssem, rsem, lssem, lrsem):
    cx, cy, cz = lax.axis_index("cx"), lax.axis_index("cy"), lax.axis_index("cz")
    me = (cx * 2 + cy) * 2 + cz
    chip = cx * 2 + cy
    link = 1 - (cx + cz - 2 * cx * cz)
    mine = 1 - link

    def over(role):
        x = cx + link - 2 * cx * link
        y = cy + mine - 2 * cy * mine
        return {"cx": x, "cy": y, "cz": x + (1 - role) - 2 * x * (1 - role)}

    sib = {"cz": 1 - cz}

    barrier = pltpu.get_barrier_semaphore()
    for dev in ({"cy": 1 - cy, "cz": 1 - cx}, {"cx": 1 - cx, "cz": 1 - cx}, sib):
        pl.semaphore_signal(barrier, inc=1, device_id=dev, device_id_type=pl.DeviceIdType.MESH)

    loads = [pltpu.make_async_copy(x, raw.at[i], lsem.at[i]) for i, x in enumerate((k_hbm, v_hbm))]
    for x in loads:
        x.start()

    def qload(h):
        return pltpu.make_async_copy(q_hbm.at[:, pl.ds(pl.multiple_of(h * G, G), G), :], qt.at[h], qsem.at[h])

    def rdma(src, dst, send, recv, h, dev):
        return pltpu.make_async_remote_copy(src, dst, ssem.at[send, h], rsem.at[recv, h], dev,
                                            pl.DeviceIdType.MESH)

    def swap(h):
        return rdma(kv1.at[h, :, 0, cz], kv1.at[h, :, 0, cz], 0, 5, h, sib)

    def out_k(h):
        return rdma(kv1.at[h, 0, 0], kv1.at[h, 0, 1 + link], 1, link, h, over(1))

    def out_v(h):
        return rdma(kv1.at[h, 1, 0], kv1.at[h, 1, 1 + link], 2, link, h, over(0))

    def half(h, i, z):
        return rdma(kv1.at[h, i, 0, z], kv1.at[h, i, 1 + link, z], 1 + i, link, h, over(1 - i))

    def relay(h):
        return rdma(kv1.at[h, mine, 1:3], kv1.at[h, mine, 1:3], 3, 2, h, sib)

    def forward(h):
        return rdma(kv1.at[h, mine, 2 - link], kv2.at[h, mine], 4, 3, h, over(link))

    def last(part):
        z = 0 if part == 0 else 1
        return pltpu.make_async_remote_copy(kv1.at[HKV - 1, mine, 2 - link, z], kv2.at[HKV - 1, mine, z],
                                            lssem.at[part], lrsem.at[part], over(mine if part == 2 else link),
                                            pl.DeviceIdType.MESH)

    def last_relay():
        return rdma(kv2.at[HKV - 1, mine, 0], kv2.at[HKV - 1, mine, 0], 5, 4, HKV - 1, sib)

    def relay2(h):
        return rdma(kv2.at[h, mine], kv2.at[h, mine], 5, 4, h, sib)

    def arrived(dst, recv, h):
        rdma(dst, dst, 0, recv, h, sib).wait_recv()

    def mask(nslot, far_chip, ref):
        r = lax.broadcasted_iota(jnp.int32, (nslot * SUB, QB), 0)
        c = lax.broadcasted_iota(jnp.int32, (nslot * SUB, QB), 1)
        x = r // SUB
        kpos = (r % SUB) * 8 + (chip ^ (x // 2 + far_chip)) * 2 + x % 2
        qpos = (c // G) * 8 + me
        ref[...] = jnp.where(kpos <= qpos, 0.0, -1e30)

    def relaid(h, i):
        kv1[h, i, 0, cz] = wide[i, pl.ds(h, T, stride=HKV), :].astype(BF)

    for i in range(2):
        loads[i].wait()
        wide[i] = raw[i].astype(F32).reshape(T * HKV, D)
        relaid(0, i)
        relaid(1, i)
        if i == 0:
            pl.semaphore_wait(barrier, 3)
        half(0, i, cz).start()
    swap(0).start()

    for h in range(2, HKV):
        for i in range(2):
            relaid(h, i)
        if h == 2:
            for i in range(2):
                half(1, i, cz).start()
        swap(h - 1).start()

    mask(2, 0, bias0)
    swap(HKV - 1).start()

    for h in range(2):
        arrived(kv1.at[h, :, 0, cz], 5, h)
        for i in range(2):
            half(h, i, 1 - cz).start()

    @pl.loop(2, HKV)
    def _(h):
        arrived(kv1.at[h, :, 0, cz], 5, h)
        out_k(h).start()
        out_v(h).start()

    @pl.loop(0, HKV)
    def _(h):
        qload(h).start()

    mask(4, 1, bias1)
    mask(2, 3, bias2)

    def pass_on(h):
        arrived(kv1.at[h, mine, 1], 0, h)
        arrived(kv1.at[h, mine, 2], 1, h)
        relay(h).start()

        @pl.when(h < HKV - 1)
        def _():
            forward(h).start()

        @pl.when(h == HKV - 1)
        def _():
            for part in range(3):
                last(part).start()

    def pass_on2(h):
        @pl.when(h < HKV - 1)
        def _():
            arrived(kv2.at[h, mine], 3, h)
            relay2(h).start()

        @pl.when(h == HKV - 1)
        def _():
            last(0).wait_recv()
            last_relay().start()

    @pl.loop(0, HKV // U0)
    def _(g):
        heads = [g * U0 + u for u in range(U0)]

        def arrive(u):
            h = heads[u]
            qload(h).wait()

        attend(heads, near(kv1, 0), 2, bias0, qt, oacc, ml, vt, sref, arrive, first=True)

    pass_on(jnp.int32(0))

    @pl.loop(0, HKV - 1)
    def _(h):
        pass_on(h + 1)
        arrived(kv1.at[h, link, 1:3], 2, h)
        attend([h], near(kv1, 1), 4, bias1, qt, oacc, ml, vt, sref)

    arrived(kv1.at[HKV - 1, link, 1:3], 2, HKV - 1)
    attend([HKV - 1], near(kv1, 1), 4, bias1, qt, oacc, ml, vt, sref, hook=lambda: pass_on2(jnp.int32(0)))

    @pl.loop(0, (HKV - 1) // U2)
    def _(g):
        heads = [g * U2 + u for u in range(U2)]

        def arrive(u):
            pass_on2(heads[u] + 1)
            arrived(kv2.at[heads[u], link], 4, heads[u])

        attend(heads, far(kv2), 2, bias2, qt, oacc, ml, vt, sref, arrive, out=lambda u: ob.at[:, pl.ds(pl.multiple_of(heads[u] * G, G), G), :])

    for part in (1, 2):
        last(part).wait_recv()
    last_relay().wait_recv()

    @pl.loop(0, HKV)
    def _(h):
        for sent in (swap, out_k, out_v, relay):
            sent(h).wait_send()

    @pl.loop(0, HKV - 1)
    def _(h):
        forward(h).wait_send()
        relay2(h).wait_send()

    for part in range(3):
        last(part).wait_send()
    last_relay().wait_send()


def spread(ob, qt, kv2, bias2, oacc, ml, o_hbm, last, vt, sref, sem):
    done = (HKV - 1) * G

    def put(b):
        rows = pl.ds(pl.multiple_of(b * SUB, SUB), SUB)
        return pltpu.make_async_copy(ob.at[rows], o_hbm.at[rows, :done, :], sem.at[b])

    @pl.loop(0, NB)
    def _(b):
        put(b).start()

    attend([HKV - 1], far(kv2), 2, bias2, qt, oacc, ml, vt, sref, out=lambda u: last)
    tail = pltpu.make_async_copy(last, o_hbm.at[:, done:, :], sem.at[NB])
    tail.start()

    @pl.loop(0, NB)
    def _(b):
        put(b).wait()

    tail.wait()


def solution(mesh):
    spec = P(("dp", "cx", "cy", "cz"))

    def local(q, k, v):
        hbm = pl.BlockSpec(memory_space=pltpu.HBM)
        vmem = pl.BlockSpec(memory_space=pltpu.VMEM)
        parts = pl.pallas_call(
            kernel,
            out_shape=[
                pltpu.VMEM((T, (HKV - 1) * G, D), BF),
                pltpu.VMEM((HKV, T, G, D), BF),
                pltpu.VMEM((HKV, 2, 2, T, D), BF),
                pltpu.VMEM((S2 * SUB, QB), F32),
                pltpu.VMEM((HKV, NB, D, QB), F32),
                pltpu.VMEM((HKV, NB, 8, QB), F32),
            ],
            in_specs=[hbm] * 3,
            out_specs=[vmem] * 6,
            scratch_shapes=[
                pltpu.VMEM((2, T, HKV, D), BF),
                pltpu.VMEM((2, T * HKV, D), F32),
                pltpu.VMEM((HKV, 2, 3, 2, T, D), BF),
                pltpu.VMEM((max(U0, U1, U2), D, 4 * T), BF),
                pltpu.VMEM((AHEAD + 1, 4 * T, QB), F32),
                pltpu.VMEM((2 * SUB, QB), F32),
                pltpu.VMEM((4 * SUB, QB), F32),
                pltpu.SemaphoreType.DMA((2,)),
                pltpu.SemaphoreType.DMA((HKV,)),
                pltpu.SemaphoreType.DMA((6, HKV)),
                pltpu.SemaphoreType.DMA((6, HKV)),
                pltpu.SemaphoreType.DMA((3,)),
                pltpu.SemaphoreType.DMA((3,)),
            ],
            compiler_params=pltpu.CompilerParams(
                vmem_limit_bytes=36 << 20, collective_id=0, has_side_effects=True),
        )(*(pltpu.with_memory_space_constraint(x, pltpu.HBM) for x in (q, k, v)))
        return pl.pallas_call(
            spread,
            out_shape=jax.ShapeDtypeStruct(q.shape, q.dtype),
            in_specs=[vmem] * 6,
            out_specs=hbm,
            scratch_shapes=[
                pltpu.VMEM((T, G, D), BF),
                pltpu.VMEM((1, D, S2 * T), BF),
                pltpu.VMEM((AHEAD + 1, S2 * T, QB), F32),
                pltpu.SemaphoreType.DMA((NB + 1,)),
            ],
            compiler_params=pltpu.CompilerParams(vmem_limit_bytes=8 << 20),
        )(*parts)

    return jax.shard_map(local, mesh=mesh, in_specs=(spec, spec, spec), out_specs=spec, check_vma=False)
```

```python
import jax
import jax.numpy as jnp
from jax import lax
from jax.experimental import pallas as pl
from jax.experimental.pallas import tpu as pltpu
from jax.sharding import PartitionSpec as P

T = 256
CUT = 128
HKV = 8
G = 8
D = 128
NB = 8
SUB = T // NB
QB = SUB * G
S1 = 6
S2 = 2
C = (D ** -0.5) * 1.4426950408889634
ORDER = (0, 2, 4, 6, 7, 5, 3, 1)
AHEAD = 4
HOOK = 4
U0, U1, U2 = 1, 1, 1
BF = jnp.bfloat16
F32 = jnp.float32
NT = (((1,), (1,)), ((), ()))


def chunks(n):
    return [(r, min(r + 256, n)) for r in range(0, n, 256)]


def by_tile(piece, kind, ns):
    return jnp.concatenate([piece(kind, x, t) for t in range(NB) for x in range(ns)], axis=0)


def fold(f, x):
    return f(x.reshape(-1, 8, x.shape[-1]), axis=0)


def attend(heads, piece_of, ns, bias, qt, oacc, ml, vt, sref, arrive=None, first=False, out=None, hook=None):
    rows = ns * SUB
    items = [(u, j) for u in range(len(heads)) for j in ORDER]
    tops = {}

    def scores(i, c):
        u, j = items[i]
        h = heads[u]
        r0, r1 = c
        if j == ORDER[0] and r0 == 0:
            if arrive:
                arrive(u)
            vt[u, :, :ns * T] = by_tile(piece_of(h), 1, ns).T
        parts = [piece_of(h)(0, x % ns, x // ns) for x in range(r0 // SUB, r1 // SUB)]
        s = lax.dot_general(jnp.concatenate(parts, axis=0), qt[h, j * SUB:(j + 1) * SUB].reshape(QB, D), NT,
                            preferred_element_type=F32)
        lo = max(r0, j * rows)
        if lo < r1:
            d = s[lo - r0:] + bias[lo - j * rows:r1 - j * rows]
            s = d if lo == r0 else jnp.concatenate([s[:lo - r0], d], axis=0)
        sref[i % (AHEAD + 1), r0:r1] = s
        m = fold(jnp.max, s)
        tops[i] = jnp.maximum(tops[i], m) if i in tops else m

    def values(i, c, m, acc):
        u, j = items[i]
        r0, r1 = c
        p = jnp.exp2((sref[i % (AHEAD + 1), r0:r1] - m) * C)
        l = fold(jnp.sum, p)
        o = jnp.dot(vt[u, :, r0:r1], p.astype(BF), preferred_element_type=F32)
        return (acc[0] + l, acc[1] + o) if acc else (l, o)

    def finish(i, m, a, l, o):
        u, j = items[i]
        h = heads[u]
        if not first:
            l = ml[h, j, 1:2] * a + l
        if out is None:
            oacc[h, j] = o if first else oacc[h, j] * a + o
            ml[h, j, 0:1] = m
            ml[h, j, 1:2] = l
            return
        r = 1.0 / l
        o = oacc[h, j] * (a * r) + o * r
        out(u)[j * SUB:(j + 1) * SUB] = o.T.astype(BF).reshape(SUB, G, D)

    todo = [(i, c) for i, (u, j) in enumerate(items) for c in chunks((j + 1) * rows)]
    total = len(todo)
    sizes = [len(chunks((j + 1) * rows)) for u, j in items]
    at = 0
    while at < total and todo[at][0] < AHEAD:
        scores(*todo[at])
        at += 1
    for i, (u, j) in enumerate(items):
        if hook and i == HOOK:
            hook()
        top = jnp.max(tops[i], axis=0, keepdims=True)
        m, a = top, None
        if not first:
            m1 = ml[heads[u], j, 0:1]
            m = jnp.maximum(top, m1)
            a = jnp.exp2((m1 - m) * C)
        acc = None
        goal = sum(sizes[:i + AHEAD + 1])
        start = at
        mine = chunks((j + 1) * rows)
        for t, c in enumerate(mine):
            upto = start + (goal - start) * (t + 1) // len(mine)
            while at < upto:
                scores(*todo[at])
                at += 1
            acc = values(i, c, m, acc)
        finish(i, m, a, jnp.sum(acc[0], axis=0, keepdims=True), acc[1])


def near(kv1, chip):
    def of(h):
        return lambda kind, x, t: kv1[h, kind, chip + x // 2, x % 2, t * SUB:(t + 1) * SUB]
    return of


def far(kv2):
    def of(h):
        return lambda kind, x, t: kv2[h, kind, x, t * SUB:(t + 1) * SUB]
    return of


def kernel(q_hbm, k_hbm, v_hbm, ob, qt, kv2, bias2, oacc, ml, raw, wide, kv1, vt, sref, bias0, bias1,
           lsem, qsem, ssem, rsem, lssem, lrsem):
    cx, cy, cz = lax.axis_index("cx"), lax.axis_index("cy"), lax.axis_index("cz")
    me = (cx * 2 + cy) * 2 + cz
    chip = cx * 2 + cy
    link = 1 - (cx + cz - 2 * cx * cz)
    mine = 1 - link

    def over(role):
        x = cx + link - 2 * cx * link
        y = cy + mine - 2 * cy * mine
        return {"cx": x, "cy": y, "cz": x + (1 - role) - 2 * x * (1 - role)}

    sib = {"cz": 1 - cz}

    barrier = pltpu.get_barrier_semaphore()
    for dev in ({"cy": 1 - cy, "cz": 1 - cx}, {"cx": 1 - cx, "cz": 1 - cx}, sib):
        pl.semaphore_signal(barrier, inc=1, device_id=dev, device_id_type=pl.DeviceIdType.MESH)

    loads = [pltpu.make_async_copy(x, raw.at[i], lsem.at[i]) for i, x in enumerate((k_hbm, v_hbm))]
    for x in loads:
        x.start()

    def qload(h):
        return pltpu.make_async_copy(q_hbm.at[:, pl.ds(pl.multiple_of(h * G, G), G), :], qt.at[h], qsem.at[h])

    def rdma(src, dst, send, recv, h, dev):
        return pltpu.make_async_remote_copy(src, dst, ssem.at[send, h], rsem.at[recv, h], dev,
                                            pl.DeviceIdType.MESH)

    def swap(h):
        return rdma(kv1.at[h, :, 0, cz], kv1.at[h, :, 0, cz], 0, 5, h, sib)

    def out_k(h):
        return rdma(kv1.at[h, 0, 0], kv1.at[h, 0, 1 + link], 1, link, h, over(1))

    def out_v(h):
        return rdma(kv1.at[h, 1, 0], kv1.at[h, 1, 1 + link], 2, link, h, over(0))

    def half(h, i, z):
        return rdma(kv1.at[h, i, 0, z], kv1.at[h, i, 1 + link, z], 1 + i, link, h, over(1 - i))

    def relay(h):
        return rdma(kv1.at[h, mine, 1:3], kv1.at[h, mine, 1:3], 3, 2, h, sib)

    def forward(h):
        return rdma(kv1.at[h, mine, 2 - link], kv2.at[h, mine], 4, 3, h, over(link))

    def last(part):
        z, rows = ((0, pl.ds(0, T)), (1, pl.ds(0, CUT)), (1, pl.ds(CUT, T - CUT)), (1, pl.ds(CUT, T - CUT)))[part]
        return pltpu.make_async_remote_copy(kv1.at[HKV - 1, mine, 2 - link, z, rows], kv2.at[HKV - 1, mine, z, rows],
                                            lssem.at[part], lrsem.at[part], over(mine if part == 3 else link),
                                            pl.DeviceIdType.MESH)

    def last_relay(z):
        rows = pl.ds(0, CUT if z else T)
        return pltpu.make_async_remote_copy(kv2.at[HKV - 1, mine, z, rows], kv2.at[HKV - 1, mine, z, rows],
                                            lssem.at[4 + z], lrsem.at[4 + z], sib, pl.DeviceIdType.MESH)

    def relay2(h):
        return rdma(kv2.at[h, mine], kv2.at[h, mine], 5, 4, h, sib)

    def arrived(dst, recv, h):
        rdma(dst, dst, 0, recv, h, sib).wait_recv()

    def mask(nslot, far_chip, ref):
        r = lax.broadcasted_iota(jnp.int32, (nslot * SUB, QB), 0)
        c = lax.broadcasted_iota(jnp.int32, (nslot * SUB, QB), 1)
        x = r // SUB
        kpos = (r % SUB) * 8 + (chip ^ (x // 2 + far_chip)) * 2 + x % 2
        qpos = (c // G) * 8 + me
        ref[...] = jnp.where(kpos <= qpos, 0.0, -1e30)

    def relaid(h, i):
        kv1[h, i, 0, cz] = wide[i, pl.ds(h, T, stride=HKV), :].astype(BF)

    for i in range(2):
        loads[i].wait()
        wide[i] = raw[i].astype(F32).reshape(T * HKV, D)
        relaid(0, i)
        relaid(1, i)
        if i == 0:
            pl.semaphore_wait(barrier, 3)
        half(0, i, cz).start()
    swap(0).start()

    for h in range(2, HKV):
        for i in range(2):
            relaid(h, i)
        if h == 2:
            for i in range(2):
                half(1, i, cz).start()
        swap(h - 1).start()

    mask(2, 0, bias0)
    swap(HKV - 1).start()

    for h in range(2):
        arrived(kv1.at[h, :, 0, cz], 5, h)
        for i in range(2):
            half(h, i, 1 - cz).start()

    @pl.loop(2, HKV)
    def _(h):
        arrived(kv1.at[h, :, 0, cz], 5, h)
        out_k(h).start()
        out_v(h).start()

    @pl.loop(0, HKV)
    def _(h):
        qload(h).start()

    mask(4, 1, bias1)
    mask(2, 3, bias2)

    def pass_on(h):
        arrived(kv1.at[h, mine, 1], 0, h)
        arrived(kv1.at[h, mine, 2], 1, h)
        relay(h).start()

        @pl.when(h < HKV - 1)
        def _():
            forward(h).start()

        @pl.when(h == HKV - 1)
        def _():
            for part in range(4):
                last(part).start()

    def pass_on2(h):
        @pl.when(h < HKV - 1)
        def _():
            arrived(kv2.at[h, mine], 3, h)
            relay2(h).start()

        @pl.when(h == HKV - 1)
        def _():
            for z in range(2):
                last(z).wait_recv()
                last_relay(z).start()

    @pl.loop(0, HKV // U0)
    def _(g):
        heads = [g * U0 + u for u in range(U0)]

        def arrive(u):
            h = heads[u]
            qload(h).wait()

        attend(heads, near(kv1, 0), 2, bias0, qt, oacc, ml, vt, sref, arrive, first=True)

    pass_on(jnp.int32(0))

    @pl.loop(0, HKV - 1)
    def _(h):
        pass_on(h + 1)
        arrived(kv1.at[h, link, 1:3], 2, h)
        attend([h], near(kv1, 1), 4, bias1, qt, oacc, ml, vt, sref)

    arrived(kv1.at[HKV - 1, link, 1:3], 2, HKV - 1)
    attend([HKV - 1], near(kv1, 1), 4, bias1, qt, oacc, ml, vt, sref, hook=lambda: pass_on2(jnp.int32(0)))

    @pl.loop(0, HKV)
    def _(h):
        for sent in (swap, out_k, out_v, relay):
            sent(h).wait_send()

    @pl.loop(0, (HKV - 1) // U2)
    def _(g):
        heads = [g * U2 + u for u in range(U2)]

        def arrive(u):
            pass_on2(heads[u] + 1)
            arrived(kv2.at[heads[u], link], 4, heads[u])

        attend(heads, far(kv2), 2, bias2, qt, oacc, ml, vt, sref, arrive, out=lambda u: ob.at[heads[u]])

    @pl.loop(0, HKV - 1)
    def _(h):
        forward(h).wait_send()
        relay2(h).wait_send()

    for z in range(2):
        last_relay(z).wait_recv()
    for part in (2, 3):
        last(part).wait_recv()

    for part in range(4):
        last(part).wait_send()
    for z in range(2):
        last_relay(z).wait_send()


def spread(ob, qt, kv2, bias2, oacc, ml, o_hbm, last, vt, sref, sem):
    def put(src, h):
        return pltpu.make_async_copy(src, o_hbm.at[:, pl.ds(pl.multiple_of(h * G, G), G), :], sem.at[h])

    @pl.loop(0, HKV - 1)
    def _(h):
        put(ob.at[h], h).start()

    attend([HKV - 1], far(kv2), 2, bias2, qt, oacc, ml, vt, sref, out=lambda u: last)
    put(last, HKV - 1).start()

    @pl.loop(0, HKV - 1)
    def _(h):
        put(ob.at[h], h).wait()

    put(last, HKV - 1).wait()


def solution(mesh):
    spec = P(("dp", "cx", "cy", "cz"))

    def local(q, k, v):
        hbm = pl.BlockSpec(memory_space=pltpu.HBM)
        vmem = pl.BlockSpec(memory_space=pltpu.VMEM)
        parts = pl.pallas_call(
            kernel,
            out_shape=[
                pltpu.VMEM((HKV - 1, T, G, D), BF),
                pltpu.VMEM((HKV, T, G, D), BF),
                pltpu.VMEM((HKV, 2, 2, T, D), BF),
                pltpu.VMEM((S2 * SUB, QB), F32),
                pltpu.VMEM((HKV, NB, D, QB), F32),
                pltpu.VMEM((HKV, NB, 8, QB), F32),
            ],
            in_specs=[hbm] * 3,
            out_specs=[vmem] * 6,
            scratch_shapes=[
                pltpu.VMEM((2, T, HKV, D), BF),
                pltpu.VMEM((2, T * HKV, D), F32),
                pltpu.VMEM((HKV, 2, 3, 2, T, D), BF),
                pltpu.VMEM((max(U0, U1, U2), D, 4 * T), BF),
                pltpu.VMEM((AHEAD + 1, 4 * T, QB), F32),
                pltpu.VMEM((2 * SUB, QB), F32),
                pltpu.VMEM((4 * SUB, QB), F32),
                pltpu.SemaphoreType.DMA((2,)),
                pltpu.SemaphoreType.DMA((HKV,)),
                pltpu.SemaphoreType.DMA((6, HKV)),
                pltpu.SemaphoreType.DMA((6, HKV)),
                pltpu.SemaphoreType.DMA((6,)),
                pltpu.SemaphoreType.DMA((6,)),
            ],
            compiler_params=pltpu.CompilerParams(
                vmem_limit_bytes=36 << 20, collective_id=0, has_side_effects=True),
        )(*(pltpu.with_memory_space_constraint(x, pltpu.HBM) for x in (q, k, v)))
        return pl.pallas_call(
            spread,
            out_shape=jax.ShapeDtypeStruct(q.shape, q.dtype),
            in_specs=[vmem] * 6,
            out_specs=hbm,
            scratch_shapes=[
                pltpu.VMEM((T, G, D), BF),
                pltpu.VMEM((1, D, S2 * T), BF),
                pltpu.VMEM((AHEAD + 1, S2 * T, QB), F32),
                pltpu.SemaphoreType.DMA((HKV,)),
            ],
            compiler_params=pltpu.CompilerParams(vmem_limit_bytes=8 << 20),
        )(*parts)

    return jax.shard_map(local, mesh=mesh, in_specs=(spec, spec, spec), out_specs=spec, check_vma=False)
```

```python
import jax
import jax.numpy as jnp
from jax import lax
from jax.experimental import pallas as pl
from jax.experimental.pallas import tpu as pltpu
from jax.sharding import PartitionSpec as P

T = 256
CUT = 128
SENDS = ((2, 2), (4, 2), (6, 1), (7, 1))
HKV = 8
G = 8
D = 128
NB = 8
SUB = T // NB
QB = SUB * G
S1 = 6
S2 = 2
C = (D ** -0.5) * 1.4426950408889634
ORDER = (0, 2, 4, 6, 7, 5, 3, 1)
AHEAD = 4
HOOK = 4
U0, U1, U2 = 1, 1, 1
BF = jnp.bfloat16
F32 = jnp.float32
NT = (((1,), (1,)), ((), ()))


def chunks(n):
    return [(r, min(r + 256, n)) for r in range(0, n, 256)]


def by_tile(piece, kind, ns):
    return jnp.concatenate([piece(kind, x, t) for t in range(NB) for x in range(ns)], axis=0)


def fold(f, x):
    return f(x.reshape(-1, 8, x.shape[-1]), axis=0)


def attend(heads, piece_of, ns, bias, qt, oacc, ml, vt, sref, arrive=None, first=False, out=None, hook=None):
    rows = ns * SUB
    items = [(u, j) for u in range(len(heads)) for j in ORDER]
    tops = {}

    def scores(i, c):
        u, j = items[i]
        h = heads[u]
        r0, r1 = c
        if j == ORDER[0] and r0 == 0:
            if arrive:
                arrive(u)
            vt[u, :, :ns * T] = by_tile(piece_of(h), 1, ns).T
        parts = [piece_of(h)(0, x % ns, x // ns) for x in range(r0 // SUB, r1 // SUB)]
        s = lax.dot_general(jnp.concatenate(parts, axis=0), qt[h, j * SUB:(j + 1) * SUB].reshape(QB, D), NT,
                            preferred_element_type=F32)
        lo = max(r0, j * rows)
        if lo < r1:
            d = s[lo - r0:] + bias[lo - j * rows:r1 - j * rows]
            s = d if lo == r0 else jnp.concatenate([s[:lo - r0], d], axis=0)
        sref[i % (AHEAD + 1), r0:r1] = s
        m = fold(jnp.max, s)
        tops[i] = jnp.maximum(tops[i], m) if i in tops else m

    def values(i, c, m, acc):
        u, j = items[i]
        r0, r1 = c
        p = jnp.exp2((sref[i % (AHEAD + 1), r0:r1] - m) * C)
        l = fold(jnp.sum, p)
        o = jnp.dot(vt[u, :, r0:r1], p.astype(BF), preferred_element_type=F32)
        return (acc[0] + l, acc[1] + o) if acc else (l, o)

    def finish(i, m, a, l, o):
        u, j = items[i]
        h = heads[u]
        if not first:
            l = ml[h, j, 1:2] * a + l
        if out is None:
            oacc[h, j] = o if first else oacc[h, j] * a + o
            ml[h, j, 0:1] = m
            ml[h, j, 1:2] = l
            return
        r = 1.0 / l
        o = oacc[h, j] * (a * r) + o * r
        out(u)[j * SUB:(j + 1) * SUB] = o.T.astype(BF).reshape(SUB, G, D)

    todo = [(i, c) for i, (u, j) in enumerate(items) for c in chunks((j + 1) * rows)]
    total = len(todo)
    sizes = [len(chunks((j + 1) * rows)) for u, j in items]
    at = 0
    while at < total and todo[at][0] < AHEAD:
        scores(*todo[at])
        at += 1
    for i, (u, j) in enumerate(items):
        if hook and i == HOOK:
            hook()
        top = jnp.max(tops[i], axis=0, keepdims=True)
        m, a = top, None
        if not first:
            m1 = ml[heads[u], j, 0:1]
            m = jnp.maximum(top, m1)
            a = jnp.exp2((m1 - m) * C)
        acc = None
        goal = sum(sizes[:i + AHEAD + 1])
        start = at
        mine = chunks((j + 1) * rows)
        for t, c in enumerate(mine):
            upto = start + (goal - start) * (t + 1) // len(mine)
            while at < upto:
                scores(*todo[at])
                at += 1
            acc = values(i, c, m, acc)
        finish(i, m, a, jnp.sum(acc[0], axis=0, keepdims=True), acc[1])


def near(kv1, chip):
    def of(h):
        return lambda kind, x, t: kv1[h, kind, chip + x // 2, x % 2, t * SUB:(t + 1) * SUB]
    return of


def far(kv2):
    def of(h):
        return lambda kind, x, t: kv2[h, kind, x, t * SUB:(t + 1) * SUB]
    return of


def kernel(q_hbm, k_hbm, v_hbm, ob, qt, kv2, bias2, oacc, ml, raw, wide, kv1, vt, sref, bias0, bias1,
           lsem, qsem, ssem, rsem, lssem, lrsem):
    cx, cy, cz = lax.axis_index("cx"), lax.axis_index("cy"), lax.axis_index("cz")
    me = (cx * 2 + cy) * 2 + cz
    chip = cx * 2 + cy
    link = 1 - (cx + cz - 2 * cx * cz)
    mine = 1 - link

    def over(role):
        x = cx + link - 2 * cx * link
        y = cy + mine - 2 * cy * mine
        return {"cx": x, "cy": y, "cz": x + (1 - role) - 2 * x * (1 - role)}

    sib = {"cz": 1 - cz}

    barrier = pltpu.get_barrier_semaphore()
    for dev in ({"cy": 1 - cy, "cz": 1 - cx}, {"cx": 1 - cx, "cz": 1 - cx}, sib):
        pl.semaphore_signal(barrier, inc=1, device_id=dev, device_id_type=pl.DeviceIdType.MESH)

    loads = [pltpu.make_async_copy(x, raw.at[i], lsem.at[i]) for i, x in enumerate((k_hbm, v_hbm))]
    for x in loads:
        x.start()

    def qload(h):
        return pltpu.make_async_copy(q_hbm.at[:, pl.ds(pl.multiple_of(h * G, G), G), :], qt.at[h], qsem.at[h])

    def rdma(src, dst, send, recv, h, dev):
        return pltpu.make_async_remote_copy(src, dst, ssem.at[send, h], rsem.at[recv, h], dev,
                                            pl.DeviceIdType.MESH)

    def swap(h):
        return rdma(kv1.at[h, :, 0, cz], kv1.at[h, :, 0, cz], 0, 5, h, sib)

    def out(h, i, n):
        heads = pl.ds(h, n)
        return rdma(kv1.at[heads, i, 0], kv1.at[heads, i, 1 + link], 1 + i, link, h, over(1 - i))

    def half(h, i, z):
        return rdma(kv1.at[h, i, 0, z], kv1.at[h, i, 1 + link, z], 1 + i, link, h, over(1 - i))

    def relay(h):
        return rdma(kv1.at[h, mine, 1:3], kv1.at[h, mine, 1:3], 3, 2, h, sib)

    def forward(h):
        return rdma(kv1.at[h, mine, 2 - link], kv2.at[h, mine], 4, 3, h, over(link))

    def last(part):
        z, rows = ((0, pl.ds(0, T)), (1, pl.ds(0, CUT)), (1, pl.ds(CUT, T - CUT)), (1, pl.ds(CUT, T - CUT)))[part]
        return pltpu.make_async_remote_copy(kv1.at[HKV - 1, mine, 2 - link, z, rows], kv2.at[HKV - 1, mine, z, rows],
                                            lssem.at[part], lrsem.at[part], over(mine if part == 3 else link),
                                            pl.DeviceIdType.MESH)

    def last_relay(z):
        rows = pl.ds(0, CUT if z else T)
        return pltpu.make_async_remote_copy(kv2.at[HKV - 1, mine, z, rows], kv2.at[HKV - 1, mine, z, rows],
                                            lssem.at[4 + z], lrsem.at[4 + z], sib, pl.DeviceIdType.MESH)

    def relay2(h):
        return rdma(kv2.at[h, mine], kv2.at[h, mine], 5, 4, h, sib)

    def arrived(dst, recv, h):
        rdma(dst, dst, 0, recv, h, sib).wait_recv()

    def mask(nslot, far_chip, ref):
        r = lax.broadcasted_iota(jnp.int32, (nslot * SUB, QB), 0)
        c = lax.broadcasted_iota(jnp.int32, (nslot * SUB, QB), 1)
        x = r // SUB
        kpos = (r % SUB) * 8 + (chip ^ (x // 2 + far_chip)) * 2 + x % 2
        qpos = (c // G) * 8 + me
        ref[...] = jnp.where(kpos <= qpos, 0.0, -1e30)

    def relaid(h, i):
        kv1[h, i, 0, cz] = wide[i, pl.ds(h, T, stride=HKV), :].astype(BF)

    def relaid(h, i):
        kv1[h, i, 0, cz] = wide[i, pl.ds(h, T, stride=HKV), :].astype(BF)

    for i in range(2):
        loads[i].wait()
        wide[i] = raw[i].astype(F32).reshape(T * HKV, D)
        relaid(0, i)
        if i == 0:
            pl.semaphore_wait(barrier, 3)
        else:
            relaid(1, 0)
        half(0, i, cz).start()
    swap(0).start()
    relaid(1, 1)

    for h in range(2, HKV):
        for i in range(2):
            relaid(h, i)
        if h == 2:
            for i in range(2):
                half(1, i, cz).start()
        swap(h - 1).start()

    mask(2, 0, bias0)
    swap(HKV - 1).start()

    for h in range(2):
        arrived(kv1.at[h, :, 0, cz], 5, h)
        for i in range(2):
            half(h, i, 1 - cz).start()

    for h, n in SENDS:
        for x in range(h, h + n):
            arrived(kv1.at[x, :, 0, cz], 5, x)
        for i in range(2):
            out(h, i, n).start()

    @pl.loop(0, HKV)
    def _(h):
        qload(h).start()

    mask(4, 1, bias1)
    mask(2, 3, bias2)

    def pass_on(h):
        middle = (h >= 2) & (h < 6)

        @pl.when(jnp.logical_not(middle))
        def _():
            arrived(kv1.at[h, mine, 1], 0, h)
            arrived(kv1.at[h, mine, 2], 1, h)

        @pl.when(middle & (h % 2 == 0))
        def _():
            arrived(kv1.at[0:2, mine, 1], 0, h)
            arrived(kv1.at[0:2, mine, 2], 1, h)

        relay(h).start()

        @pl.when(h < HKV - 1)
        def _():
            forward(h).start()

        @pl.when(h == HKV - 1)
        def _():
            for part in range(4):
                last(part).start()

    def pass_on2(h):
        @pl.when(h < HKV - 1)
        def _():
            arrived(kv2.at[h, mine], 3, h)
            relay2(h).start()

        @pl.when(h == HKV - 1)
        def _():
            for z in range(2):
                last(z).wait_recv()
                last_relay(z).start()

    @pl.loop(0, HKV // U0)
    def _(g):
        heads = [g * U0 + u for u in range(U0)]

        def arrive(u):
            h = heads[u]
            qload(h).wait()

        attend(heads, near(kv1, 0), 2, bias0, qt, oacc, ml, vt, sref, arrive, first=True)

    pass_on(jnp.int32(0))

    @pl.loop(0, HKV - 1)
    def _(h):
        pass_on(h + 1)
        arrived(kv1.at[h, link, 1:3], 2, h)
        attend([h], near(kv1, 1), 4, bias1, qt, oacc, ml, vt, sref)

    arrived(kv1.at[HKV - 1, link, 1:3], 2, HKV - 1)
    attend([HKV - 1], near(kv1, 1), 4, bias1, qt, oacc, ml, vt, sref, hook=lambda: pass_on2(jnp.int32(0)))

    for h, n in ((0, 1), (1, 1)) + SENDS:
        for i in range(2):
            out(h, i, n).wait_send()

    @pl.loop(0, HKV)
    def _(h):
        swap(h).wait_send()
        relay(h).wait_send()

    @pl.loop(0, (HKV - 1) // U2)
    def _(g):
        heads = [g * U2 + u for u in range(U2)]

        def arrive(u):
            pass_on2(heads[u] + 1)
            arrived(kv2.at[heads[u], link], 4, heads[u])

        attend(heads, far(kv2), 2, bias2, qt, oacc, ml, vt, sref, arrive, out=lambda u: ob.at[heads[u]])

    @pl.loop(0, HKV - 1)
    def _(h):
        forward(h).wait_send()
        relay2(h).wait_send()

    for z in range(2):
        last_relay(z).wait_recv()
    for part in (2, 3):
        last(part).wait_recv()

    for part in range(4):
        last(part).wait_send()
    for z in range(2):
        last_relay(z).wait_send()


def spread(ob, qt, kv2, bias2, oacc, ml, o_hbm, last, vt, sref, sem):
    def put(src, h):
        return pltpu.make_async_copy(src, o_hbm.at[:, pl.ds(pl.multiple_of(h * G, G), G), :], sem.at[h])

    @pl.loop(0, HKV - 1)
    def _(h):
        put(ob.at[h], h).start()

    attend([HKV - 1], far(kv2), 2, bias2, qt, oacc, ml, vt, sref, out=lambda u: last)
    put(last, HKV - 1).start()

    @pl.loop(0, HKV - 1)
    def _(h):
        put(ob.at[h], h).wait()

    put(last, HKV - 1).wait()


def solution(mesh):
    spec = P(("dp", "cx", "cy", "cz"))

    def local(q, k, v):
        hbm = pl.BlockSpec(memory_space=pltpu.HBM)
        vmem = pl.BlockSpec(memory_space=pltpu.VMEM)
        parts = pl.pallas_call(
            kernel,
            out_shape=[
                pltpu.VMEM((HKV - 1, T, G, D), BF),
                pltpu.VMEM((HKV, T, G, D), BF),
                pltpu.VMEM((HKV, 2, 2, T, D), BF),
                pltpu.VMEM((S2 * SUB, QB), F32),
                pltpu.VMEM((HKV, NB, D, QB), F32),
                pltpu.VMEM((HKV, NB, 8, QB), F32),
            ],
            in_specs=[hbm] * 3,
            out_specs=[vmem] * 6,
            scratch_shapes=[
                pltpu.VMEM((2, T, HKV, D), BF),
                pltpu.VMEM((2, T * HKV, D), F32),
                pltpu.VMEM((HKV, 2, 3, 2, T, D), BF),
                pltpu.VMEM((max(U0, U1, U2), D, 4 * T), BF),
                pltpu.VMEM((AHEAD + 1, 4 * T, QB), F32),
                pltpu.VMEM((2 * SUB, QB), F32),
                pltpu.VMEM((4 * SUB, QB), F32),
                pltpu.SemaphoreType.DMA((2,)),
                pltpu.SemaphoreType.DMA((HKV,)),
                pltpu.SemaphoreType.DMA((6, HKV)),
                pltpu.SemaphoreType.DMA((6, HKV)),
                pltpu.SemaphoreType.DMA((6,)),
                pltpu.SemaphoreType.DMA((6,)),
            ],
            compiler_params=pltpu.CompilerParams(
                vmem_limit_bytes=36 << 20, collective_id=0, has_side_effects=True),
        )(*(pltpu.with_memory_space_constraint(x, pltpu.HBM) for x in (q, k, v)))
        return pl.pallas_call(
            spread,
            out_shape=jax.ShapeDtypeStruct(q.shape, q.dtype),
            in_specs=[vmem] * 6,
            out_specs=hbm,
            scratch_shapes=[
                pltpu.VMEM((T, G, D), BF),
                pltpu.VMEM((1, D, S2 * T), BF),
                pltpu.VMEM((AHEAD + 1, S2 * T, QB), F32),
                pltpu.SemaphoreType.DMA((HKV,)),
            ],
            compiler_params=pltpu.CompilerParams(vmem_limit_bytes=8 << 20),
        )(*parts)

    return jax.shard_map(local, mesh=mesh, in_specs=(spec, spec, spec), out_specs=spec, check_vma=False)
```

```python
import jax
import jax.numpy as jnp
from jax import lax
from jax.experimental import pallas as pl
from jax.experimental.pallas import tpu as pltpu
from jax.sharding import PartitionSpec as P

T = 256
CUT = 128
SENDS = ((2, 2), (4, 2), (6, 1), (7, 1))
HKV = 8
G = 8
D = 128
NB = 8
SUB = T // NB
QB = SUB * G
S1 = 6
S2 = 2
C = (D ** -0.5) * 1.4426950408889634
ORDER = (0, 2, 4, 6, 7, 5, 3, 1)
AHEAD = 4
HOOK = 4
U0, U1, U2 = 1, 1, 1
BF = jnp.bfloat16
F32 = jnp.float32
NT = (((1,), (1,)), ((), ()))


def chunks(n):
    return [(r, min(r + 256, n)) for r in range(0, n, 256)]


def by_tile(piece, kind, ns):
    return jnp.concatenate([piece(kind, x, t) for t in range(NB) for x in range(ns)], axis=0)


def fold(f, x):
    return f(x.reshape(-1, 8, x.shape[-1]), axis=0)


def attend(heads, piece_of, ns, bias, qt, oacc, ml, vt, sref, arrive=None, first=False, out=None, hook=None):
    rows = ns * SUB
    items = [(u, j) for u in range(len(heads)) for j in ORDER]
    tops = {}

    def scores(i, c):
        u, j = items[i]
        h = heads[u]
        r0, r1 = c
        if j == ORDER[0] and r0 == 0:
            if arrive:
                arrive(u)
            vt[u, :, :ns * T] = by_tile(piece_of(h), 1, ns).T
        parts = [piece_of(h)(0, x % ns, x // ns) for x in range(r0 // SUB, r1 // SUB)]
        s = lax.dot_general(jnp.concatenate(parts, axis=0), qt[h, j * SUB:(j + 1) * SUB].reshape(QB, D), NT,
                            preferred_element_type=F32)
        lo = max(r0, j * rows)
        if lo < r1:
            d = s[lo - r0:] + bias[lo - j * rows:r1 - j * rows]
            s = d if lo == r0 else jnp.concatenate([s[:lo - r0], d], axis=0)
        sref[i % (AHEAD + 1), r0:r1] = s
        m = fold(jnp.max, s)
        tops[i] = jnp.maximum(tops[i], m) if i in tops else m

    def values(i, c, m, acc):
        u, j = items[i]
        r0, r1 = c
        p = jnp.exp2((sref[i % (AHEAD + 1), r0:r1] - m) * C)
        l = fold(jnp.sum, p)
        o = jnp.dot(vt[u, :, r0:r1], p.astype(BF), preferred_element_type=F32)
        return (acc[0] + l, acc[1] + o) if acc else (l, o)

    def finish(i, m, a, l, o):
        u, j = items[i]
        h = heads[u]
        if not first:
            l = ml[h, j, 1:2] * a + l
        if out is None:
            oacc[h, j] = o if first else oacc[h, j] * a + o
            ml[h, j, 0:1] = m
            ml[h, j, 1:2] = l
            return
        r = 1.0 / l
        o = oacc[h, j] * (a * r) + o * r
        out(u)[j * SUB:(j + 1) * SUB] = o.T.astype(BF).reshape(SUB, G, D)

    todo = [(i, c) for i, (u, j) in enumerate(items) for c in chunks((j + 1) * rows)]
    total = len(todo)
    sizes = [len(chunks((j + 1) * rows)) for u, j in items]
    at = 0
    while at < total and todo[at][0] < AHEAD:
        scores(*todo[at])
        at += 1
    for i, (u, j) in enumerate(items):
        if hook and i == HOOK:
            hook()
        top = jnp.max(tops[i], axis=0, keepdims=True)
        m, a = top, None
        if not first:
            m1 = ml[heads[u], j, 0:1]
            m = jnp.maximum(top, m1)
            a = jnp.exp2((m1 - m) * C)
        acc = None
        goal = sum(sizes[:i + AHEAD + 1])
        start = at
        mine = chunks((j + 1) * rows)
        for t, c in enumerate(mine):
            upto = start + (goal - start) * (t + 1) // len(mine)
            while at < upto:
                scores(*todo[at])
                at += 1
            acc = values(i, c, m, acc)
        finish(i, m, a, jnp.sum(acc[0], axis=0, keepdims=True), acc[1])


def near(kv1, chip):
    def of(h):
        return lambda kind, x, t: kv1[h, kind, chip + x // 2, x % 2, t * SUB:(t + 1) * SUB]
    return of


def far(kv2):
    def of(h):
        return lambda kind, x, t: kv2[h, kind, x, t * SUB:(t + 1) * SUB]
    return of


def kernel(q_hbm, k_hbm, v_hbm, ob, qt, kv2, bias2, oacc, ml, raw, wide, kv1, vt, sref, bias0, bias1,
           lsem, qsem, ssem, rsem, lssem, lrsem):
    cx, cy, cz = lax.axis_index("cx"), lax.axis_index("cy"), lax.axis_index("cz")
    me = (cx * 2 + cy) * 2 + cz
    chip = cx * 2 + cy
    link = 1 - (cx + cz - 2 * cx * cz)
    mine = 1 - link

    def over(role):
        x = cx + link - 2 * cx * link
        y = cy + mine - 2 * cy * mine
        return {"cx": x, "cy": y, "cz": x + (1 - role) - 2 * x * (1 - role)}

    sib = {"cz": 1 - cz}

    loads = [pltpu.make_async_copy(x, raw.at[i], lsem.at[i]) for i, x in enumerate((k_hbm, v_hbm))]
    for x in loads:
        x.start()

    barrier = pltpu.get_barrier_semaphore()
    for dev in ({"cy": 1 - cy, "cz": 1 - cx}, {"cx": 1 - cx, "cz": 1 - cx}, sib):
        pl.semaphore_signal(barrier, inc=1, device_id=dev, device_id_type=pl.DeviceIdType.MESH)

    def qload(h):
        return pltpu.make_async_copy(q_hbm.at[:, pl.ds(pl.multiple_of(h * G, G), G), :], qt.at[h], qsem.at[h])

    def rdma(src, dst, send, recv, h, dev):
        return pltpu.make_async_remote_copy(src, dst, ssem.at[send, h], rsem.at[recv, h], dev,
                                            pl.DeviceIdType.MESH)

    def swap(h):
        return rdma(kv1.at[h, :, 0, cz], kv1.at[h, :, 0, cz], 0, 5, h, sib)

    def out(h, i, n):
        heads = pl.ds(h, n)
        return rdma(kv1.at[heads, i, 0], kv1.at[heads, i, 1 + link], 1 + i, link, h, over(1 - i))

    def half(h, i, z):
        return rdma(kv1.at[h, i, 0, z], kv1.at[h, i, 1 + link, z], 1 + i, link, h, over(1 - i))

    def relay(h):
        return rdma(kv1.at[h, mine, 1:3], kv1.at[h, mine, 1:3], 3, 2, h, sib)

    def forward(h, z=None):
        src, dst = kv1.at[h, mine, 2 - link], kv2.at[h, mine]
        if z is None:
            return rdma(src, dst, 4, 3, h, over(link))
        return pltpu.make_async_remote_copy(src.at[z], dst.at[z], lssem.at[6 + z], lrsem.at[6 + z], over(link),
                                            pl.DeviceIdType.MESH)

    def last(part):
        z, rows = ((0, pl.ds(0, T)), (1, pl.ds(0, CUT)), (1, pl.ds(CUT, T - CUT)), (1, pl.ds(CUT, T - CUT)))[part]
        return pltpu.make_async_remote_copy(kv1.at[HKV - 1, mine, 2 - link, z, rows], kv2.at[HKV - 1, mine, z, rows],
                                            lssem.at[part], lrsem.at[part], over(mine if part == 3 else link),
                                            pl.DeviceIdType.MESH)

    def last_relay(z):
        rows = pl.ds(0, CUT if z else T)
        return pltpu.make_async_remote_copy(kv2.at[HKV - 1, mine, z, rows], kv2.at[HKV - 1, mine, z, rows],
                                            lssem.at[4 + z], lrsem.at[4 + z], sib, pl.DeviceIdType.MESH)

    def relay2(h):
        return rdma(kv2.at[h, mine], kv2.at[h, mine], 5, 4, h, sib)

    def arrived(dst, recv, h):
        rdma(dst, dst, 0, recv, h, sib).wait_recv()

    def mask(nslot, far_chip, ref):
        r = lax.broadcasted_iota(jnp.int32, (nslot * SUB, QB), 0)
        c = lax.broadcasted_iota(jnp.int32, (nslot * SUB, QB), 1)
        x = r // SUB
        kpos = (r % SUB) * 8 + (chip ^ (x // 2 + far_chip)) * 2 + x % 2
        qpos = (c // G) * 8 + me
        ref[...] = jnp.where(kpos <= qpos, 0.0, -1e30)

    def relaid(h, i):
        kv1[h, i, 0, cz] = wide[i, pl.ds(h, T, stride=HKV), :].astype(BF)

    def relaid(h, i):
        kv1[h, i, 0, cz] = wide[i, pl.ds(h, T, stride=HKV), :].astype(BF)

    for i in range(2):
        loads[i].wait()
        wide[i] = raw[i].astype(F32).reshape(T * HKV, D)
        relaid(0, i)
        if i == 0:
            pl.semaphore_wait(barrier, 3)
        else:
            relaid(1, 0)
        half(0, i, cz).start()
    swap(0).start()
    relaid(1, 1)

    for h in range(2, HKV):
        for i in range(2):
            relaid(h, i)
        if h == 2:
            for i in range(2):
                half(1, i, cz).start()
        swap(h - 1).start()

    mask(2, 0, bias0)
    swap(HKV - 1).start()

    for h in range(2):
        arrived(kv1.at[h, :, 0, cz], 5, h)
        for i in range(2):
            half(h, i, 1 - cz).start()

    for h, n in SENDS:
        for x in range(h, h + n):
            arrived(kv1.at[x, :, 0, cz], 5, x)
        for i in range(2):
            out(h, i, n).start()

    @pl.loop(0, HKV)
    def _(h):
        qload(h).start()

    mask(4, 1, bias1)
    mask(2, 3, bias2)

    def pass_on(h):
        middle = (h >= 2) & (h < 6)

        @pl.when(jnp.logical_not(middle))
        def _():
            arrived(kv1.at[h, mine, 1], 0, h)
            arrived(kv1.at[h, mine, 2], 1, h)

        @pl.when(middle & (h % 2 == 0))
        def _():
            arrived(kv1.at[0:2, mine, 1], 0, h)
            arrived(kv1.at[0:2, mine, 2], 1, h)

        relay(h).start()

        @pl.when(h < HKV - 2)
        def _():
            forward(h).start()

        @pl.when(h == HKV - 2)
        def _():
            for z in range(2):
                forward(h, z).start()

        @pl.when(h == HKV - 1)
        def _():
            for part in range(4):
                last(part).start()

    def pass_on2(h):
        @pl.when(h < HKV - 2)
        def _():
            arrived(kv2.at[h, mine], 3, h)
            relay2(h).start()

        @pl.when(h == HKV - 2)
        def _():
            for z in range(2):
                forward(h, z).wait_recv()
                rdma(kv2.at[h, mine, z], kv2.at[h, mine, z], 5, 4, h, sib).start()

        @pl.when(h == HKV - 1)
        def _():
            for z in range(2):
                last(z).wait_recv()
                last_relay(z).start()

    @pl.loop(0, HKV // U0)
    def _(g):
        heads = [g * U0 + u for u in range(U0)]

        def arrive(u):
            h = heads[u]
            qload(h).wait()

        attend(heads, near(kv1, 0), 2, bias0, qt, oacc, ml, vt, sref, arrive, first=True)

    pass_on(jnp.int32(0))

    @pl.loop(0, HKV - 1)
    def _(h):
        pass_on(h + 1)
        arrived(kv1.at[h, link, 1:3], 2, h)
        attend([h], near(kv1, 1), 4, bias1, qt, oacc, ml, vt, sref)

    arrived(kv1.at[HKV - 1, link, 1:3], 2, HKV - 1)
    attend([HKV - 1], near(kv1, 1), 4, bias1, qt, oacc, ml, vt, sref, hook=lambda: pass_on2(jnp.int32(0)))

    for h, n in ((0, 1), (1, 1)) + SENDS:
        for i in range(2):
            out(h, i, n).wait_send()

    @pl.loop(0, HKV)
    def _(h):
        swap(h).wait_send()
        relay(h).wait_send()

    def diagonal(h, before=None):
        pass_on2(h + 1)
        if before:
            before()
        arrived(kv2.at[h, link], 4, h)
        attend([h], far(kv2), 2, bias2, qt, oacc, ml, vt, sref, out=lambda u: ob.at[h])

    @pl.loop(0, HKV - 2)
    def _(h):
        diagonal(h)

    def old_sends():
        @pl.loop(0, HKV - 2)
        def _(h):
            forward(h).wait_send()
            relay2(h).wait_send()

    diagonal(jnp.int32(HKV - 2), old_sends)
    for z in range(2):
        forward(HKV - 2, z).wait_send()
    relay2(HKV - 2).wait_send()
    for z in range(2):
        last_relay(z).wait_recv()
    for part in (2, 3):
        last(part).wait_recv()

    for part in range(4):
        last(part).wait_send()
    for z in range(2):
        last_relay(z).wait_send()


def spread(ob, qt, kv2, bias2, oacc, ml, o_hbm, last, vt, sref, sem):
    def put(src, h):
        return pltpu.make_async_copy(src, o_hbm.at[:, pl.ds(pl.multiple_of(h * G, G), G), :], sem.at[h])

    @pl.loop(0, HKV - 1)
    def _(h):
        put(ob.at[h], h).start()

    attend([HKV - 1], far(kv2), 2, bias2, qt, oacc, ml, vt, sref, out=lambda u: last)
    put(last, HKV - 1).start()

    @pl.loop(0, HKV - 1)
    def _(h):
        put(ob.at[h], h).wait()

    put(last, HKV - 1).wait()


def solution(mesh):
    spec = P(("dp", "cx", "cy", "cz"))

    def local(q, k, v):
        hbm = pl.BlockSpec(memory_space=pltpu.HBM)
        vmem = pl.BlockSpec(memory_space=pltpu.VMEM)
        parts = pl.pallas_call(
            kernel,
            out_shape=[
                pltpu.VMEM((HKV - 1, T, G, D), BF),
                pltpu.VMEM((HKV, T, G, D), BF),
                pltpu.VMEM((HKV, 2, 2, T, D), BF),
                pltpu.VMEM((S2 * SUB, QB), F32),
                pltpu.VMEM((HKV, NB, D, QB), F32),
                pltpu.VMEM((HKV, NB, 8, QB), F32),
            ],
            in_specs=[hbm] * 3,
            out_specs=[vmem] * 6,
            scratch_shapes=[
                pltpu.VMEM((2, T, HKV, D), BF),
                pltpu.VMEM((2, T * HKV, D), F32),
                pltpu.VMEM((HKV, 2, 3, 2, T, D), BF),
                pltpu.VMEM((max(U0, U1, U2), D, 4 * T), BF),
                pltpu.VMEM((AHEAD + 1, 4 * T, QB), F32),
                pltpu.VMEM((2 * SUB, QB), F32),
                pltpu.VMEM((4 * SUB, QB), F32),
                pltpu.SemaphoreType.DMA((2,)),
                pltpu.SemaphoreType.DMA((HKV,)),
                pltpu.SemaphoreType.DMA((6, HKV)),
                pltpu.SemaphoreType.DMA((6, HKV)),
                pltpu.SemaphoreType.DMA((8,)),
                pltpu.SemaphoreType.DMA((8,)),
            ],
            compiler_params=pltpu.CompilerParams(
                vmem_limit_bytes=36 << 20, collective_id=0, has_side_effects=True),
        )(*(pltpu.with_memory_space_constraint(x, pltpu.HBM) for x in (q, k, v)))
        return pl.pallas_call(
            spread,
            out_shape=jax.ShapeDtypeStruct(q.shape, q.dtype),
            in_specs=[vmem] * 6,
            out_specs=hbm,
            scratch_shapes=[
                pltpu.VMEM((T, G, D), BF),
                pltpu.VMEM((1, D, S2 * T), BF),
                pltpu.VMEM((AHEAD + 1, S2 * T, QB), F32),
                pltpu.SemaphoreType.DMA((HKV,)),
            ],
            compiler_params=pltpu.CompilerParams(vmem_limit_bytes=8 << 20),
        )(*parts)

    return jax.shard_map(local, mesh=mesh, in_specs=(spec, spec, spec), out_specs=spec, check_vma=False)
```

```python
import jax
import jax.numpy as jnp
from jax import lax
from jax.experimental import pallas as pl
from jax.experimental.pallas import tpu as pltpu
from jax.sharding import PartitionSpec as P

T = 256
CUT = 128
SENDS = ((2, 2), (4, 2), (6, 1), (7, 1))
HKV = 8
G = 8
D = 128
NB = 8
SUB = T // NB
QB = SUB * G
S1 = 6
S2 = 2
C = (D ** -0.5) * 1.4426950408889634
ORDER = (0, 2, 4, 6, 7, 5, 3, 1)
AHEAD = 4
U0, U1, U2 = 1, 1, 1
BF = jnp.bfloat16
F32 = jnp.float32
NT = (((1,), (1,)), ((), ()))


def chunks(n):
    return [(r, min(r + 256, n)) for r in range(0, n, 256)]


def by_tile(piece, kind, ns):
    return jnp.concatenate([piece(kind, x, t) for t in range(NB) for x in range(ns)], axis=0)


def fold(f, x):
    return f(x.reshape(-1, 8, x.shape[-1]), axis=0)


def attend(heads, piece_of, ns, bias, qt, oacc, ml, vt, sref, arrive=None, first=False, out=None, hook=None):
    rows = ns * SUB
    items = [(u, j) for u in range(len(heads)) for j in ORDER]
    tops = {}

    def scores(i, c):
        u, j = items[i]
        h = heads[u]
        r0, r1 = c
        if j == ORDER[0] and r0 == 0:
            if arrive:
                arrive(u)
            vt[u, :, :ns * T] = by_tile(piece_of(h), 1, ns).T
        parts = [piece_of(h)(0, x % ns, x // ns) for x in range(r0 // SUB, r1 // SUB)]
        s = lax.dot_general(jnp.concatenate(parts, axis=0), qt[h, j * SUB:(j + 1) * SUB].reshape(QB, D), NT,
                            preferred_element_type=F32)
        lo = max(r0, j * rows)
        if lo < r1:
            d = s[lo - r0:] + bias[lo - j * rows:r1 - j * rows]
            s = d if lo == r0 else jnp.concatenate([s[:lo - r0], d], axis=0)
        sref[i % (AHEAD + 1), r0:r1] = s
        m = fold(jnp.max, s)
        tops[i] = jnp.maximum(tops[i], m) if i in tops else m

    def values(i, c, m, acc):
        u, j = items[i]
        r0, r1 = c
        p = jnp.exp2((sref[i % (AHEAD + 1), r0:r1] - m) * C)
        l = fold(jnp.sum, p)
        o = jnp.dot(vt[u, :, r0:r1], p.astype(BF), preferred_element_type=F32)
        return (acc[0] + l, acc[1] + o) if acc else (l, o)

    def finish(i, m, a, l, o):
        u, j = items[i]
        h = heads[u]
        if not first:
            l = ml[h, j, 1:2] * a + l
        if out is None:
            oacc[h, j] = o if first else oacc[h, j] * a + o
            ml[h, j, 0:1] = m
            ml[h, j, 1:2] = l
            return
        r = 1.0 / l
        o = oacc[h, j] * (a * r) + o * r
        out(u)[j * SUB:(j + 1) * SUB] = o.T.astype(BF).reshape(SUB, G, D)

    todo = [(i, c) for i, (u, j) in enumerate(items) for c in chunks((j + 1) * rows)]
    total = len(todo)
    sizes = [len(chunks((j + 1) * rows)) for u, j in items]
    at = 0
    while at < total and todo[at][0] < AHEAD:
        scores(*todo[at])
        at += 1
    for i, (u, j) in enumerate(items):
        if hook and i == hook[0]:
            hook[1]()
        top = jnp.max(tops[i], axis=0, keepdims=True)
        m, a = top, None
        if not first:
            m1 = ml[heads[u], j, 0:1]
            m = jnp.maximum(top, m1)
            a = jnp.exp2((m1 - m) * C)
        acc = None
        goal = sum(sizes[:i + AHEAD + 1])
        start = at
        mine = chunks((j + 1) * rows)
        for t, c in enumerate(mine):
            upto = start + (goal - start) * (t + 1) // len(mine)
            while at < upto:
                scores(*todo[at])
                at += 1
            acc = values(i, c, m, acc)
        finish(i, m, a, jnp.sum(acc[0], axis=0, keepdims=True), acc[1])


def near(kv1, chip):
    def of(h):
        return lambda kind, x, t: kv1[h, kind, chip + x // 2, x % 2, t * SUB:(t + 1) * SUB]
    return of


def far(kv2):
    def of(h):
        return lambda kind, x, t: kv2[h, kind, x, t * SUB:(t + 1) * SUB]
    return of


def kernel(q_hbm, k_hbm, v_hbm, ob, qt, kv2, bias2, oacc, ml, raw, wide, kv1, vt, sref, bias0, bias1,
           lsem, qsem, ssem, rsem, lssem, lrsem):
    cx, cy, cz = lax.axis_index("cx"), lax.axis_index("cy"), lax.axis_index("cz")
    me = (cx * 2 + cy) * 2 + cz
    chip = cx * 2 + cy
    link = 1 - (cx + cz - 2 * cx * cz)
    mine = 1 - link

    def over(role):
        x = cx + link - 2 * cx * link
        y = cy + mine - 2 * cy * mine
        return {"cx": x, "cy": y, "cz": x + (1 - role) - 2 * x * (1 - role)}

    sib = {"cz": 1 - cz}

    loads = [pltpu.make_async_copy(x, raw.at[i], lsem.at[i]) for i, x in enumerate((k_hbm, v_hbm))]
    for x in loads:
        x.start()

    barrier = pltpu.get_barrier_semaphore()
    for dev in ({"cy": 1 - cy, "cz": 1 - cx}, {"cx": 1 - cx, "cz": 1 - cx}, sib):
        pl.semaphore_signal(barrier, inc=1, device_id=dev, device_id_type=pl.DeviceIdType.MESH)

    def qload(h):
        return pltpu.make_async_copy(q_hbm.at[:, pl.ds(pl.multiple_of(h * G, G), G), :], qt.at[h], qsem.at[h])

    def rdma(src, dst, send, recv, h, dev):
        return pltpu.make_async_remote_copy(src, dst, ssem.at[send, h], rsem.at[recv, h], dev,
                                            pl.DeviceIdType.MESH)

    def swap(h):
        return rdma(kv1.at[h, :, 0, cz], kv1.at[h, :, 0, cz], 0, 5, h, sib)

    def out(h, i, n):
        heads = pl.ds(h, n)
        return rdma(kv1.at[heads, i, 0], kv1.at[heads, i, 1 + link], 1 + i, link, h, over(1 - i))

    def half(h, i, z):
        return rdma(kv1.at[h, i, 0, z], kv1.at[h, i, 1 + link, z], 1 + i, link, h, over(1 - i))

    def relay(h):
        return rdma(kv1.at[h, mine, 1:3], kv1.at[h, mine, 1:3], 3, 2, h, sib)

    def forward(h, z=None):
        src, dst = kv1.at[h, mine, 2 - link], kv2.at[h, mine]
        if z is None:
            return rdma(src, dst, 4, 3, h, over(link))
        return pltpu.make_async_remote_copy(src.at[z], dst.at[z], lssem.at[6 + z], lrsem.at[6 + z], over(link),
                                            pl.DeviceIdType.MESH)

    def last(part):
        z, rows = ((0, pl.ds(0, T)), (1, pl.ds(0, CUT)), (1, pl.ds(CUT, T - CUT)), (1, pl.ds(CUT, T - CUT)))[part]
        return pltpu.make_async_remote_copy(kv1.at[HKV - 1, mine, 2 - link, z, rows], kv2.at[HKV - 1, mine, z, rows],
                                            lssem.at[part], lrsem.at[part], over(mine if part == 3 else link),
                                            pl.DeviceIdType.MESH)

    def last_relay(z):
        rows = pl.ds(0, CUT if z else T)
        return pltpu.make_async_remote_copy(kv2.at[HKV - 1, mine, z, rows], kv2.at[HKV - 1, mine, z, rows],
                                            lssem.at[4 + z], lrsem.at[4 + z], sib, pl.DeviceIdType.MESH)

    def relay2(h):
        return rdma(kv2.at[h, mine], kv2.at[h, mine], 5, 4, h, sib)

    def arrived(dst, recv, h):
        rdma(dst, dst, 0, recv, h, sib).wait_recv()

    def mask(nslot, far_chip, ref):
        r = lax.broadcasted_iota(jnp.int32, (nslot * SUB, QB), 0)
        c = lax.broadcasted_iota(jnp.int32, (nslot * SUB, QB), 1)
        x = r // SUB
        kpos = (r % SUB) * 8 + (chip ^ (x // 2 + far_chip)) * 2 + x % 2
        qpos = (c // G) * 8 + me
        ref[...] = jnp.where(kpos <= qpos, 0.0, -1e30)

    def relaid(h, i):
        kv1[h, i, 0, cz] = wide[i, pl.ds(h, T, stride=HKV), :].astype(BF)

    def relaid(h, i):
        kv1[h, i, 0, cz] = wide[i, pl.ds(h, T, stride=HKV), :].astype(BF)

    for i in range(2):
        loads[i].wait()
        wide[i] = raw[i].astype(F32).reshape(T * HKV, D)
        relaid(0, i)
        if i == 0:
            pl.semaphore_wait(barrier, 3)
        else:
            relaid(1, 0)
        half(0, i, cz).start()
    swap(0).start()
    relaid(1, 1)

    for h in range(2, HKV):
        for i in range(2):
            relaid(h, i)
        if h == 2:
            for i in range(2):
                half(1, i, cz).start()
        swap(h - 1).start()

    mask(2, 0, bias0)
    swap(HKV - 1).start()

    for h in range(2):
        arrived(kv1.at[h, :, 0, cz], 5, h)
        for i in range(2):
            half(h, i, 1 - cz).start()

    for h, n in SENDS:
        for x in range(h, h + n):
            arrived(kv1.at[x, :, 0, cz], 5, x)
        for i in range(2):
            out(h, i, n).start()

    @pl.loop(0, HKV)
    def _(h):
        qload(h).start()

    mask(4, 1, bias1)
    mask(2, 3, bias2)

    def pass_on(h):
        middle = (h >= 2) & (h < 6)

        @pl.when(jnp.logical_not(middle))
        def _():
            arrived(kv1.at[h, mine, 1], 0, h)
            arrived(kv1.at[h, mine, 2], 1, h)

        @pl.when(middle & (h % 2 == 0))
        def _():
            arrived(kv1.at[0:2, mine, 1], 0, h)
            arrived(kv1.at[0:2, mine, 2], 1, h)

        relay(h).start()

        @pl.when(h < HKV - 2)
        def _():
            forward(h).start()

        @pl.when(h == HKV - 2)
        def _():
            for z in range(2):
                forward(h, z).start()

        @pl.when(h == HKV - 1)
        def _():
            for part in range(4):
                last(part).start()

    def pass_on2(h):
        @pl.when(h < HKV - 2)
        def _():
            arrived(kv2.at[h, mine], 3, h)
            relay2(h).start()

        @pl.when(h == HKV - 2)
        def _():
            for z in range(2):
                forward(h, z).wait_recv()
                rdma(kv2.at[h, mine, z], kv2.at[h, mine, z], 5, 4, h, sib).start()

        @pl.when(h == HKV - 1)
        def _():
            last(0).wait_recv()
            last_relay(0).start()

    @pl.loop(0, HKV // U0)
    def _(g):
        heads = [g * U0 + u for u in range(U0)]

        def arrive(u):
            h = heads[u]
            qload(h).wait()

        attend(heads, near(kv1, 0), 2, bias0, qt, oacc, ml, vt, sref, arrive, first=True)

    pass_on(jnp.int32(0))

    def neighbours(h, hook=None):
        arrived(kv1.at[h, link, 1:3], 2, h)
        attend([h], near(kv1, 1), 4, bias1, qt, oacc, ml, vt, sref, hook=hook)

    @pl.loop(0, HKV - 2)
    def _(h):
        pass_on(h + 1)
        neighbours(h)

    neighbours(HKV - 2, (6, lambda: pass_on(jnp.int32(HKV - 1))))
    neighbours(HKV - 1, (4, lambda: pass_on2(jnp.int32(0))))

    for h, n in ((0, 1), (1, 1)) + SENDS:
        for i in range(2):
            out(h, i, n).wait_send()

    @pl.loop(0, HKV)
    def _(h):
        swap(h).wait_send()
        relay(h).wait_send()

    def diagonal(h, before=None, hook=None):
        pass_on2(h + 1)
        if before:
            before()
        arrived(kv2.at[h, link], 4, h)
        attend([h], far(kv2), 2, bias2, qt, oacc, ml, vt, sref, out=lambda u: ob.at[h], hook=hook)

    @pl.loop(0, HKV - 2)
    def _(h):
        diagonal(h)

    def old_sends():
        @pl.loop(0, HKV - 2)
        def _(h):
            forward(h).wait_send()
            relay2(h).wait_send()

    def late():
        last(1).wait_recv()
        last_relay(1).start()

    diagonal(jnp.int32(HKV - 2), old_sends, (3, late))
    for z in range(2):
        forward(HKV - 2, z).wait_send()
    relay2(HKV - 2).wait_send()
    for z in range(2):
        last_relay(z).wait_recv()
    for part in (2, 3):
        last(part).wait_recv()

    for part in range(4):
        last(part).wait_send()
    for z in range(2):
        last_relay(z).wait_send()


def spread(ob, qt, kv2, bias2, oacc, ml, o_hbm, last, vt, sref, sem):
    def put(src, h):
        return pltpu.make_async_copy(src, o_hbm.at[:, pl.ds(pl.multiple_of(h * G, G), G), :], sem.at[h])

    @pl.loop(0, HKV - 1)
    def _(h):
        put(ob.at[h], h).start()

    attend([HKV - 1], far(kv2), 2, bias2, qt, oacc, ml, vt, sref, out=lambda u: last)
    put(last, HKV - 1).start()

    @pl.loop(0, HKV - 1)
    def _(h):
        put(ob.at[h], h).wait()

    put(last, HKV - 1).wait()


def solution(mesh):
    spec = P(("dp", "cx", "cy", "cz"))

    def local(q, k, v):
        hbm = pl.BlockSpec(memory_space=pltpu.HBM)
        vmem = pl.BlockSpec(memory_space=pltpu.VMEM)
        parts = pl.pallas_call(
            kernel,
            out_shape=[
                pltpu.VMEM((HKV - 1, T, G, D), BF),
                pltpu.VMEM((HKV, T, G, D), BF),
                pltpu.VMEM((HKV, 2, 2, T, D), BF),
                pltpu.VMEM((S2 * SUB, QB), F32),
                pltpu.VMEM((HKV, NB, D, QB), F32),
                pltpu.VMEM((HKV, NB, 8, QB), F32),
            ],
            in_specs=[hbm] * 3,
            out_specs=[vmem] * 6,
            scratch_shapes=[
                pltpu.VMEM((2, T, HKV, D), BF),
                pltpu.VMEM((2, T * HKV, D), F32),
                pltpu.VMEM((HKV, 2, 3, 2, T, D), BF),
                pltpu.VMEM((max(U0, U1, U2), D, 4 * T), BF),
                pltpu.VMEM((AHEAD + 1, 4 * T, QB), F32),
                pltpu.VMEM((2 * SUB, QB), F32),
                pltpu.VMEM((4 * SUB, QB), F32),
                pltpu.SemaphoreType.DMA((2,)),
                pltpu.SemaphoreType.DMA((HKV,)),
                pltpu.SemaphoreType.DMA((6, HKV)),
                pltpu.SemaphoreType.DMA((6, HKV)),
                pltpu.SemaphoreType.DMA((8,)),
                pltpu.SemaphoreType.DMA((8,)),
            ],
            compiler_params=pltpu.CompilerParams(
                vmem_limit_bytes=36 << 20, collective_id=0, has_side_effects=True),
        )(*(pltpu.with_memory_space_constraint(x, pltpu.HBM) for x in (q, k, v)))
        return pl.pallas_call(
            spread,
            out_shape=jax.ShapeDtypeStruct(q.shape, q.dtype),
            in_specs=[vmem] * 6,
            out_specs=hbm,
            scratch_shapes=[
                pltpu.VMEM((T, G, D), BF),
                pltpu.VMEM((1, D, S2 * T), BF),
                pltpu.VMEM((AHEAD + 1, S2 * T, QB), F32),
                pltpu.SemaphoreType.DMA((HKV,)),
            ],
            compiler_params=pltpu.CompilerParams(vmem_limit_bytes=8 << 20),
        )(*parts)

    return jax.shard_map(local, mesh=mesh, in_specs=(spec, spec, spec), out_specs=spec, check_vma=False)
```

```python
import jax
import jax.numpy as jnp
from jax import lax
from jax.experimental import pallas as pl
from jax.experimental.pallas import tpu as pltpu
from jax.sharding import PartitionSpec as P

T = 256
CUT = 128
SENDS = ((2, 2), (4, 2), (6, 1), (7, 1))
HKV = 8
G = 8
D = 128
NB = 8
SUB = T // NB
QB = SUB * G
S1 = 6
S2 = 2
C = (D ** -0.5) * 1.4426950408889634
ORDER = (0, 2, 4, 6, 7, 5, 3, 1)
AHEAD = 4
U0, U1, U2 = 1, 1, 1
BF = jnp.bfloat16
F32 = jnp.float32
NT = (((1,), (1,)), ((), ()))


def chunks(n):
    return [(r, min(r + 256, n)) for r in range(0, n, 256)]


def by_tile(piece, kind, ns):
    return jnp.concatenate([piece(kind, x, t) for t in range(NB) for x in range(ns)], axis=0)


def fold(f, x):
    return f(x.reshape(-1, 8, x.shape[-1]), axis=0)


def attend(heads, piece_of, ns, bias, qt, oacc, ml, vt, sref, arrive=None, first=False, out=None, hook=None):
    rows = ns * SUB
    items = [(u, j) for u in range(len(heads)) for j in ORDER]
    tops = {}

    def scores(i, c):
        u, j = items[i]
        h = heads[u]
        r0, r1 = c
        if j == ORDER[0] and r0 == 0:
            if arrive:
                arrive(u)
            vt[u, :, :ns * T] = by_tile(piece_of(h), 1, ns).T
        parts = [piece_of(h)(0, x % ns, x // ns) for x in range(r0 // SUB, r1 // SUB)]
        s = lax.dot_general(jnp.concatenate(parts, axis=0), qt[h, j * SUB:(j + 1) * SUB].reshape(QB, D), NT,
                            preferred_element_type=F32)
        lo = max(r0, j * rows)
        if lo < r1:
            d = s[lo - r0:] + bias[lo - j * rows:r1 - j * rows]
            s = d if lo == r0 else jnp.concatenate([s[:lo - r0], d], axis=0)
        sref[i % (AHEAD + 1), r0:r1] = s
        m = fold(jnp.max, s)
        tops[i] = jnp.maximum(tops[i], m) if i in tops else m

    def values(i, c, m, acc):
        u, j = items[i]
        r0, r1 = c
        p = jnp.exp2((sref[i % (AHEAD + 1), r0:r1] - m) * C)
        l = fold(jnp.sum, p)
        o = jnp.dot(vt[u, :, r0:r1], p.astype(BF), preferred_element_type=F32)
        return (acc[0] + l, acc[1] + o) if acc else (l, o)

    def finish(i, m, a, l, o):
        u, j = items[i]
        h = heads[u]
        if not first:
            l = ml[h, j, 1:2] * a + l
        if out is None:
            oacc[h, j] = o if first else oacc[h, j] * a + o
            ml[h, j, 0:1] = m
            ml[h, j, 1:2] = l
            return
        r = 1.0 / l
        o = oacc[h, j] * (a * r) + o * r
        out(u)[j * SUB:(j + 1) * SUB] = o.T.astype(BF).reshape(SUB, G, D)

    todo = [(i, c) for i, (u, j) in enumerate(items) for c in chunks((j + 1) * rows)]
    total = len(todo)
    sizes = [len(chunks((j + 1) * rows)) for u, j in items]
    at = 0
    while at < total and todo[at][0] < AHEAD:
        scores(*todo[at])
        at += 1
    for i, (u, j) in enumerate(items):
        if hook and i == hook[0]:
            hook[1]()
        top = jnp.max(tops[i], axis=0, keepdims=True)
        m, a = top, None
        if not first:
            m1 = ml[heads[u], j, 0:1]
            m = jnp.maximum(top, m1)
            a = jnp.exp2((m1 - m) * C)
        acc = None
        goal = sum(sizes[:i + AHEAD + 1])
        start = at
        mine = chunks((j + 1) * rows)
        for t, c in enumerate(mine):
            upto = start + (goal - start) * (t + 1) // len(mine)
            while at < upto:
                scores(*todo[at])
                at += 1
            acc = values(i, c, m, acc)
        finish(i, m, a, jnp.sum(acc[0], axis=0, keepdims=True), acc[1])


def near(kv1, chip):
    def of(h):
        return lambda kind, x, t: kv1[h, kind, chip + x // 2, x % 2, t * SUB:(t + 1) * SUB]
    return of


def far(kv2):
    def of(h):
        return lambda kind, x, t: kv2[h, kind, x, t * SUB:(t + 1) * SUB]
    return of


def kernel(q_hbm, k_hbm, v_hbm, ob, qt, kv2, bias2, oacc, ml, raw, wide, kv1, vt, sref, bias0, bias1,
           lsem, qsem, ssem, rsem, lssem, lrsem):
    cx, cy, cz = lax.axis_index("cx"), lax.axis_index("cy"), lax.axis_index("cz")
    me = (cx * 2 + cy) * 2 + cz
    chip = cx * 2 + cy
    link = 1 - (cx + cz - 2 * cx * cz)
    mine = 1 - link

    def over(role):
        x = cx + link - 2 * cx * link
        y = cy + mine - 2 * cy * mine
        return {"cx": x, "cy": y, "cz": x + (1 - role) - 2 * x * (1 - role)}

    sib = {"cz": 1 - cz}

    barrier = pltpu.get_barrier_semaphore()
    for dev in ({"cy": 1 - cy, "cz": 1 - cx}, {"cx": 1 - cx, "cz": 1 - cx}, sib):
        pl.semaphore_signal(barrier, inc=1, device_id=dev, device_id_type=pl.DeviceIdType.MESH)

    loads = [pltpu.make_async_copy(x, raw.at[i], lsem.at[i]) for i, x in enumerate((k_hbm, v_hbm))]
    for x in loads:
        x.start()

    def qload(h):
        return pltpu.make_async_copy(q_hbm.at[:, pl.ds(pl.multiple_of(h * G, G), G), :], qt.at[h], qsem.at[h])

    def rdma(src, dst, send, recv, h, dev):
        return pltpu.make_async_remote_copy(src, dst, ssem.at[send, h], rsem.at[recv, h], dev,
                                            pl.DeviceIdType.MESH)

    def swap(h):
        return rdma(kv1.at[h, :, 0, cz], kv1.at[h, :, 0, cz], 0, 5, h, sib)

    def out(h, i, n):
        heads = pl.ds(h, n)
        return rdma(kv1.at[heads, i, 0], kv1.at[heads, i, 1 + link], 1 + i, link, h, over(1 - i))

    def half(h, i, z):
        return rdma(kv1.at[h, i, 0, z], kv1.at[h, i, 1 + link, z], 1 + i, link, h, over(1 - i))

    def relay(h):
        return rdma(kv1.at[h, mine, 1:3], kv1.at[h, mine, 1:3], 3, 2, h, sib)

    def forward(h):
        return rdma(kv1.at[h, mine, 2 - link], kv2.at[h, mine], 4, 3, h, over(link))

    def last(part):
        z, rows = ((0, pl.ds(0, T)), (1, pl.ds(0, CUT)), (1, pl.ds(CUT, T - CUT)), (1, pl.ds(CUT, T - CUT)))[part]
        return pltpu.make_async_remote_copy(kv1.at[HKV - 1, mine, 2 - link, z, rows], kv2.at[HKV - 1, mine, z, rows],
                                            lssem.at[part], lrsem.at[part], over(mine if part == 3 else link),
                                            pl.DeviceIdType.MESH)

    def last_relay(z):
        rows = pl.ds(0, CUT if z else T)
        return pltpu.make_async_remote_copy(kv2.at[HKV - 1, mine, z, rows], kv2.at[HKV - 1, mine, z, rows],
                                            lssem.at[4 + z], lrsem.at[4 + z], sib, pl.DeviceIdType.MESH)

    def relay2(h):
        return rdma(kv2.at[h, mine], kv2.at[h, mine], 5, 4, h, sib)

    def arrived(dst, recv, h):
        rdma(dst, dst, 0, recv, h, sib).wait_recv()

    def mask(nslot, far_chip, ref):
        r = lax.broadcasted_iota(jnp.int32, (nslot * SUB, QB), 0)
        c = lax.broadcasted_iota(jnp.int32, (nslot * SUB, QB), 1)
        x = r // SUB
        kpos = (r % SUB) * 8 + (chip ^ (x // 2 + far_chip)) * 2 + x % 2
        qpos = (c // G) * 8 + me
        ref[...] = jnp.where(kpos <= qpos, 0.0, -1e30)

    def relaid(h, i):
        kv1[h, i, 0, cz] = wide[i, pl.ds(h, T, stride=HKV), :].astype(BF)

    def relaid(h, i):
        kv1[h, i, 0, cz] = wide[i, pl.ds(h, T, stride=HKV), :].astype(BF)

    for i in range(2):
        loads[i].wait()
        wide[i] = raw[i].astype(F32).reshape(T * HKV, D)
        relaid(0, i)
        if i == 0:
            pl.semaphore_wait(barrier, 3)
        else:
            relaid(1, 0)
        half(0, i, cz).start()
    swap(0).start()
    relaid(1, 1)

    for h in range(2, HKV):
        for i in range(2):
            relaid(h, i)
        if h == 2:
            for i in range(2):
                half(1, i, cz).start()
        swap(h - 1).start()

    mask(2, 0, bias0)
    swap(HKV - 1).start()

    for h in range(2):
        arrived(kv1.at[h, :, 0, cz], 5, h)
        for i in range(2):
            half(h, i, 1 - cz).start()

    for h, n in SENDS:
        for x in range(h, h + n):
            arrived(kv1.at[x, :, 0, cz], 5, x)
        for i in range(2):
            out(h, i, n).start()

    @pl.loop(0, HKV)
    def _(h):
        qload(h).start()

    mask(4, 1, bias1)
    mask(2, 3, bias2)

    def pass_on(h):
        middle = (h >= 2) & (h < 6)

        @pl.when(jnp.logical_not(middle))
        def _():
            arrived(kv1.at[h, mine, 1], 0, h)
            arrived(kv1.at[h, mine, 2], 1, h)

        @pl.when(middle & (h % 2 == 0))
        def _():
            arrived(kv1.at[0:2, mine, 1], 0, h)
            arrived(kv1.at[0:2, mine, 2], 1, h)

        relay(h).start()

        @pl.when(h < HKV - 1)
        def _():
            forward(h).start()

        @pl.when(h == HKV - 1)
        def _():
            for part in range(4):
                last(part).start()

    def pass_on2(h):
        @pl.when(h < HKV - 1)
        def _():
            arrived(kv2.at[h, mine], 3, h)
            relay2(h).start()

        @pl.when(h == HKV - 1)
        def _():
            for z in range(2):
                last(z).wait_recv()
                last_relay(z).start()

    @pl.loop(0, HKV // U0)
    def _(g):
        heads = [g * U0 + u for u in range(U0)]

        def arrive(u):
            h = heads[u]
            qload(h).wait()

        attend(heads, near(kv1, 0), 2, bias0, qt, oacc, ml, vt, sref, arrive, first=True)

    pass_on(jnp.int32(0))

    def neighbours(h, hook=None):
        arrived(kv1.at[h, link, 1:3], 2, h)
        attend([h], near(kv1, 1), 4, bias1, qt, oacc, ml, vt, sref, hook=hook)

    @pl.loop(0, HKV - 2)
    def _(h):
        pass_on(h + 1)
        neighbours(h)

    neighbours(HKV - 2, (4, lambda: pass_on(jnp.int32(HKV - 1))))
    neighbours(HKV - 1, (4, lambda: pass_on2(jnp.int32(0))))

    for h, n in ((0, 1), (1, 1)) + SENDS:
        for i in range(2):
            out(h, i, n).wait_send()

    @pl.loop(0, HKV)
    def _(h):
        swap(h).wait_send()
        relay(h).wait_send()

    @pl.loop(0, (HKV - 1) // U2)
    def _(g):
        heads = [g * U2 + u for u in range(U2)]

        def arrive(u):
            pass_on2(heads[u] + 1)
            arrived(kv2.at[heads[u], link], 4, heads[u])

        attend(heads, far(kv2), 2, bias2, qt, oacc, ml, vt, sref, arrive, out=lambda u: ob.at[heads[u]])

    @pl.loop(0, HKV - 1)
    def _(h):
        forward(h).wait_send()
        relay2(h).wait_send()

    for z in range(2):
        last_relay(z).wait_recv()
    for part in (2, 3):
        last(part).wait_recv()

    for part in range(4):
        last(part).wait_send()
    for z in range(2):
        last_relay(z).wait_send()


def spread(ob, qt, kv2, bias2, oacc, ml, o_hbm, last, vt, sref, sem):
    def put(src, h):
        return pltpu.make_async_copy(src, o_hbm.at[:, pl.ds(pl.multiple_of(h * G, G), G), :], sem.at[h])

    @pl.loop(0, HKV - 1)
    def _(h):
        put(ob.at[h], h).start()

    attend([HKV - 1], far(kv2), 2, bias2, qt, oacc, ml, vt, sref, out=lambda u: last)
    put(last, HKV - 1).start()

    @pl.loop(0, HKV - 1)
    def _(h):
        put(ob.at[h], h).wait()

    put(last, HKV - 1).wait()


def solution(mesh):
    spec = P(("dp", "cx", "cy", "cz"))

    def local(q, k, v):
        hbm = pl.BlockSpec(memory_space=pltpu.HBM)
        vmem = pl.BlockSpec(memory_space=pltpu.VMEM)
        parts = pl.pallas_call(
            kernel,
            out_shape=[
                pltpu.VMEM((HKV - 1, T, G, D), BF),
                pltpu.VMEM((HKV, T, G, D), BF),
                pltpu.VMEM((HKV, 2, 2, T, D), BF),
                pltpu.VMEM((S2 * SUB, QB), F32),
                pltpu.VMEM((HKV, NB, D, QB), F32),
                pltpu.VMEM((HKV, NB, 8, QB), F32),
            ],
            in_specs=[hbm] * 3,
            out_specs=[vmem] * 6,
            scratch_shapes=[
                pltpu.VMEM((2, T, HKV, D), BF),
                pltpu.VMEM((2, T * HKV, D), F32),
                pltpu.VMEM((HKV, 2, 3, 2, T, D), BF),
                pltpu.VMEM((max(U0, U1, U2), D, 4 * T), BF),
                pltpu.VMEM((AHEAD + 1, 4 * T, QB), F32),
                pltpu.VMEM((2 * SUB, QB), F32),
                pltpu.VMEM((4 * SUB, QB), F32),
                pltpu.SemaphoreType.DMA((2,)),
                pltpu.SemaphoreType.DMA((HKV,)),
                pltpu.SemaphoreType.DMA((6, HKV)),
                pltpu.SemaphoreType.DMA((6, HKV)),
                pltpu.SemaphoreType.DMA((6,)),
                pltpu.SemaphoreType.DMA((6,)),
            ],
            compiler_params=pltpu.CompilerParams(
                vmem_limit_bytes=36 << 20, collective_id=0, has_side_effects=True),
        )(*(pltpu.with_memory_space_constraint(x, pltpu.HBM) for x in (q, k, v)))
        return pl.pallas_call(
            spread,
            out_shape=jax.ShapeDtypeStruct(q.shape, q.dtype),
            in_specs=[vmem] * 6,
            out_specs=hbm,
            scratch_shapes=[
                pltpu.VMEM((T, G, D), BF),
                pltpu.VMEM((1, D, S2 * T), BF),
                pltpu.VMEM((AHEAD + 1, S2 * T, QB), F32),
                pltpu.SemaphoreType.DMA((HKV,)),
            ],
            compiler_params=pltpu.CompilerParams(vmem_limit_bytes=8 << 20),
        )(*parts)

    return jax.shard_map(local, mesh=mesh, in_specs=(spec, spec, spec), out_specs=spec, check_vma=False)
```

```python
import jax
import jax.numpy as jnp
from jax import lax
from jax.experimental import pallas as pl
from jax.experimental.pallas import tpu as pltpu
from jax.sharding import PartitionSpec as P

T = 256
CUT = 128
SENDS = ((2, 2), (4, 2), (6, 1), (7, 1))
HKV = 8
G = 8
D = 128
NB = 8
SUB = T // NB
QB = SUB * G
S1 = 6
S2 = 2
C = (D ** -0.5) * 1.4426950408889634
ORDER = (0, 2, 4, 6, 7, 5, 3, 1)
AHEAD = 4
HOOK = 4
U0, U1, U2 = 1, 1, 1
BF = jnp.bfloat16
F32 = jnp.float32
NT = (((1,), (1,)), ((), ()))


def chunks(n):
    return [(r, min(r + 256, n)) for r in range(0, n, 256)]


def by_tile(piece, kind, ns):
    return jnp.concatenate([piece(kind, x, t) for t in range(NB) for x in range(ns)], axis=0)


def fold(f, x):
    return f(x.reshape(-1, 8, x.shape[-1]), axis=0)


def attend(heads, piece_of, ns, bias, qt, oacc, ml, vt, sref, arrive=None, first=False, out=None, hook=None):
    rows = ns * SUB
    items = [(u, j) for u in range(len(heads)) for j in ORDER]
    tops = {}

    def scores(i, c):
        u, j = items[i]
        h = heads[u]
        r0, r1 = c
        if j == ORDER[0] and r0 == 0:
            if arrive:
                arrive(u)
            vt[u, :, :ns * T] = by_tile(piece_of(h), 1, ns).T
        parts = [piece_of(h)(0, x % ns, x // ns) for x in range(r0 // SUB, r1 // SUB)]
        s = lax.dot_general(jnp.concatenate(parts, axis=0), qt[h, j * SUB:(j + 1) * SUB].reshape(QB, D), NT,
                            preferred_element_type=F32)
        lo = max(r0, j * rows)
        if lo < r1:
            d = s[lo - r0:] + bias[lo - j * rows:r1 - j * rows]
            s = d if lo == r0 else jnp.concatenate([s[:lo - r0], d], axis=0)
        sref[i % (AHEAD + 1), r0:r1] = s
        m = fold(jnp.max, s)
        tops[i] = jnp.maximum(tops[i], m) if i in tops else m

    def values(i, c, m, acc):
        u, j = items[i]
        r0, r1 = c
        p = jnp.exp2((sref[i % (AHEAD + 1), r0:r1] - m) * C)
        l = fold(jnp.sum, p)
        o = jnp.dot(vt[u, :, r0:r1], p.astype(BF), preferred_element_type=F32)
        return (acc[0] + l, acc[1] + o) if acc else (l, o)

    def finish(i, m, a, l, o):
        u, j = items[i]
        h = heads[u]
        if not first:
            l = ml[h, j, 1:2] * a + l
        if out is None:
            oacc[h, j] = o if first else oacc[h, j] * a + o
            ml[h, j, 0:1] = m
            ml[h, j, 1:2] = l
            return
        r = 1.0 / l
        o = oacc[h, j] * (a * r) + o * r
        out(u)[j * SUB:(j + 1) * SUB] = o.T.astype(BF).reshape(SUB, G, D)

    todo = [(i, c) for i, (u, j) in enumerate(items) for c in chunks((j + 1) * rows)]
    total = len(todo)
    sizes = [len(chunks((j + 1) * rows)) for u, j in items]
    at = 0
    while at < total and todo[at][0] < AHEAD:
        scores(*todo[at])
        at += 1
    for i, (u, j) in enumerate(items):
        if hook and i == HOOK:
            hook()
        top = jnp.max(tops[i], axis=0, keepdims=True)
        m, a = top, None
        if not first:
            m1 = ml[heads[u], j, 0:1]
            m = jnp.maximum(top, m1)
            a = jnp.exp2((m1 - m) * C)
        acc = None
        goal = sum(sizes[:i + AHEAD + 1])
        start = at
        mine = chunks((j + 1) * rows)
        for t, c in enumerate(mine):
            upto = start + (goal - start) * (t + 1) // len(mine)
            while at < upto:
                scores(*todo[at])
                at += 1
            acc = values(i, c, m, acc)
        finish(i, m, a, jnp.sum(acc[0], axis=0, keepdims=True), acc[1])


def near(kv1, chip):
    def of(h):
        return lambda kind, x, t: kv1[h, kind, chip + x // 2, x % 2, t * SUB:(t + 1) * SUB]
    return of


def far(kv2):
    def of(h):
        return lambda kind, x, t: kv2[h, kind, x, t * SUB:(t + 1) * SUB]
    return of


def kernel(q_hbm, k_hbm, v_hbm, ob, qt, kv2, bias2, oacc, ml, raw, wide, kv1, vt, sref, bias0, bias1,
           lsem, qsem, ssem, rsem, lssem, lrsem):
    cx, cy, cz = lax.axis_index("cx"), lax.axis_index("cy"), lax.axis_index("cz")
    me = (cx * 2 + cy) * 2 + cz
    chip = cx * 2 + cy
    link = 1 - (cx + cz - 2 * cx * cz)
    mine = 1 - link

    def over(role):
        x = cx + link - 2 * cx * link
        y = cy + mine - 2 * cy * mine
        return {"cx": x, "cy": y, "cz": x + (1 - role) - 2 * x * (1 - role)}

    sib = {"cz": 1 - cz}

    half_t = T // 2
    loads = [pltpu.make_async_copy(x.at[pl.ds(r, half_t)], raw.at[i, pl.ds(r, half_t)], lsem.at[2 * i + r // half_t])
             for i, x in enumerate((k_hbm, v_hbm)) for r in (0, half_t)]
    for x in loads:
        x.start()

    barrier = pltpu.get_barrier_semaphore()
    for dev in ({"cy": 1 - cy, "cz": 1 - cx}, {"cx": 1 - cx, "cz": 1 - cx}, sib):
        pl.semaphore_signal(barrier, inc=1, device_id=dev, device_id_type=pl.DeviceIdType.MESH)

    def qload(h):
        return pltpu.make_async_copy(q_hbm.at[:, pl.ds(pl.multiple_of(h * G, G), G), :], qt.at[h], qsem.at[h])

    def rdma(src, dst, send, recv, h, dev):
        return pltpu.make_async_remote_copy(src, dst, ssem.at[send, h], rsem.at[recv, h], dev,
                                            pl.DeviceIdType.MESH)

    def swap(h):
        return rdma(kv1.at[h, :, 0, cz], kv1.at[h, :, 0, cz], 0, 5, h, sib)

    def out(h, i, n):
        heads = pl.ds(h, n)
        return rdma(kv1.at[heads, i, 0], kv1.at[heads, i, 1 + link], 1 + i, link, h, over(1 - i))

    def half(h, i, z):
        return rdma(kv1.at[h, i, 0, z], kv1.at[h, i, 1 + link, z], 1 + i, link, h, over(1 - i))

    def relay(h):
        return rdma(kv1.at[h, mine, 1:3], kv1.at[h, mine, 1:3], 3, 2, h, sib)

    def forward(h):
        return rdma(kv1.at[h, mine, 2 - link], kv2.at[h, mine], 4, 3, h, over(link))

    def last(part):
        z, rows = ((0, pl.ds(0, T)), (1, pl.ds(0, CUT)), (1, pl.ds(CUT, T - CUT)), (1, pl.ds(CUT, T - CUT)))[part]
        return pltpu.make_async_remote_copy(kv1.at[HKV - 1, mine, 2 - link, z, rows], kv2.at[HKV - 1, mine, z, rows],
                                            lssem.at[part], lrsem.at[part], over(mine if part == 3 else link),
                                            pl.DeviceIdType.MESH)

    def last_relay(z):
        rows = pl.ds(0, CUT if z else T)
        return pltpu.make_async_remote_copy(kv2.at[HKV - 1, mine, z, rows], kv2.at[HKV - 1, mine, z, rows],
                                            lssem.at[4 + z], lrsem.at[4 + z], sib, pl.DeviceIdType.MESH)

    def relay2(h):
        return rdma(kv2.at[h, mine], kv2.at[h, mine], 5, 4, h, sib)

    def arrived(dst, recv, h):
        rdma(dst, dst, 0, recv, h, sib).wait_recv()

    def mask(nslot, far_chip, ref):
        r = lax.broadcasted_iota(jnp.int32, (nslot * SUB, QB), 0)
        c = lax.broadcasted_iota(jnp.int32, (nslot * SUB, QB), 1)
        x = r // SUB
        kpos = (r % SUB) * 8 + (chip ^ (x // 2 + far_chip)) * 2 + x % 2
        qpos = (c // G) * 8 + me
        ref[...] = jnp.where(kpos <= qpos, 0.0, -1e30)

    def relaid(h, i):
        kv1[h, i, 0, cz] = wide[i, pl.ds(h, T, stride=HKV), :].astype(BF)

    def relaid(h, i):
        kv1[h, i, 0, cz] = wide[i, pl.ds(h, T, stride=HKV), :].astype(BF)

    for i in range(2):
        for r in range(2):
            loads[2 * i + r].wait()
            rows = raw[i, r * half_t:(r + 1) * half_t]
            wide[i, r * half_t * HKV:(r + 1) * half_t * HKV] = rows.astype(F32).reshape(half_t * HKV, D)
        relaid(0, i)
        if i == 0:
            pl.semaphore_wait(barrier, 3)
        else:
            relaid(1, 0)
        half(0, i, cz).start()
    swap(0).start()
    relaid(1, 1)

    for h in range(2, HKV):
        for i in range(2):
            relaid(h, i)
        if h == 2:
            for i in range(2):
                half(1, i, cz).start()
        swap(h - 1).start()

    mask(2, 0, bias0)
    swap(HKV - 1).start()

    for h in range(2):
        arrived(kv1.at[h, :, 0, cz], 5, h)
        for i in range(2):
            half(h, i, 1 - cz).start()

    for h, n in SENDS:
        for x in range(h, h + n):
            arrived(kv1.at[x, :, 0, cz], 5, x)
        for i in range(2):
            out(h, i, n).start()

    @pl.loop(0, HKV)
    def _(h):
        qload(h).start()

    mask(4, 1, bias1)
    mask(2, 3, bias2)

    def pass_on(h):
        middle = (h >= 2) & (h < 6)

        @pl.when(jnp.logical_not(middle))
        def _():
            arrived(kv1.at[h, mine, 1], 0, h)
            arrived(kv1.at[h, mine, 2], 1, h)

        @pl.when(middle & (h % 2 == 0))
        def _():
            arrived(kv1.at[0:2, mine, 1], 0, h)
            arrived(kv1.at[0:2, mine, 2], 1, h)

        relay(h).start()

        @pl.when(h < HKV - 1)
        def _():
            forward(h).start()

        @pl.when(h == HKV - 1)
        def _():
            for part in range(4):
                last(part).start()

    def pass_on2(h):
        @pl.when(h < HKV - 1)
        def _():
            arrived(kv2.at[h, mine], 3, h)
            relay2(h).start()

        @pl.when(h == HKV - 1)
        def _():
            for z in range(2):
                last(z).wait_recv()
                last_relay(z).start()

    @pl.loop(0, HKV // U0)
    def _(g):
        heads = [g * U0 + u for u in range(U0)]

        def arrive(u):
            h = heads[u]
            qload(h).wait()

        attend(heads, near(kv1, 0), 2, bias0, qt, oacc, ml, vt, sref, arrive, first=True)

    pass_on(jnp.int32(0))

    @pl.loop(0, HKV - 1)
    def _(h):
        pass_on(h + 1)
        arrived(kv1.at[h, link, 1:3], 2, h)
        attend([h], near(kv1, 1), 4, bias1, qt, oacc, ml, vt, sref)

    arrived(kv1.at[HKV - 1, link, 1:3], 2, HKV - 1)
    attend([HKV - 1], near(kv1, 1), 4, bias1, qt, oacc, ml, vt, sref, hook=lambda: pass_on2(jnp.int32(0)))

    for h, n in ((0, 1), (1, 1)) + SENDS:
        for i in range(2):
            out(h, i, n).wait_send()

    @pl.loop(0, HKV)
    def _(h):
        swap(h).wait_send()
        relay(h).wait_send()

    @pl.loop(0, (HKV - 1) // U2)
    def _(g):
        heads = [g * U2 + u for u in range(U2)]

        def arrive(u):
            pass_on2(heads[u] + 1)
            arrived(kv2.at[heads[u], link], 4, heads[u])

        attend(heads, far(kv2), 2, bias2, qt, oacc, ml, vt, sref, arrive, out=lambda u: ob.at[heads[u]])

    @pl.loop(0, HKV - 1)
    def _(h):
        forward(h).wait_send()
        relay2(h).wait_send()

    for z in range(2):
        last_relay(z).wait_recv()
    for part in (2, 3):
        last(part).wait_recv()

    for part in range(4):
        last(part).wait_send()
    for z in range(2):
        last_relay(z).wait_send()


def spread(ob, qt, kv2, bias2, oacc, ml, o_hbm, last, vt, sref, sem):
    def put(src, h):
        return pltpu.make_async_copy(src, o_hbm.at[:, pl.ds(pl.multiple_of(h * G, G), G), :], sem.at[h])

    @pl.loop(0, HKV - 1)
    def _(h):
        put(ob.at[h], h).start()

    attend([HKV - 1], far(kv2), 2, bias2, qt, oacc, ml, vt, sref, out=lambda u: last)
    put(last, HKV - 1).start()

    @pl.loop(0, HKV - 1)
    def _(h):
        put(ob.at[h], h).wait()

    put(last, HKV - 1).wait()


def solution(mesh):
    spec = P(("dp", "cx", "cy", "cz"))

    def local(q, k, v):
        hbm = pl.BlockSpec(memory_space=pltpu.HBM)
        vmem = pl.BlockSpec(memory_space=pltpu.VMEM)
        parts = pl.pallas_call(
            kernel,
            out_shape=[
                pltpu.VMEM((HKV - 1, T, G, D), BF),
                pltpu.VMEM((HKV, T, G, D), BF),
                pltpu.VMEM((HKV, 2, 2, T, D), BF),
                pltpu.VMEM((S2 * SUB, QB), F32),
                pltpu.VMEM((HKV, NB, D, QB), F32),
                pltpu.VMEM((HKV, NB, 8, QB), F32),
            ],
            in_specs=[hbm] * 3,
            out_specs=[vmem] * 6,
            scratch_shapes=[
                pltpu.VMEM((2, T, HKV, D), BF),
                pltpu.VMEM((2, T * HKV, D), F32),
                pltpu.VMEM((HKV, 2, 3, 2, T, D), BF),
                pltpu.VMEM((max(U0, U1, U2), D, 4 * T), BF),
                pltpu.VMEM((AHEAD + 1, 4 * T, QB), F32),
                pltpu.VMEM((2 * SUB, QB), F32),
                pltpu.VMEM((4 * SUB, QB), F32),
                pltpu.SemaphoreType.DMA((4,)),
                pltpu.SemaphoreType.DMA((HKV,)),
                pltpu.SemaphoreType.DMA((6, HKV)),
                pltpu.SemaphoreType.DMA((6, HKV)),
                pltpu.SemaphoreType.DMA((6,)),
                pltpu.SemaphoreType.DMA((6,)),
            ],
            compiler_params=pltpu.CompilerParams(
                vmem_limit_bytes=36 << 20, collective_id=0, has_side_effects=True),
        )(*(pltpu.with_memory_space_constraint(x, pltpu.HBM) for x in (q, k, v)))
        return pl.pallas_call(
            spread,
            out_shape=jax.ShapeDtypeStruct(q.shape, q.dtype),
            in_specs=[vmem] * 6,
            out_specs=hbm,
            scratch_shapes=[
                pltpu.VMEM((T, G, D), BF),
                pltpu.VMEM((1, D, S2 * T), BF),
                pltpu.VMEM((AHEAD + 1, S2 * T, QB), F32),
                pltpu.SemaphoreType.DMA((HKV,)),
            ],
            compiler_params=pltpu.CompilerParams(vmem_limit_bytes=8 << 20),
        )(*parts)

    return jax.shard_map(local, mesh=mesh, in_specs=(spec, spec, spec), out_specs=spec, check_vma=False)
```

```python
import jax
import jax.numpy as jnp
from jax import lax
from jax.experimental import pallas as pl
from jax.experimental.pallas import tpu as pltpu
from jax.sharding import PartitionSpec as P

T = 256
CUT = 192
SENDS = ((2, 2), (4, 2), (6, 1), (7, 1))
HKV = 8
G = 8
D = 128
NB = 8
SUB = T // NB
QB = SUB * G
S1 = 6
S2 = 2
C = (D ** -0.5) * 1.4426950408889634
ORDER = (0, 2, 4, 6, 7, 5, 3, 1)
AHEAD = 4
HOOK = 4
U0, U1, U2 = 1, 1, 1
BF = jnp.bfloat16
F32 = jnp.float32
NT = (((1,), (1,)), ((), ()))


def chunks(n):
    return [(r, min(r + 256, n)) for r in range(0, n, 256)]


def by_tile(piece, kind, ns):
    return jnp.concatenate([piece(kind, x, t) for t in range(NB) for x in range(ns)], axis=0)


def fold(f, x):
    return f(x.reshape(-1, 8, x.shape[-1]), axis=0)


def attend(heads, piece_of, ns, bias, qt, oacc, ml, vt, sref, arrive=None, first=False, out=None, hook=None):
    rows = ns * SUB
    items = [(u, j) for u in range(len(heads)) for j in ORDER]
    tops = {}

    def scores(i, c):
        u, j = items[i]
        h = heads[u]
        r0, r1 = c
        if j == ORDER[0] and r0 == 0:
            if arrive:
                arrive(u)
            vt[u, :, :ns * T] = by_tile(piece_of(h), 1, ns).T
        parts = [piece_of(h)(0, x % ns, x // ns) for x in range(r0 // SUB, r1 // SUB)]
        s = lax.dot_general(jnp.concatenate(parts, axis=0), qt[h, j * SUB:(j + 1) * SUB].reshape(QB, D), NT,
                            preferred_element_type=F32)
        lo = max(r0, j * rows)
        if lo < r1:
            d = s[lo - r0:] + bias[lo - j * rows:r1 - j * rows]
            s = d if lo == r0 else jnp.concatenate([s[:lo - r0], d], axis=0)
        sref[i % (AHEAD + 1), r0:r1] = s
        m = fold(jnp.max, s)
        tops[i] = jnp.maximum(tops[i], m) if i in tops else m

    def values(i, c, m, acc):
        u, j = items[i]
        r0, r1 = c
        p = jnp.exp2((sref[i % (AHEAD + 1), r0:r1] - m) * C)
        l = fold(jnp.sum, p)
        o = jnp.dot(vt[u, :, r0:r1], p.astype(BF), preferred_element_type=F32)
        return (acc[0] + l, acc[1] + o) if acc else (l, o)

    def finish(i, m, a, l, o):
        u, j = items[i]
        h = heads[u]
        if not first:
            l = ml[h, j, 1:2] * a + l
        if out is None:
            oacc[h, j] = o if first else oacc[h, j] * a + o
            ml[h, j, 0:1] = m
            ml[h, j, 1:2] = l
            return
        r = 1.0 / l
        o = oacc[h, j] * (a * r) + o * r
        out(u)[j * SUB:(j + 1) * SUB] = o.T.astype(BF).reshape(SUB, G, D)

    todo = [(i, c) for i, (u, j) in enumerate(items) for c in chunks((j + 1) * rows)]
    total = len(todo)
    sizes = [len(chunks((j + 1) * rows)) for u, j in items]
    at = 0
    while at < total and todo[at][0] < AHEAD:
        scores(*todo[at])
        at += 1
    for i, (u, j) in enumerate(items):
        if hook and i == HOOK:
            hook()
        top = jnp.max(tops[i], axis=0, keepdims=True)
        m, a = top, None
        if not first:
            m1 = ml[heads[u], j, 0:1]
            m = jnp.maximum(top, m1)
            a = jnp.exp2((m1 - m) * C)
        acc = None
        goal = sum(sizes[:i + AHEAD + 1])
        start = at
        mine = chunks((j + 1) * rows)
        for t, c in enumerate(mine):
            upto = start + (goal - start) * (t + 1) // len(mine)
            while at < upto:
                scores(*todo[at])
                at += 1
            acc = values(i, c, m, acc)
        finish(i, m, a, jnp.sum(acc[0], axis=0, keepdims=True), acc[1])


def near(kv1, chip):
    def of(h):
        return lambda kind, x, t: kv1[h, kind, chip + x // 2, x % 2, t * SUB:(t + 1) * SUB]
    return of


def far(kv2):
    def of(h):
        return lambda kind, x, t: kv2[h, kind, x, t * SUB:(t + 1) * SUB]
    return of


def kernel(q_hbm, k_hbm, v_hbm, ob, qt, kv2, bias2, oacc, ml, raw, wide, kv1, vt, sref, bias0, bias1,
           lsem, qsem, ssem, rsem, lssem, lrsem):
    cx, cy, cz = lax.axis_index("cx"), lax.axis_index("cy"), lax.axis_index("cz")
    me = (cx * 2 + cy) * 2 + cz
    chip = cx * 2 + cy
    link = 1 - (cx + cz - 2 * cx * cz)
    mine = 1 - link

    def over(role):
        x = cx + link - 2 * cx * link
        y = cy + mine - 2 * cy * mine
        return {"cx": x, "cy": y, "cz": x + (1 - role) - 2 * x * (1 - role)}

    sib = {"cz": 1 - cz}

    half_t = T // 2
    loads = [pltpu.make_async_copy(x.at[pl.ds(r, half_t)], raw.at[i, pl.ds(r, half_t)], lsem.at[2 * i + r // half_t])
             for i, x in enumerate((k_hbm, v_hbm)) for r in (0, half_t)]
    for x in loads:
        x.start()

    barrier = pltpu.get_barrier_semaphore()
    for dev in ({"cy": 1 - cy, "cz": 1 - cx}, {"cx": 1 - cx, "cz": 1 - cx}, sib):
        pl.semaphore_signal(barrier, inc=1, device_id=dev, device_id_type=pl.DeviceIdType.MESH)

    def qload(h):
        return pltpu.make_async_copy(q_hbm.at[:, pl.ds(pl.multiple_of(h * G, G), G), :], qt.at[h], qsem.at[h])

    def rdma(src, dst, send, recv, h, dev):
        return pltpu.make_async_remote_copy(src, dst, ssem.at[send, h], rsem.at[recv, h], dev,
                                            pl.DeviceIdType.MESH)

    def swap(h):
        return rdma(kv1.at[h, :, 0, cz], kv1.at[h, :, 0, cz], 0, 5, h, sib)

    def out(h, i, n):
        heads = pl.ds(h, n)
        return rdma(kv1.at[heads, i, 0], kv1.at[heads, i, 1 + link], 1 + i, link, h, over(1 - i))

    def half(h, i, z):
        return rdma(kv1.at[h, i, 0, z], kv1.at[h, i, 1 + link, z], 1 + i, link, h, over(1 - i))

    def relay(h):
        return rdma(kv1.at[h, mine, 1:3], kv1.at[h, mine, 1:3], 3, 2, h, sib)

    def forward(h):
        return rdma(kv1.at[h, mine, 2 - link], kv2.at[h, mine], 4, 3, h, over(link))

    def last(part):
        z, rows = ((0, pl.ds(0, T)), (1, pl.ds(0, CUT)), (1, pl.ds(CUT, T - CUT)), (1, pl.ds(CUT, T - CUT)))[part]
        return pltpu.make_async_remote_copy(kv1.at[HKV - 1, mine, 2 - link, z, rows], kv2.at[HKV - 1, mine, z, rows],
                                            lssem.at[part], lrsem.at[part], over(mine if part == 3 else link),
                                            pl.DeviceIdType.MESH)

    def last_relay(z):
        rows = pl.ds(0, CUT if z else T)
        return pltpu.make_async_remote_copy(kv2.at[HKV - 1, mine, z, rows], kv2.at[HKV - 1, mine, z, rows],
                                            lssem.at[4 + z], lrsem.at[4 + z], sib, pl.DeviceIdType.MESH)

    def relay2(h):
        return rdma(kv2.at[h, mine], kv2.at[h, mine], 5, 4, h, sib)

    def arrived(dst, recv, h):
        rdma(dst, dst, 0, recv, h, sib).wait_recv()

    def mask(nslot, far_chip, ref):
        r = lax.broadcasted_iota(jnp.int32, (nslot * SUB, QB), 0)
        c = lax.broadcasted_iota(jnp.int32, (nslot * SUB, QB), 1)
        x = r // SUB
        kpos = (r % SUB) * 8 + (chip ^ (x // 2 + far_chip)) * 2 + x % 2
        qpos = (c // G) * 8 + me
        ref[...] = jnp.where(kpos <= qpos, 0.0, -1e30)

    def relaid(h, i):
        kv1[h, i, 0, cz] = wide[i, pl.ds(h, T, stride=HKV), :].astype(BF)

    def relaid(h, i):
        kv1[h, i, 0, cz] = wide[i, pl.ds(h, T, stride=HKV), :].astype(BF)

    for i in range(2):
        for r in range(2):
            loads[2 * i + r].wait()
            rows = raw[i, r * half_t:(r + 1) * half_t]
            wide[i, r * half_t * HKV:(r + 1) * half_t * HKV] = rows.astype(F32).reshape(half_t * HKV, D)
        relaid(0, i)
        if i == 0:
            pl.semaphore_wait(barrier, 3)
        else:
            relaid(1, 0)
        half(0, i, cz).start()
    swap(0).start()
    relaid(1, 1)

    for h in range(2, HKV):
        for i in range(2):
            relaid(h, i)
        if h == 2:
            for i in range(2):
                half(1, i, cz).start()
        swap(h - 1).start()

    mask(2, 0, bias0)
    swap(HKV - 1).start()

    for h in range(2):
        arrived(kv1.at[h, :, 0, cz], 5, h)
        for i in range(2):
            half(h, i, 1 - cz).start()

    for h, n in SENDS:
        for x in range(h, h + n):
            arrived(kv1.at[x, :, 0, cz], 5, x)
        for i in range(2):
            out(h, i, n).start()

    @pl.loop(0, HKV)
    def _(h):
        qload(h).start()

    mask(4, 1, bias1)
    mask(2, 3, bias2)

    def pass_on(h):
        middle = (h >= 2) & (h < 6)

        @pl.when(jnp.logical_not(middle))
        def _():
            arrived(kv1.at[h, mine, 1], 0, h)
            arrived(kv1.at[h, mine, 2], 1, h)

        @pl.when(middle & (h % 2 == 0))
        def _():
            arrived(kv1.at[0:2, mine, 1], 0, h)
            arrived(kv1.at[0:2, mine, 2], 1, h)

        relay(h).start()

        @pl.when(h < HKV - 1)
        def _():
            forward(h).start()

        @pl.when(h == HKV - 1)
        def _():
            for part in range(4):
                last(part).start()

    def pass_on2(h):
        @pl.when(h < HKV - 1)
        def _():
            arrived(kv2.at[h, mine], 3, h)
            relay2(h).start()

        @pl.when(h == HKV - 1)
        def _():
            for z in range(2):
                last(z).wait_recv()
                last_relay(z).start()

    @pl.loop(0, HKV // U0)
    def _(g):
        heads = [g * U0 + u for u in range(U0)]

        def arrive(u):
            h = heads[u]
            qload(h).wait()

        attend(heads, near(kv1, 0), 2, bias0, qt, oacc, ml, vt, sref, arrive, first=True)

    pass_on(jnp.int32(0))

    @pl.loop(0, HKV - 1)
    def _(h):
        pass_on(h + 1)
        arrived(kv1.at[h, link, 1:3], 2, h)
        attend([h], near(kv1, 1), 4, bias1, qt, oacc, ml, vt, sref)

    arrived(kv1.at[HKV - 1, link, 1:3], 2, HKV - 1)
    attend([HKV - 1], near(kv1, 1), 4, bias1, qt, oacc, ml, vt, sref, hook=lambda: pass_on2(jnp.int32(0)))

    for h, n in ((0, 1), (1, 1)) + SENDS:
        for i in range(2):
            out(h, i, n).wait_send()

    @pl.loop(0, HKV)
    def _(h):
        swap(h).wait_send()
        relay(h).wait_send()

    @pl.loop(0, (HKV - 1) // U2)
    def _(g):
        heads = [g * U2 + u for u in range(U2)]

        def arrive(u):
            pass_on2(heads[u] + 1)
            arrived(kv2.at[heads[u], link], 4, heads[u])

        attend(heads, far(kv2), 2, bias2, qt, oacc, ml, vt, sref, arrive, out=lambda u: ob.at[heads[u]])

    @pl.loop(0, HKV - 1)
    def _(h):
        forward(h).wait_send()
        relay2(h).wait_send()

    for z in range(2):
        last_relay(z).wait_recv()
    for part in (2, 3):
        last(part).wait_recv()

    for part in range(4):
        last(part).wait_send()
    for z in range(2):
        last_relay(z).wait_send()


def spread(ob, qt, kv2, bias2, oacc, ml, o_hbm, last, vt, sref, sem):
    def put(src, h):
        return pltpu.make_async_copy(src, o_hbm.at[:, pl.ds(pl.multiple_of(h * G, G), G), :], sem.at[h])

    @pl.loop(0, HKV - 1)
    def _(h):
        put(ob.at[h], h).start()

    attend([HKV - 1], far(kv2), 2, bias2, qt, oacc, ml, vt, sref, out=lambda u: last)
    put(last, HKV - 1).start()

    @pl.loop(0, HKV - 1)
    def _(h):
        put(ob.at[h], h).wait()

    put(last, HKV - 1).wait()


def solution(mesh):
    spec = P(("dp", "cx", "cy", "cz"))

    def local(q, k, v):
        hbm = pl.BlockSpec(memory_space=pltpu.HBM)
        vmem = pl.BlockSpec(memory_space=pltpu.VMEM)
        parts = pl.pallas_call(
            kernel,
            out_shape=[
                pltpu.VMEM((HKV - 1, T, G, D), BF),
                pltpu.VMEM((HKV, T, G, D), BF),
                pltpu.VMEM((HKV, 2, 2, T, D), BF),
                pltpu.VMEM((S2 * SUB, QB), F32),
                pltpu.VMEM((HKV, NB, D, QB), F32),
                pltpu.VMEM((HKV, NB, 8, QB), F32),
            ],
            in_specs=[hbm] * 3,
            out_specs=[vmem] * 6,
            scratch_shapes=[
                pltpu.VMEM((2, T, HKV, D), BF),
                pltpu.VMEM((2, T * HKV, D), F32),
                pltpu.VMEM((HKV, 2, 3, 2, T, D), BF),
                pltpu.VMEM((max(U0, U1, U2), D, 4 * T), BF),
                pltpu.VMEM((AHEAD + 1, 4 * T, QB), F32),
                pltpu.VMEM((2 * SUB, QB), F32),
                pltpu.VMEM((4 * SUB, QB), F32),
                pltpu.SemaphoreType.DMA((4,)),
                pltpu.SemaphoreType.DMA((HKV,)),
                pltpu.SemaphoreType.DMA((6, HKV)),
                pltpu.SemaphoreType.DMA((6, HKV)),
                pltpu.SemaphoreType.DMA((6,)),
                pltpu.SemaphoreType.DMA((6,)),
            ],
            compiler_params=pltpu.CompilerParams(
                vmem_limit_bytes=36 << 20, collective_id=0, has_side_effects=True),
        )(*(pltpu.with_memory_space_constraint(x, pltpu.HBM) for x in (q, k, v)))
        return pl.pallas_call(
            spread,
            out_shape=jax.ShapeDtypeStruct(q.shape, q.dtype),
            in_specs=[vmem] * 6,
            out_specs=hbm,
            scratch_shapes=[
                pltpu.VMEM((T, G, D), BF),
                pltpu.VMEM((1, D, S2 * T), BF),
                pltpu.VMEM((AHEAD + 1, S2 * T, QB), F32),
                pltpu.SemaphoreType.DMA((HKV,)),
            ],
            compiler_params=pltpu.CompilerParams(vmem_limit_bytes=8 << 20),
        )(*parts)

    return jax.shard_map(local, mesh=mesh, in_specs=(spec, spec, spec), out_specs=spec, check_vma=False)
```

```python
import jax
import jax.numpy as jnp
from jax import lax
from jax.experimental import pallas as pl
from jax.experimental.pallas import tpu as pltpu
from jax.sharding import PartitionSpec as P

T = 256
CUT = 64
SENDS = ((2, 2), (4, 2), (6, 1), (7, 1))
HKV = 8
G = 8
D = 128
NB = 8
SUB = T // NB
QB = SUB * G
S1 = 6
S2 = 2
C = (D ** -0.5) * 1.4426950408889634
ORDER = (0, 2, 4, 6, 7, 5, 3, 1)
AHEAD = 4
HOOK = 4
U0, U1, U2 = 1, 1, 1
BF = jnp.bfloat16
F32 = jnp.float32
NT = (((1,), (1,)), ((), ()))


def chunks(n):
    return [(r, min(r + 256, n)) for r in range(0, n, 256)]


def by_tile(piece, kind, ns):
    return jnp.concatenate([piece(kind, x, t) for t in range(NB) for x in range(ns)], axis=0)


def fold(f, x):
    return f(x.reshape(-1, 8, x.shape[-1]), axis=0)


def attend(heads, piece_of, ns, bias, qt, oacc, ml, vt, sref, arrive=None, first=False, out=None, hook=None):
    rows = ns * SUB
    items = [(u, j) for u in range(len(heads)) for j in ORDER]
    tops = {}

    def scores(i, c):
        u, j = items[i]
        h = heads[u]
        r0, r1 = c
        if j == ORDER[0] and r0 == 0:
            if arrive:
                arrive(u)
            vt[u, :, :ns * T] = by_tile(piece_of(h), 1, ns).T
        parts = [piece_of(h)(0, x % ns, x // ns) for x in range(r0 // SUB, r1 // SUB)]
        s = lax.dot_general(jnp.concatenate(parts, axis=0), qt[h, j * SUB:(j + 1) * SUB].reshape(QB, D), NT,
                            preferred_element_type=F32)
        lo = max(r0, j * rows)
        if lo < r1:
            d = s[lo - r0:] + bias[lo - j * rows:r1 - j * rows]
            s = d if lo == r0 else jnp.concatenate([s[:lo - r0], d], axis=0)
        sref[i % (AHEAD + 1), r0:r1] = s
        m = fold(jnp.max, s)
        tops[i] = jnp.maximum(tops[i], m) if i in tops else m

    def values(i, c, m, acc):
        u, j = items[i]
        r0, r1 = c
        p = jnp.exp2((sref[i % (AHEAD + 1), r0:r1] - m) * C)
        l = fold(jnp.sum, p)
        o = jnp.dot(vt[u, :, r0:r1], p.astype(BF), preferred_element_type=F32)
        return (acc[0] + l, acc[1] + o) if acc else (l, o)

    def finish(i, m, a, l, o):
        u, j = items[i]
        h = heads[u]
        if not first:
            l = ml[h, j, 1:2] * a + l
        if out is None:
            oacc[h, j] = o if first else oacc[h, j] * a + o
            ml[h, j, 0:1] = m
            ml[h, j, 1:2] = l
            return
        r = 1.0 / l
        o = oacc[h, j] * (a * r) + o * r
        out(u)[j * SUB:(j + 1) * SUB] = o.T.astype(BF).reshape(SUB, G, D)

    todo = [(i, c) for i, (u, j) in enumerate(items) for c in chunks((j + 1) * rows)]
    total = len(todo)
    sizes = [len(chunks((j + 1) * rows)) for u, j in items]
    at = 0
    while at < total and todo[at][0] < AHEAD:
        scores(*todo[at])
        at += 1
    for i, (u, j) in enumerate(items):
        if hook and i == HOOK:
            hook()
        top = jnp.max(tops[i], axis=0, keepdims=True)
        m, a = top, None
        if not first:
            m1 = ml[heads[u], j, 0:1]
            m = jnp.maximum(top, m1)
            a = jnp.exp2((m1 - m) * C)
        acc = None
        goal = sum(sizes[:i + AHEAD + 1])
        start = at
        mine = chunks((j + 1) * rows)
        for t, c in enumerate(mine):
            upto = start + (goal - start) * (t + 1) // len(mine)
            while at < upto:
                scores(*todo[at])
                at += 1
            acc = values(i, c, m, acc)
        finish(i, m, a, jnp.sum(acc[0], axis=0, keepdims=True), acc[1])


def near(kv1, chip):
    def of(h):
        return lambda kind, x, t: kv1[h, kind, chip + x // 2, x % 2, t * SUB:(t + 1) * SUB]
    return of


def far(kv2):
    def of(h):
        return lambda kind, x, t: kv2[h, kind, x, t * SUB:(t + 1) * SUB]
    return of


def kernel(q_hbm, k_hbm, v_hbm, ob, qt, kv2, bias2, oacc, ml, raw, wide, kv1, vt, sref, bias0, bias1,
           lsem, qsem, ssem, rsem, lssem, lrsem):
    cx, cy, cz = lax.axis_index("cx"), lax.axis_index("cy"), lax.axis_index("cz")
    me = (cx * 2 + cy) * 2 + cz
    chip = cx * 2 + cy
    link = 1 - (cx + cz - 2 * cx * cz)
    mine = 1 - link

    def over(role):
        x = cx + link - 2 * cx * link
        y = cy + mine - 2 * cy * mine
        return {"cx": x, "cy": y, "cz": x + (1 - role) - 2 * x * (1 - role)}

    sib = {"cz": 1 - cz}

    half_t = T // 2
    loads = [pltpu.make_async_copy(x.at[pl.ds(r, half_t)], raw.at[i, pl.ds(r, half_t)], lsem.at[2 * i + r // half_t])
             for i, x in enumerate((k_hbm, v_hbm)) for r in (0, half_t)]
    for x in loads:
        x.start()

    barrier = pltpu.get_barrier_semaphore()
    for dev in ({"cy": 1 - cy, "cz": 1 - cx}, {"cx": 1 - cx, "cz": 1 - cx}, sib):
        pl.semaphore_signal(barrier, inc=1, device_id=dev, device_id_type=pl.DeviceIdType.MESH)

    def qload(h):
        return pltpu.make_async_copy(q_hbm.at[:, pl.ds(pl.multiple_of(h * G, G), G), :], qt.at[h], qsem.at[h])

    def rdma(src, dst, send, recv, h, dev):
        return pltpu.make_async_remote_copy(src, dst, ssem.at[send, h], rsem.at[recv, h], dev,
                                            pl.DeviceIdType.MESH)

    def swap(h):
        return rdma(kv1.at[h, :, 0, cz], kv1.at[h, :, 0, cz], 0, 5, h, sib)

    def out(h, i, n):
        heads = pl.ds(h, n)
        return rdma(kv1.at[heads, i, 0], kv1.at[heads, i, 1 + link], 1 + i, link, h, over(1 - i))

    def half(h, i, z):
        return rdma(kv1.at[h, i, 0, z], kv1.at[h, i, 1 + link, z], 1 + i, link, h, over(1 - i))

    def relay(h):
        return rdma(kv1.at[h, mine, 1:3], kv1.at[h, mine, 1:3], 3, 2, h, sib)

    def forward(h):
        return rdma(kv1.at[h, mine, 2 - link], kv2.at[h, mine], 4, 3, h, over(link))

    def last(part):
        z, rows = ((0, pl.ds(0, T)), (1, pl.ds(0, CUT)), (1, pl.ds(CUT, T - CUT)), (1, pl.ds(CUT, T - CUT)))[part]
        return pltpu.make_async_remote_copy(kv1.at[HKV - 1, mine, 2 - link, z, rows], kv2.at[HKV - 1, mine, z, rows],
                                            lssem.at[part], lrsem.at[part], over(mine if part == 3 else link),
                                            pl.DeviceIdType.MESH)

    def last_relay(z):
        rows = pl.ds(0, CUT if z else T)
        return pltpu.make_async_remote_copy(kv2.at[HKV - 1, mine, z, rows], kv2.at[HKV - 1, mine, z, rows],
                                            lssem.at[4 + z], lrsem.at[4 + z], sib, pl.DeviceIdType.MESH)

    def relay2(h):
        return rdma(kv2.at[h, mine], kv2.at[h, mine], 5, 4, h, sib)

    def arrived(dst, recv, h):
        rdma(dst, dst, 0, recv, h, sib).wait_recv()

    def mask(nslot, far_chip, ref):
        r = lax.broadcasted_iota(jnp.int32, (nslot * SUB, QB), 0)
        c = lax.broadcasted_iota(jnp.int32, (nslot * SUB, QB), 1)
        x = r // SUB
        kpos = (r % SUB) * 8 + (chip ^ (x // 2 + far_chip)) * 2 + x % 2
        qpos = (c // G) * 8 + me
        ref[...] = jnp.where(kpos <= qpos, 0.0, -1e30)

    def relaid(h, i):
        kv1[h, i, 0, cz] = wide[i, pl.ds(h, T, stride=HKV), :].astype(BF)

    def relaid(h, i):
        kv1[h, i, 0, cz] = wide[i, pl.ds(h, T, stride=HKV), :].astype(BF)

    for i in range(2):
        for r in range(2):
            loads[2 * i + r].wait()
            rows = raw[i, r * half_t:(r + 1) * half_t]
            wide[i, r * half_t * HKV:(r + 1) * half_t * HKV] = rows.astype(F32).reshape(half_t * HKV, D)
        relaid(0, i)
        if i == 0:
            pl.semaphore_wait(barrier, 3)
        else:
            relaid(1, 0)
        half(0, i, cz).start()
    swap(0).start()
    relaid(1, 1)

    for h in range(2, HKV):
        for i in range(2):
            relaid(h, i)
        if h == 2:
            for i in range(2):
                half(1, i, cz).start()
        swap(h - 1).start()

    mask(2, 0, bias0)
    swap(HKV - 1).start()

    for h in range(2):
        arrived(kv1.at[h, :, 0, cz], 5, h)
        for i in range(2):
            half(h, i, 1 - cz).start()

    for h, n in SENDS:
        for x in range(h, h + n):
            arrived(kv1.at[x, :, 0, cz], 5, x)
        for i in range(2):
            out(h, i, n).start()

    @pl.loop(0, HKV)
    def _(h):
        qload(h).start()

    mask(4, 1, bias1)
    mask(2, 3, bias2)

    def pass_on(h):
        middle = (h >= 2) & (h < 6)

        @pl.when(jnp.logical_not(middle))
        def _():
            arrived(kv1.at[h, mine, 1], 0, h)
            arrived(kv1.at[h, mine, 2], 1, h)

        @pl.when(middle & (h % 2 == 0))
        def _():
            arrived(kv1.at[0:2, mine, 1], 0, h)
            arrived(kv1.at[0:2, mine, 2], 1, h)

        relay(h).start()

        @pl.when(h < HKV - 1)
        def _():
            forward(h).start()

        @pl.when(h == HKV - 1)
        def _():
            for part in range(4):
                last(part).start()

    def pass_on2(h):
        @pl.when(h < HKV - 1)
        def _():
            arrived(kv2.at[h, mine], 3, h)
            relay2(h).start()

        @pl.when(h == HKV - 1)
        def _():
            for z in range(2):
                last(z).wait_recv()
                last_relay(z).start()

    @pl.loop(0, HKV // U0)
    def _(g):
        heads = [g * U0 + u for u in range(U0)]

        def arrive(u):
            h = heads[u]
            qload(h).wait()

        attend(heads, near(kv1, 0), 2, bias0, qt, oacc, ml, vt, sref, arrive, first=True)

    pass_on(jnp.int32(0))

    @pl.loop(0, HKV - 1)
    def _(h):
        pass_on(h + 1)
        arrived(kv1.at[h, link, 1:3], 2, h)
        attend([h], near(kv1, 1), 4, bias1, qt, oacc, ml, vt, sref)

    arrived(kv1.at[HKV - 1, link, 1:3], 2, HKV - 1)
    attend([HKV - 1], near(kv1, 1), 4, bias1, qt, oacc, ml, vt, sref, hook=lambda: pass_on2(jnp.int32(0)))

    for h, n in ((0, 1), (1, 1)) + SENDS:
        for i in range(2):
            out(h, i, n).wait_send()

    @pl.loop(0, HKV)
    def _(h):
        swap(h).wait_send()
        relay(h).wait_send()

    @pl.loop(0, (HKV - 1) // U2)
    def _(g):
        heads = [g * U2 + u for u in range(U2)]

        def arrive(u):
            pass_on2(heads[u] + 1)
            arrived(kv2.at[heads[u], link], 4, heads[u])

        attend(heads, far(kv2), 2, bias2, qt, oacc, ml, vt, sref, arrive, out=lambda u: ob.at[heads[u]])

    @pl.loop(0, HKV - 1)
    def _(h):
        forward(h).wait_send()
        relay2(h).wait_send()

    for z in range(2):
        last_relay(z).wait_recv()
    for part in (2, 3):
        last(part).wait_recv()

    for part in range(4):
        last(part).wait_send()
    for z in range(2):
        last_relay(z).wait_send()


def spread(ob, qt, kv2, bias2, oacc, ml, o_hbm, last, vt, sref, sem):
    def put(src, h):
        return pltpu.make_async_copy(src, o_hbm.at[:, pl.ds(pl.multiple_of(h * G, G), G), :], sem.at[h])

    @pl.loop(0, HKV - 1)
    def _(h):
        put(ob.at[h], h).start()

    attend([HKV - 1], far(kv2), 2, bias2, qt, oacc, ml, vt, sref, out=lambda u: last)
    put(last, HKV - 1).start()

    @pl.loop(0, HKV - 1)
    def _(h):
        put(ob.at[h], h).wait()

    put(last, HKV - 1).wait()


def solution(mesh):
    spec = P(("dp", "cx", "cy", "cz"))

    def local(q, k, v):
        hbm = pl.BlockSpec(memory_space=pltpu.HBM)
        vmem = pl.BlockSpec(memory_space=pltpu.VMEM)
        parts = pl.pallas_call(
            kernel,
            out_shape=[
                pltpu.VMEM((HKV - 1, T, G, D), BF),
                pltpu.VMEM((HKV, T, G, D), BF),
                pltpu.VMEM((HKV, 2, 2, T, D), BF),
                pltpu.VMEM((S2 * SUB, QB), F32),
                pltpu.VMEM((HKV, NB, D, QB), F32),
                pltpu.VMEM((HKV, NB, 8, QB), F32),
            ],
            in_specs=[hbm] * 3,
            out_specs=[vmem] * 6,
            scratch_shapes=[
                pltpu.VMEM((2, T, HKV, D), BF),
                pltpu.VMEM((2, T * HKV, D), F32),
                pltpu.VMEM((HKV, 2, 3, 2, T, D), BF),
                pltpu.VMEM((max(U0, U1, U2), D, 4 * T), BF),
                pltpu.VMEM((AHEAD + 1, 4 * T, QB), F32),
                pltpu.VMEM((2 * SUB, QB), F32),
                pltpu.VMEM((4 * SUB, QB), F32),
                pltpu.SemaphoreType.DMA((4,)),
                pltpu.SemaphoreType.DMA((HKV,)),
                pltpu.SemaphoreType.DMA((6, HKV)),
                pltpu.SemaphoreType.DMA((6, HKV)),
                pltpu.SemaphoreType.DMA((6,)),
                pltpu.SemaphoreType.DMA((6,)),
            ],
            compiler_params=pltpu.CompilerParams(
                vmem_limit_bytes=36 << 20, collective_id=0, has_side_effects=True),
        )(*(pltpu.with_memory_space_constraint(x, pltpu.HBM) for x in (q, k, v)))
        return pl.pallas_call(
            spread,
            out_shape=jax.ShapeDtypeStruct(q.shape, q.dtype),
            in_specs=[vmem] * 6,
            out_specs=hbm,
            scratch_shapes=[
                pltpu.VMEM((T, G, D), BF),
                pltpu.VMEM((1, D, S2 * T), BF),
                pltpu.VMEM((AHEAD + 1, S2 * T, QB), F32),
                pltpu.SemaphoreType.DMA((HKV,)),
            ],
            compiler_params=pltpu.CompilerParams(vmem_limit_bytes=8 << 20),
        )(*parts)

    return jax.shard_map(local, mesh=mesh, in_specs=(spec, spec, spec), out_specs=spec, check_vma=False)
```

```python
import jax
import jax.numpy as jnp
from jax import lax
from jax.experimental import pallas as pl
from jax.experimental.pallas import tpu as pltpu
from jax.sharding import PartitionSpec as P

T = 256
CUT = 96
SENDS = ((2, 2), (4, 2), (6, 1), (7, 1))
HKV = 8
G = 8
D = 128
NB = 8
SUB = T // NB
QB = SUB * G
S1 = 6
S2 = 2
C = (D ** -0.5) * 1.4426950408889634
ORDER = (0, 2, 4, 6, 7, 5, 3, 1)
AHEAD = 4
HOOK = 4
U0, U1, U2 = 1, 1, 1
BF = jnp.bfloat16
F32 = jnp.float32
NT = (((1,), (1,)), ((), ()))


def chunks(n):
    return [(r, min(r + 256, n)) for r in range(0, n, 256)]


def by_tile(piece, kind, ns):
    return jnp.concatenate([piece(kind, x, t) for t in range(NB) for x in range(ns)], axis=0)


def fold(f, x):
    return f(x.reshape(-1, 8, x.shape[-1]), axis=0)


def attend(heads, piece_of, ns, bias, qt, oacc, ml, vt, sref, arrive=None, first=False, out=None, hook=None):
    rows = ns * SUB
    items = [(u, j) for u in range(len(heads)) for j in ORDER]
    tops = {}

    def scores(i, c):
        u, j = items[i]
        h = heads[u]
        r0, r1 = c
        if j == ORDER[0] and r0 == 0:
            if arrive:
                arrive(u)
            vt[u, :, :ns * T] = by_tile(piece_of(h), 1, ns).T
        parts = [piece_of(h)(0, x % ns, x // ns) for x in range(r0 // SUB, r1 // SUB)]
        s = lax.dot_general(jnp.concatenate(parts, axis=0), qt[h, j * SUB:(j + 1) * SUB].reshape(QB, D), NT,
                            preferred_element_type=F32)
        lo = max(r0, j * rows)
        if lo < r1:
            d = s[lo - r0:] + bias[lo - j * rows:r1 - j * rows]
            s = d if lo == r0 else jnp.concatenate([s[:lo - r0], d], axis=0)
        sref[i % (AHEAD + 1), r0:r1] = s
        m = fold(jnp.max, s)
        tops[i] = jnp.maximum(tops[i], m) if i in tops else m

    def values(i, c, m, acc):
        u, j = items[i]
        r0, r1 = c
        p = jnp.exp2((sref[i % (AHEAD + 1), r0:r1] - m) * C)
        l = fold(jnp.sum, p)
        o = jnp.dot(vt[u, :, r0:r1], p.astype(BF), preferred_element_type=F32)
        return (acc[0] + l, acc[1] + o) if acc else (l, o)

    def finish(i, m, a, l, o):
        u, j = items[i]
        h = heads[u]
        if not first:
            l = ml[h, j, 1:2] * a + l
        if out is None:
            oacc[h, j] = o if first else oacc[h, j] * a + o
            ml[h, j, 0:1] = m
            ml[h, j, 1:2] = l
            return
        r = 1.0 / l
        o = oacc[h, j] * (a * r) + o * r
        out(u)[j * SUB:(j + 1) * SUB] = o.T.astype(BF).reshape(SUB, G, D)

    todo = [(i, c) for i, (u, j) in enumerate(items) for c in chunks((j + 1) * rows)]
    total = len(todo)
    sizes = [len(chunks((j + 1) * rows)) for u, j in items]
    at = 0
    while at < total and todo[at][0] < AHEAD:
        scores(*todo[at])
        at += 1
    for i, (u, j) in enumerate(items):
        if hook and i == HOOK:
            hook()
        top = jnp.max(tops[i], axis=0, keepdims=True)
        m, a = top, None
        if not first:
            m1 = ml[heads[u], j, 0:1]
            m = jnp.maximum(top, m1)
            a = jnp.exp2((m1 - m) * C)
        acc = None
        goal = sum(sizes[:i + AHEAD + 1])
        start = at
        mine = chunks((j + 1) * rows)
        for t, c in enumerate(mine):
            upto = start + (goal - start) * (t + 1) // len(mine)
            while at < upto:
                scores(*todo[at])
                at += 1
            acc = values(i, c, m, acc)
        finish(i, m, a, jnp.sum(acc[0], axis=0, keepdims=True), acc[1])


def near(kv1, chip):
    def of(h):
        return lambda kind, x, t: kv1[h, kind, chip + x // 2, x % 2, t * SUB:(t + 1) * SUB]
    return of


def far(kv2):
    def of(h):
        return lambda kind, x, t: kv2[h, kind, x, t * SUB:(t + 1) * SUB]
    return of


def kernel(q_hbm, k_hbm, v_hbm, ob, qt, kv2, bias2, oacc, ml, raw, wide, kv1, vt, sref, bias0, bias1,
           lsem, qsem, ssem, rsem, lssem, lrsem):
    cx, cy, cz = lax.axis_index("cx"), lax.axis_index("cy"), lax.axis_index("cz")
    me = (cx * 2 + cy) * 2 + cz
    chip = cx * 2 + cy
    link = 1 - (cx + cz - 2 * cx * cz)
    mine = 1 - link

    def over(role):
        x = cx + link - 2 * cx * link
        y = cy + mine - 2 * cy * mine
        return {"cx": x, "cy": y, "cz": x + (1 - role) - 2 * x * (1 - role)}

    sib = {"cz": 1 - cz}

    half_t = T // 2
    loads = [pltpu.make_async_copy(x.at[pl.ds(r, half_t)], raw.at[i, pl.ds(r, half_t)], lsem.at[2 * i + r // half_t])
             for i, x in enumerate((k_hbm, v_hbm)) for r in (0, half_t)]
    for x in loads:
        x.start()

    barrier = pltpu.get_barrier_semaphore()
    for dev in ({"cy": 1 - cy, "cz": 1 - cx}, {"cx": 1 - cx, "cz": 1 - cx}, sib):
        pl.semaphore_signal(barrier, inc=1, device_id=dev, device_id_type=pl.DeviceIdType.MESH)

    def qload(h):
        return pltpu.make_async_copy(q_hbm.at[:, pl.ds(pl.multiple_of(h * G, G), G), :], qt.at[h], qsem.at[h])

    def rdma(src, dst, send, recv, h, dev):
        return pltpu.make_async_remote_copy(src, dst, ssem.at[send, h], rsem.at[recv, h], dev,
                                            pl.DeviceIdType.MESH)

    def swap(h):
        return rdma(kv1.at[h, :, 0, cz], kv1.at[h, :, 0, cz], 0, 5, h, sib)

    def out(h, i, n):
        heads = pl.ds(h, n)
        return rdma(kv1.at[heads, i, 0], kv1.at[heads, i, 1 + link], 1 + i, link, h, over(1 - i))

    def half(h, i, z):
        return rdma(kv1.at[h, i, 0, z], kv1.at[h, i, 1 + link, z], 1 + i, link, h, over(1 - i))

    def relay(h):
        return rdma(kv1.at[h, mine, 1:3], kv1.at[h, mine, 1:3], 3, 2, h, sib)

    def forward(h):
        return rdma(kv1.at[h, mine, 2 - link], kv2.at[h, mine], 4, 3, h, over(link))

    def last(part):
        z, rows = ((0, pl.ds(0, T)), (1, pl.ds(0, CUT)), (1, pl.ds(CUT, T - CUT)), (1, pl.ds(CUT, T - CUT)))[part]
        return pltpu.make_async_remote_copy(kv1.at[HKV - 1, mine, 2 - link, z, rows], kv2.at[HKV - 1, mine, z, rows],
                                            lssem.at[part], lrsem.at[part], over(mine if part == 3 else link),
                                            pl.DeviceIdType.MESH)

    def last_relay(z):
        rows = pl.ds(0, CUT if z else T)
        return pltpu.make_async_remote_copy(kv2.at[HKV - 1, mine, z, rows], kv2.at[HKV - 1, mine, z, rows],
                                            lssem.at[4 + z], lrsem.at[4 + z], sib, pl.DeviceIdType.MESH)

    def relay2(h):
        return rdma(kv2.at[h, mine], kv2.at[h, mine], 5, 4, h, sib)

    def arrived(dst, recv, h):
        rdma(dst, dst, 0, recv, h, sib).wait_recv()

    def mask(nslot, far_chip, ref):
        r = lax.broadcasted_iota(jnp.int32, (nslot * SUB, QB), 0)
        c = lax.broadcasted_iota(jnp.int32, (nslot * SUB, QB), 1)
        x = r // SUB
        kpos = (r % SUB) * 8 + (chip ^ (x // 2 + far_chip)) * 2 + x % 2
        qpos = (c // G) * 8 + me
        ref[...] = jnp.where(kpos <= qpos, 0.0, -1e30)

    def relaid(h, i):
        kv1[h, i, 0, cz] = wide[i, pl.ds(h, T, stride=HKV), :].astype(BF)

    def relaid(h, i):
        kv1[h, i, 0, cz] = wide[i, pl.ds(h, T, stride=HKV), :].astype(BF)

    for i in range(2):
        for r in range(2):
            loads[2 * i + r].wait()
            rows = raw[i, r * half_t:(r + 1) * half_t]
            wide[i, r * half_t * HKV:(r + 1) * half_t * HKV] = rows.astype(F32).reshape(half_t * HKV, D)
        relaid(0, i)
        if i == 0:
            pl.semaphore_wait(barrier, 3)
        else:
            relaid(1, 0)
        half(0, i, cz).start()
    swap(0).start()
    relaid(1, 1)

    for h in range(2, HKV):
        for i in range(2):
            relaid(h, i)
        if h == 2:
            for i in range(2):
                half(1, i, cz).start()
        swap(h - 1).start()

    mask(2, 0, bias0)
    swap(HKV - 1).start()

    for h in range(2):
        arrived(kv1.at[h, :, 0, cz], 5, h)
        for i in range(2):
            half(h, i, 1 - cz).start()

    for h, n in SENDS:
        for x in range(h, h + n):
            arrived(kv1.at[x, :, 0, cz], 5, x)
        for i in range(2):
            out(h, i, n).start()

    @pl.loop(0, HKV)
    def _(h):
        qload(h).start()

    mask(4, 1, bias1)
    mask(2, 3, bias2)

    def pass_on(h):
        middle = (h >= 2) & (h < 6)

        @pl.when(jnp.logical_not(middle))
        def _():
            arrived(kv1.at[h, mine, 1], 0, h)
            arrived(kv1.at[h, mine, 2], 1, h)

        @pl.when(middle & (h % 2 == 0))
        def _():
            arrived(kv1.at[0:2, mine, 1], 0, h)
            arrived(kv1.at[0:2, mine, 2], 1, h)

        relay(h).start()

        @pl.when(h < HKV - 1)
        def _():
            forward(h).start()

        @pl.when(h == HKV - 1)
        def _():
            for part in range(4):
                last(part).start()

    def pass_on2(h):
        @pl.when(h < HKV - 1)
        def _():
            arrived(kv2.at[h, mine], 3, h)
            relay2(h).start()

        @pl.when(h == HKV - 1)
        def _():
            for z in range(2):
                last(z).wait_recv()
                last_relay(z).start()

    @pl.loop(0, HKV // U0)
    def _(g):
        heads = [g * U0 + u for u in range(U0)]

        def arrive(u):
            h = heads[u]
            qload(h).wait()

        attend(heads, near(kv1, 0), 2, bias0, qt, oacc, ml, vt, sref, arrive, first=True)

    pass_on(jnp.int32(0))

    @pl.loop(0, HKV - 1)
    def _(h):
        pass_on(h + 1)
        arrived(kv1.at[h, link, 1:3], 2, h)
        attend([h], near(kv1, 1), 4, bias1, qt, oacc, ml, vt, sref)

    arrived(kv1.at[HKV - 1, link, 1:3], 2, HKV - 1)
    attend([HKV - 1], near(kv1, 1), 4, bias1, qt, oacc, ml, vt, sref, hook=lambda: pass_on2(jnp.int32(0)))

    for h, n in ((0, 1), (1, 1)) + SENDS:
        for i in range(2):
            out(h, i, n).wait_send()

    @pl.loop(0, HKV)
    def _(h):
        swap(h).wait_send()
        relay(h).wait_send()

    @pl.loop(0, (HKV - 1) // U2)
    def _(g):
        heads = [g * U2 + u for u in range(U2)]

        def arrive(u):
            pass_on2(heads[u] + 1)
            arrived(kv2.at[heads[u], link], 4, heads[u])

        attend(heads, far(kv2), 2, bias2, qt, oacc, ml, vt, sref, arrive, out=lambda u: ob.at[heads[u]])

    @pl.loop(0, HKV - 1)
    def _(h):
        forward(h).wait_send()
        relay2(h).wait_send()

    for z in range(2):
        last_relay(z).wait_recv()
    for part in (2, 3):
        last(part).wait_recv()

    for part in range(4):
        last(part).wait_send()
    for z in range(2):
        last_relay(z).wait_send()


def spread(ob, qt, kv2, bias2, oacc, ml, o_hbm, last, vt, sref, sem):
    def put(src, h):
        return pltpu.make_async_copy(src, o_hbm.at[:, pl.ds(pl.multiple_of(h * G, G), G), :], sem.at[h])

    @pl.loop(0, HKV - 1)
    def _(h):
        put(ob.at[h], h).start()

    attend([HKV - 1], far(kv2), 2, bias2, qt, oacc, ml, vt, sref, out=lambda u: last)
    put(last, HKV - 1).start()

    @pl.loop(0, HKV - 1)
    def _(h):
        put(ob.at[h], h).wait()

    put(last, HKV - 1).wait()


def solution(mesh):
    spec = P(("dp", "cx", "cy", "cz"))

    def local(q, k, v):
        hbm = pl.BlockSpec(memory_space=pltpu.HBM)
        vmem = pl.BlockSpec(memory_space=pltpu.VMEM)
        parts = pl.pallas_call(
            kernel,
            out_shape=[
                pltpu.VMEM((HKV - 1, T, G, D), BF),
                pltpu.VMEM((HKV, T, G, D), BF),
                pltpu.VMEM((HKV, 2, 2, T, D), BF),
                pltpu.VMEM((S2 * SUB, QB), F32),
                pltpu.VMEM((HKV, NB, D, QB), F32),
                pltpu.VMEM((HKV, NB, 8, QB), F32),
            ],
            in_specs=[hbm] * 3,
            out_specs=[vmem] * 6,
            scratch_shapes=[
                pltpu.VMEM((2, T, HKV, D), BF),
                pltpu.VMEM((2, T * HKV, D), F32),
                pltpu.VMEM((HKV, 2, 3, 2, T, D), BF),
                pltpu.VMEM((max(U0, U1, U2), D, 4 * T), BF),
                pltpu.VMEM((AHEAD + 1, 4 * T, QB), F32),
                pltpu.VMEM((2 * SUB, QB), F32),
                pltpu.VMEM((4 * SUB, QB), F32),
                pltpu.SemaphoreType.DMA((4,)),
                pltpu.SemaphoreType.DMA((HKV,)),
                pltpu.SemaphoreType.DMA((6, HKV)),
                pltpu.SemaphoreType.DMA((6, HKV)),
                pltpu.SemaphoreType.DMA((6,)),
                pltpu.SemaphoreType.DMA((6,)),
            ],
            compiler_params=pltpu.CompilerParams(
                vmem_limit_bytes=36 << 20, collective_id=0, has_side_effects=True),
        )(*(pltpu.with_memory_space_constraint(x, pltpu.HBM) for x in (q, k, v)))
        return pl.pallas_call(
            spread,
            out_shape=jax.ShapeDtypeStruct(q.shape, q.dtype),
            in_specs=[vmem] * 6,
            out_specs=hbm,
            scratch_shapes=[
                pltpu.VMEM((T, G, D), BF),
                pltpu.VMEM((1, D, S2 * T), BF),
                pltpu.VMEM((AHEAD + 1, S2 * T, QB), F32),
                pltpu.SemaphoreType.DMA((HKV,)),
            ],
            compiler_params=pltpu.CompilerParams(vmem_limit_bytes=8 << 20),
        )(*parts)

    return jax.shard_map(local, mesh=mesh, in_specs=(spec, spec, spec), out_specs=spec, check_vma=False)
```
